32 devices in a mesh: groups: 2 (over y), row: 4 (over z), col: 2 (over x), sub: 2 (over core).
Axes of the slice: x: 2, y: 2, z: 4, core: 2. Of those that a mesh axis runs over, the one named last changes fastest.
Arguments:
- matrix: float32 [16384, 8192], P(('groups', 'row'), ('col', 'sub')), parts along dimension 0, may hold values from -60 to 60
- basis_vectors: float32 [16384, 1024], P(('groups', 'row'), ('col', 'sub')), parts along dimension 0, may hold values from -0.0625 to 0.0625
- split_size: int32 [2], P('groups'), parts along dimension 0, may hold values from 256 to 767
Outputs:
- children: float32 [2, 2048, 1024], P('sub', ('groups', 'row'), 'col'), parts along dimension 1
The draws below stay inside these ranges and needn't reach their ends.
There are 2 independent parts, one for each index of `groups`. The reference program is written for one: setup_inputs(seed, part) draws one part's arguments, and reference() takes and returns one part's arrays. A program takes and returns all parts, laid end to end along the dimension named above; each array names one. Nothing has to cross between parts.
Inputs may be any that keep to these rules, and one draw needn't show every extreme that they name: The second subspace has 1024 minus split_size vectors.
All inputs are finite; a program needn't handle non-finite values.
Results may differ from the reference program's by a relative error of at most 0.00011.
Values sent between devices are 32-bit elements; how exact they have to be, the bound alone decides.
A program may use at most 128 MiB of HBM per device.

```python
import jax
import jax.numpy as jnp
from jax import lax

N = 8192
K = 1024


def draw_matrix(key, part):
    noise = jax.random.normal(key, (N, N), jnp.float32)
    symmetric = (noise + noise.T) * 0.5 ** 0.5
    return symmetric


def level_of(stream_key, dims, split, least, top_value):
    loudness = 1.0
    for position, parts in split:
        steps = jax.random.uniform(jax.random.fold_in(jax.random.fold_in(stream_key, 6), position), (parts,), jnp.float32, least / len(split), top_value / len(split))
        loudness = loudness * jnp.repeat(jnp.exp(steps), dims[position] // parts).reshape((-1,) + (1,) * (len(dims) - 1 - position))
    return loudness


def gaussian(own_key, shape, spread, most, pieces=(), kind=jnp.bfloat16):
    result = jax.random.normal(own_key, shape, jnp.float32) * spread
    if len(pieces) > 0:
        result = level_of(own_key, shape, pieces, -0.22, 0.18) * result
    return jnp.clip(result, min=-most, max=most).astype(kind)


def setup_inputs(seed: int = 0, part: int = 0) -> dict:
    splits = jax.random.split(jax.random.key(seed), 4)
    part_keys = jax.random.split(jax.random.fold_in(splits[3], part), 4)
    return {
        "matrix": draw_matrix(jax.random.fold_in(jax.random.fold_in(splits[3], part), 71), part),
        "basis_vectors": gaussian(part_keys[1], (N, K), N ** -0.5, 0.0625, ((0, 4), (1, 4)), jnp.float32),
        "split_size": jax.random.randint(part_keys[2], (1,), K // 4, 3 * K // 4).astype(jnp.int32),
    }


def reference(matrix, basis_vectors, split_size):
    image = jnp.dot(matrix, basis_vectors, precision=lax.Precision.HIGHEST, preferred_element_type=jnp.float32)
    projected = jnp.dot(basis_vectors.T, image, precision=lax.Precision.HIGHEST, preferred_element_type=jnp.float32)
    positions = jnp.arange(K, dtype=jnp.int32)
    in_first = positions < split_size[0]
    in_second = jnp.logical_not(in_first)
    mask_one = in_first[:, None] & in_first[None, :]
    mask_two = in_second[:, None] & in_second[None, :]
    nothing = jnp.zeros((), jnp.float32)
    return jnp.stack([jnp.where(mask_one, projected, nothing), jnp.where(mask_two, projected, nothing)])
```

```python
import functools

import jax
import jax.numpy as jnp
from jax import lax
from jax.experimental import pallas as pl
from jax.experimental.pallas import tpu as pltpu
from jax.sharding import PartitionSpec as P

MESH = pl.DeviceIdType.MESH
CHUNKS = 1


def gather_kernel(R, X, S, v, own, spread, lsem, xs, xr, zs, zr, ps, pr, fs, fr):
    r, x, s = lax.axis_index("row"), lax.axis_index("col"), lax.axis_index("sub")
    m, kd = v.shape
    piece = m // R

    def columns(cx, cs):
        return pl.ds(pl.multiple_of((cx * S + cs) * kd, kd), kd)

    peers = [{"col": lax.rem(x + d, X)} for d in range(1, X)]
    peers += [{"row": lax.rem(r + d, R)} for d in range(1, R)]
    peers += [{"sub": lax.rem(s + d, S)} for d in range(1, S)]
    barrier = pltpu.get_barrier_semaphore()
    for peer in peers:
        pl.semaphore_signal(barrier, inc=1, device_id=peer, device_id_type=MESH)
    pl.semaphore_wait(barrier, len(peers))

    mine = own.at[:, columns(x, s)]
    across, spreads, partner, forward = [], [], [], []
    for d in range(1, X):
        across.append(pltpu.make_async_remote_copy(
            v, mine, xs.at[d - 1], xr.at[d - 1],
            device_id={"col": lax.rem(x + d, X)}, device_id_type=MESH))
    for d in range(1, R):
        i = lax.rem(r + d, R)
        spreads.append(pltpu.make_async_remote_copy(
            v.at[pl.ds(pl.multiple_of(i * piece, piece), piece), :], spread.at[r],
            zs.at[d - 1], zr.at[d - 1],
            device_id={"row": i}, device_id_type=MESH))
    for d in range(1, S):
        partner.append(pltpu.make_async_remote_copy(
            v, mine, ps.at[d - 1], pr.at[d - 1],
            device_id={"sub": lax.rem(s + d, S)}, device_id_type=MESH))
    for copy in across + spreads + partner:
        copy.start()
    local = [
        pltpu.make_async_copy(v, mine, lsem.at[0]),
        pltpu.make_async_copy(
            v.at[pl.ds(pl.multiple_of(r * piece, piece), piece), :], spread.at[r], lsem.at[1]),
    ]
    for copy in local:
        copy.start()
    for d in range(1, X):
        across[d - 1].wait_recv()
        block = own.at[:, columns(lax.rem(x - d + X, X), s)]
        for e in range(1, S):
            copy = pltpu.make_async_remote_copy(
                block, block, fs.at[d - 1, e - 1], fr.at[d - 1, e - 1],
                device_id={"sub": lax.rem(s + e, S)}, device_id_type=MESH)
            copy.start()
            forward.append(copy)
    for copy in across:
        copy.wait_send()
    for copy in spreads + partner + forward:
        copy.wait()
    for copy in local:
        copy.wait()


def gather(v, R, X, S):
    m, kd = v.shape
    dma = pltpu.SemaphoreType.DMA
    return pl.pallas_call(
        functools.partial(gather_kernel, R, X, S),
        out_shape=(
            jax.ShapeDtypeStruct((m, kd * X * S), v.dtype),
            jax.ShapeDtypeStruct((R, m // R, kd), v.dtype),
        ),
        in_specs=[pl.BlockSpec(memory_space=pltpu.VMEM)],
        out_specs=(pl.BlockSpec(memory_space=pl.ANY), pl.BlockSpec(memory_space=pl.ANY)),
        scratch_shapes=[
            dma((2,)), dma((X - 1,)), dma((X - 1,)), dma((R - 1,)), dma((R - 1,)),
            dma((S - 1,)), dma((S - 1,)), dma((X - 1, S - 1)), dma((X - 1, S - 1)),
        ],
        compiler_params=pltpu.CompilerParams(collective_id=0, has_side_effects=True),
        cost_estimate=pl.CostEstimate(flops=0, bytes_accessed=100_000_000, transcendentals=0),
        name="gather",
    )(v)


def regroup_kernel(X, S, spread, mine, lsem, ss, rs):
    x, s = lax.axis_index("col"), lax.axis_index("sub")
    C = X * S
    k = x * S + s
    R, piece, kd = spread.shape
    per = R // C
    barrier = pltpu.get_barrier_semaphore()
    dests = [lax.rem(k + e, C) for e in range(C)]
    for j in dests[1:]:
        pl.semaphore_signal(
            barrier, inc=1, device_id={"col": j // S, "sub": lax.rem(j, S)}, device_id_type=MESH)
    pl.semaphore_wait(barrier, C - 1)
    target = mine.at[:, :, pl.ds(pl.multiple_of(k * kd, kd), kd)]
    copies = []
    for e in range(1, C):
        j = dests[e]
        copies.append(pltpu.make_async_remote_copy(
            spread.at[pl.ds(j * per, per)], target, ss.at[e - 1], rs.at[e - 1],
            device_id={"col": j // S, "sub": lax.rem(j, S)}, device_id_type=MESH))
    copies.append(pltpu.make_async_copy(spread.at[pl.ds(k * per, per)], target, lsem))
    for copy in copies:
        copy.start()
    for copy in copies:
        copy.wait()


def regroup(spread, X, S):
    R, piece, kd = spread.shape
    C = X * S
    dma = pltpu.SemaphoreType.DMA
    return pl.pallas_call(
        functools.partial(regroup_kernel, X, S),
        out_shape=jax.ShapeDtypeStruct((R // C, piece, kd * C), spread.dtype),
        in_specs=[pl.BlockSpec(memory_space=pltpu.VMEM)],
        out_specs=pl.BlockSpec(memory_space=pl.ANY),
        scratch_shapes=[dma, dma((C - 1,)), dma((C - 1,))],
        compiler_params=pltpu.CompilerParams(collective_id=1, has_side_effects=True),
        cost_estimate=pl.CostEstimate(flops=0, bytes_accessed=60_000_000, transcendentals=0),
        name="regroup",
    )(spread)


def project_kernel(R, X, S, relative, p, out, acc, from_sub, from_col, from_row, res, from_pair,
                   a_s, a_r, b_s, b_r, c_s, c_r, d_s, d_r):
    r, x, s = lax.axis_index("row"), lax.axis_index("col"), lax.axis_index("sub")
    K = p.shape[0]
    rb, kd = K // R, K // (X * S)

    def rows(i):
        return pl.ds(pl.multiple_of(i * rb, rb), rb)

    def columns(cx, cs):
        return pl.ds(pl.multiple_of((cx * S + cs) * kd, kd), kd)

    def held(i):
        if not relative:
            return rows(i)
        return rows(lax.rem(i // S + X - x, X) * S + lax.rem(i, S))

    def held_columns(d, cs):
        return columns(d if relative else col(d), cs)

    def col(d):
        return lax.rem(x + d, X)

    peers = [{"col": col(d)} for d in range(1, X)]
    peers += [{"row": lax.rem(r + d, R)} for d in range(1, R)]
    peers += [{"sub": lax.rem(s + d, S)} for d in range(1, S)]
    barrier = pltpu.get_barrier_semaphore()
    for peer in peers:
        pl.semaphore_signal(barrier, inc=1, device_id=peer, device_id_type=MESH)
    pl.semaphore_wait(barrier, len(peers))

    order = list(range(1, X)) + [0]
    steps = list(range(1, R)) + [0]
    pair = {}
    for d in order:
        for e in range(1, S):
            other = lax.rem(s + e, S)
            pair[d, e] = pltpu.make_async_remote_copy(
                p.at[:, held_columns(d, other)], from_sub.at[e - 1, d],
                a_s.at[e - 1, d], a_r.at[e - 1, d],
                device_id={"sub": other}, device_id_type=MESH)
            pair[d, e].start()
    cross = {}
    for d in order:
        for e in range(1, S):
            pair[d, e].wait_recv()
        for q in steps:
            here = rows(lax.rem(r + q, R))
            there = held(lax.rem(r + q, R))
            total = p[there, held_columns(d, s)]
            for e in range(1, S):
                total = total + from_sub[e - 1, d, there, :]
            acc[d, here, :] = total
            if d > 0:
                cross[d, q] = pltpu.make_async_remote_copy(
                    acc.at[d, here], from_col.at[d - 1, here],
                    b_s.at[d - 1, q], b_r.at[d - 1, q],
                    device_id={"col": col(d)}, device_id_type=MESH)
                cross[d, q].start()
    along = []
    for q in steps:
        i = lax.rem(r + q, R)
        here = rows(i)
        total = acc[0, here, :]
        for d in range(1, X):
            cross[d, q].wait_recv()
            total = total + from_col[d - 1, here, :]
        if q > 0:
            acc[0, here, :] = total
            copy = pltpu.make_async_remote_copy(
                acc.at[0, here], from_row.at[q - 1], c_s.at[q - 1], c_r.at[q - 1],
                device_id={"row": i}, device_id_type=MESH)
            copy.start()
            along.append(copy)
    for q in range(1, R):
        along[q - 1].wait_recv()
        total = total + from_row[q - 1]
    res[...] = total
    last = []
    for e in range(1, S):
        copy = pltpu.make_async_remote_copy(
            res, from_pair.at[e - 1], d_s.at[e - 1], d_r.at[e - 1],
            device_id={"sub": lax.rem(s + e, S)}, device_id_type=MESH)
        copy.start()
        last.append(copy)
    out[:, pl.ds(pl.multiple_of(s * kd, kd), kd)] = total
    for e in range(1, S):
        last[e - 1].wait_recv()
        out[:, pl.ds(pl.multiple_of(lax.rem(s - e + S, S) * kd, kd), kd)] = from_pair[e - 1]
    for copy in list(pair.values()) + list(cross.values()) + along + last:
        copy.wait_send()


def project(partial, R, X, S, relative):
    K = partial.shape[0]
    rb, kd = K // R, K // (X * S)
    dma = pltpu.SemaphoreType.DMA
    f32 = jnp.float32
    return pl.pallas_call(
        functools.partial(project_kernel, R, X, S, relative),
        out_shape=jax.ShapeDtypeStruct((rb, S * kd), f32),
        in_specs=[pl.BlockSpec(memory_space=pltpu.VMEM)],
        out_specs=pl.BlockSpec(memory_space=pltpu.VMEM),
        scratch_shapes=[
            pltpu.VMEM((X, K, kd), f32),
            pltpu.VMEM((S - 1, X, K, kd), f32),
            pltpu.VMEM((X - 1, K, kd), f32),
            pltpu.VMEM((R - 1, rb, kd), f32),
            pltpu.VMEM((rb, kd), f32),
            pltpu.VMEM((S - 1, rb, kd), f32),
            dma((S - 1, X)), dma((S - 1, X)), dma((X - 1, R)), dma((X - 1, R)),
            dma((R - 1,)), dma((R - 1,)), dma((S - 1,)), dma((S - 1,)),
        ],
        compiler_params=pltpu.CompilerParams(collective_id=2, has_side_effects=True),
        cost_estimate=pl.CostEstimate(flops=0, bytes_accessed=60_000_000, transcendentals=0),
        name="project",
    )(partial)


def split(value):
    high = value.astype(jnp.bfloat16)
    return high, (value - high.astype(jnp.float32)).astype(jnp.bfloat16)


def dot3(a_high, a_low, b_high, b_low, contract):
    def one(a, b):
        return lax.dot_general(a, b, ((contract, (0,)), ((), ())),
                               preferred_element_type=jnp.float32)
    return one(a_high, b_high) + (one(a_high, b_low) + one(a_low, b_high))


def image_kernel(R, S, Q, v, a, vall, img, sbuf, ubuf, tbuf, abuf, ahi, alo, vhi, vlo, rhi, rlo,
                 lsem, asem, os, orr, xs, xr, fs, fr, hs, hr, ts, tr):
    z, x, s = lax.axis_index("row"), lax.axis_index("col"), lax.axis_index("sub")
    c = x * S + s
    m, kd = v.shape
    half = S * kd
    steps = m // abuf.shape[2]
    w = m // steps
    pw = w // Q
    first = jnp.where(x == 0, c, 0)
    last = jnp.where(x == 0, R - 1, c)
    chained = (z >= first) & (z <= last)
    diag = z == c
    pair = (z == x * S + 1) & (s == 0)
    relay = (z == x * S) & (s == 1 - x)
    adds = (x == 1) & chained
    weight = jnp.where(diag, 0.5, 1.0).astype(jnp.float32)
    other = 1 - s

    def rows(i, n):
        return pl.ds(pl.multiple_of(i * n, n), n)

    def block(hh, ss):
        return pl.ds(pl.multiple_of((hh * S + ss) * kd, kd), kd)

    barrier = pltpu.get_barrier_semaphore()
    pl.semaphore_signal(barrier, inc=1, device_id={"sub": other}, device_id_type=MESH)
    pl.semaphore_signal(barrier, inc=1, device_id={"col": 1 - x}, device_id_type=MESH)

    @pl.when(z > 0)
    def _():
        for t in range(S):
            pl.semaphore_signal(barrier, inc=1, device_id={"row": z - 1, "sub": t}, device_id_type=MESH)

    @pl.when(z < R - 1)
    def _():
        for t in range(S):
            pl.semaphore_signal(barrier, inc=1, device_id={"row": z + 1, "sub": t}, device_id_type=MESH)

    def load(i):
        return pltpu.make_async_copy(a.at[:, rows(i, w)], abuf.at[lax.rem(i, 2)], asem.at[lax.rem(i, 2)])

    def mate():
        return pltpu.make_async_remote_copy(
            v, vall.at[:, block(0, s)], os, orr, device_id={"sub": other}, device_id_type=MESH)

    def across(i):
        return pltpu.make_async_remote_copy(
            v.at[rows(i, w), :], vall.at[rows(i, w), block(1, s)], xs.at[i], xr.at[i],
            device_id={"col": 1 - x}, device_id_type=MESH)

    def share(i):
        here = vall.at[rows(i, w), block(1, s)]
        return pltpu.make_async_remote_copy(
            here, here, fs.at[i], fr.at[i], device_id={"sub": other}, device_id_type=MESH)

    def hand(i):
        return pltpu.make_async_remote_copy(
            vall.at[rows(i, w), pl.ds(half, half)], ubuf.at[rows(i, w), :], hs.at[i], hr.at[i],
            device_id={"row": z + 1, "sub": 0}, device_id_type=MESH)

    def origin(k):
        return pltpu.make_async_remote_copy(
            vall.at[rows(k, pw), pl.ds(0, half)], sbuf.at[rows(k, pw), :], ts.at[k], tr.at[k],
            device_id={"row": z + 1}, device_id_type=MESH)

    def onward(k):
        return pltpu.make_async_remote_copy(
            sbuf.at[rows(k, pw), :], sbuf.at[rows(k, pw), :], ts.at[k], tr.at[k],
            device_id={"row": z + 1}, device_id_type=MESH)

    own = pltpu.make_async_copy(v, vall.at[:, block(0, s)], lsem)
    own.start()
    load(0).start()
    img[...] = jnp.zeros_like(img)
    pl.semaphore_wait(barrier, 2 + S * ((z > 0).astype(jnp.int32) + (z < R - 1).astype(jnp.int32)))
    mate().start()

    def begin(i, carry):
        across(i).start()
        return carry

    lax.fori_loop(0, steps, begin, 0)
    own.wait()
    mate().wait_recv()
    source = (x == 0) & diag

    @pl.when(source)
    def _():
        def send(k, carry):
            origin(k).start()
            return carry
        lax.fori_loop(0, steps * Q, send, 0)

    @pl.when(adds)
    def _():
        def prepare(i, carry):
            high, low = split(vall[rows(i, w), pl.ds(0, half)])
            vhi[rows(i, w), :] = high
            vlo[rows(i, w), :] = low
            return carry
        lax.fori_loop(0, steps, prepare, 0)

    def multiply(columns):
        def tile(t, carry):
            here = rows(t, w)
            img[here, columns] += dot3(ahi[here, :], alo[here, :], rhi[...], rlo[...], (1,))
            return carry
        lax.fori_loop(0, steps, tile, 0)

    def step(i, carry):
        load(i).wait()

        @pl.when(i < steps - 1)
        def _():
            load(i + 1).start()

        def cut(t, carry):
            high, low = split(abuf[lax.rem(i, 2), rows(t, w), :])
            ahi[rows(t, w), :] = high
            alo[rows(t, w), :] = low
            return carry
        lax.fori_loop(0, steps, cut, 0)

        @pl.when(adds)
        def _():
            tbuf[...] = weight * dot3(ahi[...], alo[...], vhi[...], vlo[...], (0,))

        across(i).wait_recv()
        share(i).start()

        def piece(p, carry):
            k = i * Q + p

            @pl.when(chained & (z > first))
            def _():
                onward(k).wait_recv()

            @pl.when(adds & (z == first))
            def _():
                sbuf[rows(k, pw), :] = tbuf[rows(p, pw), :]

            @pl.when(adds & (z > first))
            def _():
                sbuf[rows(k, pw), :] += tbuf[rows(p, pw), :]

            @pl.when(chained & (z < last) & jnp.logical_not(source))
            def _():
                onward(k).start()
            return carry
        lax.fori_loop(0, Q, piece, 0)

        share(i).wait_recv()

        @pl.when(relay)
        def _():
            hand(i).start()

        @pl.when((x == 0) & chained)
        def _():
            @pl.when(diag)
            def _():
                high, low = split(0.5 * vall[rows(i, w), pl.ds(0, half)])
                rhi[...] = high
                rlo[...] = low

            @pl.when(jnp.logical_not(diag))
            def _():
                high, low = split(sbuf[rows(i, w), :])
                rhi[...] = high
                rlo[...] = low
            multiply(pl.ds(0, half))

        @pl.when(diag | pair)
        def _():
            @pl.when(diag)
            def _():
                high, low = split(0.5 * vall[rows(i, w), pl.ds(half, half)])
                rhi[...] = high
                rlo[...] = low

            @pl.when(pair)
            def _():
                hand(i).wait_recv()
                high, low = split(ubuf[rows(i, w), :])
                rhi[...] = high
                rlo[...] = low
            multiply(pl.ds(half, half))
        return carry

    lax.fori_loop(0, steps, step, 0)

    @pl.when((x == 1) & diag)
    def _():
        def place(t, carry):
            img[rows(t, w), pl.ds(0, half)] = sbuf[rows(t, w), :]
            return carry
        lax.fori_loop(0, steps, place, 0)

    mate().wait_send()

    def drain(i, carry):
        across(i).wait_send()
        share(i).wait_send()

        @pl.when(relay)
        def _():
            hand(i).wait_send()
        return carry

    lax.fori_loop(0, steps, drain, 0)

    def sent(k, carry):
        @pl.when(source)
        def _():
            origin(k).wait_send()

        @pl.when(chained & (z < last) & jnp.logical_not(source))
        def _():
            onward(k).wait_send()
        return carry

    lax.fori_loop(0, steps * Q, sent, 0)


def image(v, a, R, S):
    m, kd = v.shape
    w = kd
    steps = m // w
    Q = 4
    half = S * kd
    dma = pltpu.SemaphoreType.DMA
    f32, bf16 = jnp.float32, jnp.bfloat16
    return pl.pallas_call(
        functools.partial(image_kernel, R, S, Q),
        out_shape=(jax.ShapeDtypeStruct((m, 2 * half), f32), jax.ShapeDtypeStruct((m, 2 * half), f32)),
        in_specs=[pl.BlockSpec(memory_space=pltpu.VMEM), pl.BlockSpec(memory_space=pl.ANY)],
        out_specs=(pl.BlockSpec(memory_space=pltpu.VMEM), pl.BlockSpec(memory_space=pltpu.VMEM)),
        scratch_shapes=[
            pltpu.VMEM((m, half), f32), pltpu.VMEM((m, half), f32), pltpu.VMEM((w, half), f32),
            pltpu.VMEM((2, m, w), f32), pltpu.VMEM((m, w), bf16), pltpu.VMEM((m, w), bf16),
            pltpu.VMEM((m, half), bf16), pltpu.VMEM((m, half), bf16),
            pltpu.VMEM((w, half), bf16), pltpu.VMEM((w, half), bf16),
            dma, dma((2,)), dma, dma, dma((steps,)), dma((steps,)), dma((steps,)), dma((steps,)),
            dma((steps,)), dma((steps,)), dma((steps * Q,)), dma((steps * Q,)),
        ],
        compiler_params=pltpu.CompilerParams(
            collective_id=3, has_side_effects=True, vmem_limit_bytes=60_000_000),
        cost_estimate=pl.CostEstimate(flops=0, bytes_accessed=100_000_000, transcendentals=0),
        name="image",
    )(v, a)


def partial_general(matrix, basis_vectors):
    R = lax.axis_size("row")
    S = lax.axis_size("sub")
    C = lax.axis_size("col") * S
    m, kd = basis_vectors.shape
    K = kd * C
    n = matrix.shape[1]
    per = n // m
    piece = m // R
    own, spread = gather(basis_vectors, R, C // S, S)
    width = K // CHUNKS
    images = []
    for c in range(CHUNKS):
        part = lax.dot_general(
            matrix,
            own[:, c * width : (c + 1) * width],
            (((0,), (0,)), ((), ())),
            precision=lax.Precision.HIGH,
            preferred_element_type=jnp.float32,
        )
        if c == 0:
            part, spread = lax.optimization_barrier((part, spread))
        part = part.reshape(per, R, piece, width).transpose(1, 0, 2, 3).reshape(R * per * piece, width)
        images.append(lax.psum_scatter(part, "row", scatter_dimension=0, tiled=True))
    mine = regroup(spread, C // S, S).reshape(per * piece, K)
    return jnp.concatenate(
        [
            lax.dot_general(
                mine,
                image,
                (((0,), (0,)), ((), ())),
                precision=lax.Precision.HIGH,
                preferred_element_type=jnp.float32,
            )
            for image in images
        ],
        axis=1,
    )


def partial_halves(matrix, basis_vectors, R, S):
    vectors, images = image(basis_vectors, matrix, R, S)
    part = lax.dot_general(
        vectors, images, (((0,), (0,)), ((), ())),
        precision=lax.Precision.HIGH, preferred_element_type=jnp.float32)
    return part + part.T


def shards(matrix, basis_vectors, split_size):
    R = lax.axis_size("row")
    X = lax.axis_size("col")
    S = lax.axis_size("sub")
    m, n = matrix.shape
    halves = m == n and R == X * S and X == 2 and S == 2
    if halves:
        partial_proj = partial_halves(matrix, basis_vectors, R, S)
    else:
        partial_proj = partial_general(matrix, basis_vectors)
    child_block = project(partial_proj, R, X, S, halves)
    row_ids = (
        jnp.arange(child_block.shape[0], dtype=jnp.int32)
        + lax.axis_index("row") * child_block.shape[0]
    )
    col_ids = (
        jnp.arange(child_block.shape[1], dtype=jnp.int32)
        + lax.axis_index("col") * child_block.shape[1]
    )
    leading = split_size[0]
    row_first = row_ids < leading
    col_first = col_ids < leading
    mask_one = row_first[:, None] & col_first[None, :]
    mask_two = jnp.logical_not(row_first)[:, None] & jnp.logical_not(col_first)[None, :]
    selected = jnp.where(lax.axis_index("sub") == 0, mask_one, mask_two)
    return jnp.where(selected, child_block, jnp.zeros((), jnp.float32))[None]


def solution(mesh):
    placed = (
        P(("groups", "row"), ("col", "sub")),
        P(("groups", "row"), ("col", "sub")),
        P("groups"),
    )
    return jax.shard_map(
        shards,
        mesh=mesh,
        in_specs=placed,
        out_specs=P("sub", ("groups", "row"), "col"),
        check_vma=False,
    )
```

```python
import functools

import jax
import jax.numpy as jnp
from jax import lax
from jax.experimental import pallas as pl
from jax.experimental.pallas import tpu as pltpu
from jax.sharding import PartitionSpec as P

MESH = pl.DeviceIdType.MESH
CHUNKS = 1


def gather_kernel(R, X, S, v, own, spread, lsem, xs, xr, zs, zr, ps, pr, fs, fr):
    r, x, s = lax.axis_index("row"), lax.axis_index("col"), lax.axis_index("sub")
    m, kd = v.shape
    piece = m // R

    def columns(cx, cs):
        return pl.ds(pl.multiple_of((cx * S + cs) * kd, kd), kd)

    peers = [{"col": lax.rem(x + d, X)} for d in range(1, X)]
    peers += [{"row": lax.rem(r + d, R)} for d in range(1, R)]
    peers += [{"sub": lax.rem(s + d, S)} for d in range(1, S)]
    barrier = pltpu.get_barrier_semaphore()
    for peer in peers:
        pl.semaphore_signal(barrier, inc=1, device_id=peer, device_id_type=MESH)
    pl.semaphore_wait(barrier, len(peers))

    mine = own.at[:, columns(x, s)]
    across, spreads, partner, forward = [], [], [], []
    for d in range(1, X):
        across.append(pltpu.make_async_remote_copy(
            v, mine, xs.at[d - 1], xr.at[d - 1],
            device_id={"col": lax.rem(x + d, X)}, device_id_type=MESH))
    for d in range(1, R):
        i = lax.rem(r + d, R)
        spreads.append(pltpu.make_async_remote_copy(
            v.at[pl.ds(pl.multiple_of(i * piece, piece), piece), :], spread.at[r],
            zs.at[d - 1], zr.at[d - 1],
            device_id={"row": i}, device_id_type=MESH))
    for d in range(1, S):
        partner.append(pltpu.make_async_remote_copy(
            v, mine, ps.at[d - 1], pr.at[d - 1],
            device_id={"sub": lax.rem(s + d, S)}, device_id_type=MESH))
    for copy in across + spreads + partner:
        copy.start()
    local = [
        pltpu.make_async_copy(v, mine, lsem.at[0]),
        pltpu.make_async_copy(
            v.at[pl.ds(pl.multiple_of(r * piece, piece), piece), :], spread.at[r], lsem.at[1]),
    ]
    for copy in local:
        copy.start()
    for d in range(1, X):
        across[d - 1].wait_recv()
        block = own.at[:, columns(lax.rem(x - d + X, X), s)]
        for e in range(1, S):
            copy = pltpu.make_async_remote_copy(
                block, block, fs.at[d - 1, e - 1], fr.at[d - 1, e - 1],
                device_id={"sub": lax.rem(s + e, S)}, device_id_type=MESH)
            copy.start()
            forward.append(copy)
    for copy in across:
        copy.wait_send()
    for copy in spreads + partner + forward:
        copy.wait()
    for copy in local:
        copy.wait()


def gather(v, R, X, S):
    m, kd = v.shape
    dma = pltpu.SemaphoreType.DMA
    return pl.pallas_call(
        functools.partial(gather_kernel, R, X, S),
        out_shape=(
            jax.ShapeDtypeStruct((m, kd * X * S), v.dtype),
            jax.ShapeDtypeStruct((R, m // R, kd), v.dtype),
        ),
        in_specs=[pl.BlockSpec(memory_space=pltpu.VMEM)],
        out_specs=(pl.BlockSpec(memory_space=pl.ANY), pl.BlockSpec(memory_space=pl.ANY)),
        scratch_shapes=[
            dma((2,)), dma((X - 1,)), dma((X - 1,)), dma((R - 1,)), dma((R - 1,)),
            dma((S - 1,)), dma((S - 1,)), dma((X - 1, S - 1)), dma((X - 1, S - 1)),
        ],
        compiler_params=pltpu.CompilerParams(collective_id=0, has_side_effects=True),
        cost_estimate=pl.CostEstimate(flops=0, bytes_accessed=100_000_000, transcendentals=0),
        name="gather",
    )(v)


def regroup_kernel(X, S, spread, mine, lsem, ss, rs):
    x, s = lax.axis_index("col"), lax.axis_index("sub")
    C = X * S
    k = x * S + s
    R, piece, kd = spread.shape
    per = R // C
    barrier = pltpu.get_barrier_semaphore()
    dests = [lax.rem(k + e, C) for e in range(C)]
    for j in dests[1:]:
        pl.semaphore_signal(
            barrier, inc=1, device_id={"col": j // S, "sub": lax.rem(j, S)}, device_id_type=MESH)
    pl.semaphore_wait(barrier, C - 1)
    target = mine.at[:, :, pl.ds(pl.multiple_of(k * kd, kd), kd)]
    copies = []
    for e in range(1, C):
        j = dests[e]
        copies.append(pltpu.make_async_remote_copy(
            spread.at[pl.ds(j * per, per)], target, ss.at[e - 1], rs.at[e - 1],
            device_id={"col": j // S, "sub": lax.rem(j, S)}, device_id_type=MESH))
    copies.append(pltpu.make_async_copy(spread.at[pl.ds(k * per, per)], target, lsem))
    for copy in copies:
        copy.start()
    for copy in copies:
        copy.wait()


def regroup(spread, X, S):
    R, piece, kd = spread.shape
    C = X * S
    dma = pltpu.SemaphoreType.DMA
    return pl.pallas_call(
        functools.partial(regroup_kernel, X, S),
        out_shape=jax.ShapeDtypeStruct((R // C, piece, kd * C), spread.dtype),
        in_specs=[pl.BlockSpec(memory_space=pltpu.VMEM)],
        out_specs=pl.BlockSpec(memory_space=pl.ANY),
        scratch_shapes=[dma, dma((C - 1,)), dma((C - 1,))],
        compiler_params=pltpu.CompilerParams(collective_id=1, has_side_effects=True),
        cost_estimate=pl.CostEstimate(flops=0, bytes_accessed=60_000_000, transcendentals=0),
        name="regroup",
    )(spread)


def project_kernel(R, X, S, relative, p, out, acc, from_sub, from_col, from_row, res, from_pair,
                   a_s, a_r, b_s, b_r, c_s, c_r, d_s, d_r):
    r, x, s = lax.axis_index("row"), lax.axis_index("col"), lax.axis_index("sub")
    K = p.shape[0]
    rb, kd = K // R, K // (X * S)

    def rows(i):
        return pl.ds(pl.multiple_of(i * rb, rb), rb)

    def columns(cx, cs):
        return pl.ds(pl.multiple_of((cx * S + cs) * kd, kd), kd)

    def held(i):
        if not relative:
            return rows(i)
        return rows(lax.rem(i // S + X - x, X) * S + lax.rem(i, S))

    def held_columns(d, cs):
        return columns(d if relative else col(d), cs)

    def col(d):
        return lax.rem(x + d, X)

    peers = [{"col": col(d)} for d in range(1, X)]
    peers += [{"row": lax.rem(r + d, R)} for d in range(1, R)]
    peers += [{"sub": lax.rem(s + d, S)} for d in range(1, S)]
    barrier = pltpu.get_barrier_semaphore()
    for peer in peers:
        pl.semaphore_signal(barrier, inc=1, device_id=peer, device_id_type=MESH)
    pl.semaphore_wait(barrier, len(peers))

    order = list(range(1, X)) + [0]
    steps = list(range(1, R)) + [0]
    pair = {}
    for d in order:
        for e in range(1, S):
            other = lax.rem(s + e, S)
            pair[d, e] = pltpu.make_async_remote_copy(
                p.at[:, held_columns(d, other)], from_sub.at[e - 1, d],
                a_s.at[e - 1, d], a_r.at[e - 1, d],
                device_id={"sub": other}, device_id_type=MESH)
            pair[d, e].start()
    cross = {}
    for d in order:
        for e in range(1, S):
            pair[d, e].wait_recv()
        for q in steps:
            here = rows(lax.rem(r + q, R))
            there = held(lax.rem(r + q, R))
            total = p[there, held_columns(d, s)]
            for e in range(1, S):
                total = total + from_sub[e - 1, d, there, :]
            acc[d, here, :] = total
            if d > 0:
                cross[d, q] = pltpu.make_async_remote_copy(
                    acc.at[d, here], from_col.at[d - 1, here],
                    b_s.at[d - 1, q], b_r.at[d - 1, q],
                    device_id={"col": col(d)}, device_id_type=MESH)
                cross[d, q].start()
    along = []
    for q in steps:
        i = lax.rem(r + q, R)
        here = rows(i)
        total = acc[0, here, :]
        for d in range(1, X):
            cross[d, q].wait_recv()
            total = total + from_col[d - 1, here, :]
        if q > 0:
            acc[0, here, :] = total
            copy = pltpu.make_async_remote_copy(
                acc.at[0, here], from_row.at[q - 1], c_s.at[q - 1], c_r.at[q - 1],
                device_id={"row": i}, device_id_type=MESH)
            copy.start()
            along.append(copy)
    for q in range(1, R):
        along[q - 1].wait_recv()
        total = total + from_row[q - 1]
    res[...] = total
    last = []
    for e in range(1, S):
        copy = pltpu.make_async_remote_copy(
            res, from_pair.at[e - 1], d_s.at[e - 1], d_r.at[e - 1],
            device_id={"sub": lax.rem(s + e, S)}, device_id_type=MESH)
        copy.start()
        last.append(copy)
    out[:, pl.ds(pl.multiple_of(s * kd, kd), kd)] = total
    for e in range(1, S):
        last[e - 1].wait_recv()
        out[:, pl.ds(pl.multiple_of(lax.rem(s - e + S, S) * kd, kd), kd)] = from_pair[e - 1]
    for copy in list(pair.values()) + list(cross.values()) + along + last:
        copy.wait_send()


def project(partial, R, X, S, relative):
    K = partial.shape[0]
    rb, kd = K // R, K // (X * S)
    dma = pltpu.SemaphoreType.DMA
    f32 = jnp.float32
    return pl.pallas_call(
        functools.partial(project_kernel, R, X, S, relative),
        out_shape=jax.ShapeDtypeStruct((rb, S * kd), f32),
        in_specs=[pl.BlockSpec(memory_space=pltpu.VMEM)],
        out_specs=pl.BlockSpec(memory_space=pltpu.VMEM),
        scratch_shapes=[
            pltpu.VMEM((X, K, kd), f32),
            pltpu.VMEM((S - 1, X, K, kd), f32),
            pltpu.VMEM((X - 1, K, kd), f32),
            pltpu.VMEM((R - 1, rb, kd), f32),
            pltpu.VMEM((rb, kd), f32),
            pltpu.VMEM((S - 1, rb, kd), f32),
            dma((S - 1, X)), dma((S - 1, X)), dma((X - 1, R)), dma((X - 1, R)),
            dma((R - 1,)), dma((R - 1,)), dma((S - 1,)), dma((S - 1,)),
        ],
        compiler_params=pltpu.CompilerParams(collective_id=2, has_side_effects=True),
        cost_estimate=pl.CostEstimate(flops=0, bytes_accessed=60_000_000, transcendentals=0),
        name="project",
    )(partial)


def split(value):
    high = value.astype(jnp.bfloat16)
    return high, (value - high.astype(jnp.float32)).astype(jnp.bfloat16)


def dot3(a_high, a_low, b_high, b_low, contract):
    def one(a, b):
        return lax.dot_general(a, b, ((contract, (0,)), ((), ())),
                               preferred_element_type=jnp.float32)
    return one(a_high, b_high) + (one(a_high, b_low) + one(a_low, b_high))


def image_kernel(R, S, Q, v, a, out, vall, img, ybuf, sbuf, ubuf, tbuf, abuf, ahi, alo, vhi, vlo,
                 ihi, ilo, rhi, rlo, lsem, asem, os, orr, xs, xr, fs, fr, hs, hr, ts, tr):
    z, x, s = lax.axis_index("row"), lax.axis_index("col"), lax.axis_index("sub")
    c = x * S + s
    m, kd = v.shape
    half = S * kd
    steps = m // abuf.shape[2]
    w = m // steps
    pw = w // Q
    first = jnp.where(x == 0, c, 0)
    last = jnp.where(x == 0, R - 1, c)
    chained = (z >= first) & (z <= last)
    diag = z == c
    pair = (z == x * S + 1) & (s == 0)
    relay = (z == x * S) & (s == 1 - x)
    adds = (x == 1) & chained
    weight = jnp.where(diag, 0.5, 1.0).astype(jnp.float32)
    other = 1 - s

    def rows(i, n):
        return pl.ds(pl.multiple_of(i * n, n), n)

    def block(hh, ss):
        return pl.ds(pl.multiple_of((hh * S + ss) * kd, kd), kd)

    barrier = pltpu.get_barrier_semaphore()
    pl.semaphore_signal(barrier, inc=1, device_id={"sub": other}, device_id_type=MESH)
    pl.semaphore_signal(barrier, inc=1, device_id={"col": 1 - x}, device_id_type=MESH)

    @pl.when(z > 0)
    def _():
        for t in range(S):
            pl.semaphore_signal(barrier, inc=1, device_id={"row": z - 1, "sub": t}, device_id_type=MESH)

    @pl.when(z < R - 1)
    def _():
        for t in range(S):
            pl.semaphore_signal(barrier, inc=1, device_id={"row": z + 1, "sub": t}, device_id_type=MESH)

    def load(i):
        return pltpu.make_async_copy(a.at[:, rows(i, w)], abuf.at[lax.rem(i, 2)], asem.at[lax.rem(i, 2)])

    def mate():
        return pltpu.make_async_remote_copy(
            v, vall.at[:, block(0, s)], os, orr, device_id={"sub": other}, device_id_type=MESH)

    def across(i):
        return pltpu.make_async_remote_copy(
            v.at[rows(i, w), :], vall.at[rows(i, w), block(1, s)], xs.at[i], xr.at[i],
            device_id={"col": 1 - x}, device_id_type=MESH)

    def share(i):
        here = vall.at[rows(i, w), block(1, s)]
        return pltpu.make_async_remote_copy(
            here, here, fs.at[i], fr.at[i], device_id={"sub": other}, device_id_type=MESH)

    def hand(i):
        return pltpu.make_async_remote_copy(
            vall.at[rows(i, w), pl.ds(half, half)], ubuf.at[rows(i, w), :], hs.at[i], hr.at[i],
            device_id={"row": z + 1, "sub": 0}, device_id_type=MESH)

    def origin(k):
        return pltpu.make_async_remote_copy(
            vall.at[rows(k, pw), pl.ds(0, half)], sbuf.at[rows(k, pw), :], ts.at[k], tr.at[k],
            device_id={"row": z + 1}, device_id_type=MESH)

    def onward(k):
        return pltpu.make_async_remote_copy(
            sbuf.at[rows(k, pw), :], sbuf.at[rows(k, pw), :], ts.at[k], tr.at[k],
            device_id={"row": z + 1}, device_id_type=MESH)

    own = pltpu.make_async_copy(v, vall.at[:, block(0, s)], lsem)
    own.start()
    load(0).start()
    img[...] = jnp.zeros_like(img)
    pl.semaphore_wait(barrier, 2 + S * ((z > 0).astype(jnp.int32) + (z < R - 1).astype(jnp.int32)))
    mate().start()

    def begin(i, carry):
        across(i).start()
        return carry

    lax.fori_loop(0, steps, begin, 0)
    own.wait()
    mate().wait_recv()
    source = (x == 0) & diag

    @pl.when(source)
    def _():
        def send(k, carry):
            origin(k).start()
            return carry
        lax.fori_loop(0, steps * Q, send, 0)

    def prepare(i, hh):
        here, columns = rows(i, w), pl.ds(hh * half, half)
        high, low = split(vall[here, columns])
        vhi[here, columns] = high
        vlo[here, columns] = low

    def prepare_own(i, carry):
        prepare(i, 0)
        return carry

    lax.fori_loop(0, steps, prepare_own, 0)

    def multiply(columns):
        def tile(t, carry):
            here = rows(t, w)
            img[here, columns] += dot3(ahi[here, :], alo[here, :], rhi[...], rlo[...], (1,))
            return carry
        lax.fori_loop(0, steps, tile, 0)

    def step(i, carry):
        load(i).wait()

        @pl.when(i < steps - 1)
        def _():
            load(i + 1).start()

        def cut(t, carry):
            high, low = split(abuf[lax.rem(i, 2), rows(t, w), :])
            ahi[rows(t, w), :] = high
            alo[rows(t, w), :] = low
            return carry
        lax.fori_loop(0, steps, cut, 0)

        @pl.when(adds)
        def _():
            tbuf[...] = weight * dot3(ahi[...], alo[...], vhi[:, :half], vlo[:, :half], (0,))

        across(i).wait_recv()
        share(i).start()

        def piece(p, carry):
            k = i * Q + p

            @pl.when(chained & (z > first))
            def _():
                onward(k).wait_recv()

            @pl.when(adds & (z == first))
            def _():
                sbuf[rows(k, pw), :] = tbuf[rows(p, pw), :]

            @pl.when(adds & (z > first))
            def _():
                sbuf[rows(k, pw), :] += tbuf[rows(p, pw), :]

            @pl.when(chained & (z < last) & jnp.logical_not(source))
            def _():
                onward(k).start()
            return carry
        lax.fori_loop(0, Q, piece, 0)

        share(i).wait_recv()
        prepare(i, 1)

        @pl.when(relay)
        def _():
            hand(i).start()

        @pl.when((x == 0) & chained)
        def _():
            @pl.when(diag)
            def _():
                high, low = split(0.5 * vall[rows(i, w), pl.ds(0, half)])
                rhi[...] = high
                rlo[...] = low

            @pl.when(jnp.logical_not(diag))
            def _():
                high, low = split(sbuf[rows(i, w), :])
                rhi[...] = high
                rlo[...] = low
            multiply(pl.ds(0, half))

        @pl.when(diag | pair)
        def _():
            @pl.when(diag)
            def _():
                high, low = split(0.5 * vall[rows(i, w), pl.ds(half, half)])
                rhi[...] = high
                rlo[...] = low

            @pl.when(pair)
            def _():
                hand(i).wait_recv()
                high, low = split(ubuf[rows(i, w), :])
                rhi[...] = high
                rlo[...] = low
            multiply(pl.ds(half, half))
        return carry

    lax.fori_loop(0, steps, step, 0)

    @pl.when((x == 1) & diag)
    def _():
        def place(t, carry):
            img[rows(t, w), pl.ds(0, half)] = sbuf[rows(t, w), :]
            return carry
        lax.fori_loop(0, steps, place, 0)

    def fold(hh, present):
        columns = pl.ds(hh * half, half)

        @pl.when(present)
        def _():
            def halve(t, carry):
                high, low = split(img[rows(t, w), columns])
                ihi[rows(t, w), :] = high
                ilo[rows(t, w), :] = low
                return carry
            lax.fori_loop(0, steps, halve, 0)
            for b in range(2 * S):
                part = slice(b * kd, (b + 1) * kd)
                ybuf[part, columns] = dot3(vhi[:, part], vlo[:, part], ihi[...], ilo[...], (0,))

        @pl.when(jnp.logical_not(present))
        def _():
            ybuf[:, columns] = jnp.zeros((2 * half, half), jnp.float32)

    fold(1, diag | pair)
    fold(0, chained & ((x == 0) | diag))
    for b in range(2 * S):
        mine = slice(b * kd, (b + 1) * kd)
        for e in range(b, 2 * S):
            theirs = slice(e * kd, (e + 1) * kd)
            total = ybuf[mine, theirs] + ybuf[theirs, mine].T
            out[mine, theirs] = total
            if e > b:
                out[theirs, mine] = total.T

    mate().wait_send()

    def drain(i, carry):
        across(i).wait_send()
        share(i).wait_send()

        @pl.when(relay)
        def _():
            hand(i).wait_send()
        return carry

    lax.fori_loop(0, steps, drain, 0)

    def sent(k, carry):
        @pl.when(source)
        def _():
            origin(k).wait_send()

        @pl.when(chained & (z < last) & jnp.logical_not(source))
        def _():
            onward(k).wait_send()
        return carry

    lax.fori_loop(0, steps * Q, sent, 0)


def image(v, a, R, S):
    m, kd = v.shape
    w = kd
    steps = m // w
    Q = 4
    half = S * kd
    dma = pltpu.SemaphoreType.DMA
    f32, bf16 = jnp.float32, jnp.bfloat16
    return pl.pallas_call(
        functools.partial(image_kernel, R, S, Q),
        out_shape=jax.ShapeDtypeStruct((2 * half, 2 * half), f32),
        in_specs=[pl.BlockSpec(memory_space=pltpu.VMEM), pl.BlockSpec(memory_space=pl.ANY)],
        out_specs=pl.BlockSpec(memory_space=pltpu.VMEM),
        scratch_shapes=[
            pltpu.VMEM((m, 2 * half), f32), pltpu.VMEM((m, 2 * half), f32),
            pltpu.VMEM((2 * half, 2 * half), f32),
            pltpu.VMEM((m, half), f32), pltpu.VMEM((m, half), f32), pltpu.VMEM((w, half), f32),
            pltpu.VMEM((2, m, w), f32), pltpu.VMEM((m, w), bf16), pltpu.VMEM((m, w), bf16),
            pltpu.VMEM((m, 2 * half), bf16), pltpu.VMEM((m, 2 * half), bf16),
            pltpu.VMEM((m, half), bf16), pltpu.VMEM((m, half), bf16),
            pltpu.VMEM((w, half), bf16), pltpu.VMEM((w, half), bf16),
            dma, dma((2,)), dma, dma, dma((steps,)), dma((steps,)), dma((steps,)), dma((steps,)),
            dma((steps,)), dma((steps,)), dma((steps * Q,)), dma((steps * Q,)),
        ],
        compiler_params=pltpu.CompilerParams(
            collective_id=3, has_side_effects=True, vmem_limit_bytes=60_000_000),
        cost_estimate=pl.CostEstimate(flops=0, bytes_accessed=100_000_000, transcendentals=0),
        name="image",
    )(v, a)


def partial_general(matrix, basis_vectors):
    R = lax.axis_size("row")
    S = lax.axis_size("sub")
    C = lax.axis_size("col") * S
    m, kd = basis_vectors.shape
    K = kd * C
    n = matrix.shape[1]
    per = n // m
    piece = m // R
    own, spread = gather(basis_vectors, R, C // S, S)
    width = K // CHUNKS
    images = []
    for c in range(CHUNKS):
        part = lax.dot_general(
            matrix,
            own[:, c * width : (c + 1) * width],
            (((0,), (0,)), ((), ())),
            precision=lax.Precision.HIGH,
            preferred_element_type=jnp.float32,
        )
        if c == 0:
            part, spread = lax.optimization_barrier((part, spread))
        part = part.reshape(per, R, piece, width).transpose(1, 0, 2, 3).reshape(R * per * piece, width)
        images.append(lax.psum_scatter(part, "row", scatter_dimension=0, tiled=True))
    mine = regroup(spread, C // S, S).reshape(per * piece, K)
    return jnp.concatenate(
        [
            lax.dot_general(
                mine,
                image,
                (((0,), (0,)), ((), ())),
                precision=lax.Precision.HIGH,
                preferred_element_type=jnp.float32,
            )
            for image in images
        ],
        axis=1,
    )


def shards(matrix, basis_vectors, split_size):
    R = lax.axis_size("row")
    X = lax.axis_size("col")
    S = lax.axis_size("sub")
    m, n = matrix.shape
    halves = m == n and R == X * S and X == 2 and S == 2
    if halves:
        partial_proj = image(basis_vectors, matrix, R, S)
    else:
        partial_proj = partial_general(matrix, basis_vectors)
    child_block = project(partial_proj, R, X, S, halves)
    row_ids = (
        jnp.arange(child_block.shape[0], dtype=jnp.int32)
        + lax.axis_index("row") * child_block.shape[0]
    )
    col_ids = (
        jnp.arange(child_block.shape[1], dtype=jnp.int32)
        + lax.axis_index("col") * child_block.shape[1]
    )
    leading = split_size[0]
    row_first = row_ids < leading
    col_first = col_ids < leading
    mask_one = row_first[:, None] & col_first[None, :]
    mask_two = jnp.logical_not(row_first)[:, None] & jnp.logical_not(col_first)[None, :]
    selected = jnp.where(lax.axis_index("sub") == 0, mask_one, mask_two)
    return jnp.where(selected, child_block, jnp.zeros((), jnp.float32))[None]


def solution(mesh):
    placed = (
        P(("groups", "row"), ("col", "sub")),
        P(("groups", "row"), ("col", "sub")),
        P("groups"),
    )
    return jax.shard_map(
        shards,
        mesh=mesh,
        in_specs=placed,
        out_specs=P("sub", ("groups", "row"), "col"),
        check_vma=False,
    )
```

```python
import functools

import jax
import jax.numpy as jnp
from jax import lax
from jax.experimental import pallas as pl
from jax.experimental.pallas import tpu as pltpu
from jax.sharding import PartitionSpec as P

MESH = pl.DeviceIdType.MESH
CHUNKS = 1


def gather_kernel(R, X, S, v, own, spread, lsem, xs, xr, zs, zr, ps, pr, fs, fr):
    r, x, s = lax.axis_index("row"), lax.axis_index("col"), lax.axis_index("sub")
    m, kd = v.shape
    piece = m // R

    def columns(cx, cs):
        return pl.ds(pl.multiple_of((cx * S + cs) * kd, kd), kd)

    peers = [{"col": lax.rem(x + d, X)} for d in range(1, X)]
    peers += [{"row": lax.rem(r + d, R)} for d in range(1, R)]
    peers += [{"sub": lax.rem(s + d, S)} for d in range(1, S)]
    barrier = pltpu.get_barrier_semaphore()
    for peer in peers:
        pl.semaphore_signal(barrier, inc=1, device_id=peer, device_id_type=MESH)
    pl.semaphore_wait(barrier, len(peers))

    mine = own.at[:, columns(x, s)]
    across, spreads, partner, forward = [], [], [], []
    for d in range(1, X):
        across.append(pltpu.make_async_remote_copy(
            v, mine, xs.at[d - 1], xr.at[d - 1],
            device_id={"col": lax.rem(x + d, X)}, device_id_type=MESH))
    for d in range(1, R):
        i = lax.rem(r + d, R)
        spreads.append(pltpu.make_async_remote_copy(
            v.at[pl.ds(pl.multiple_of(i * piece, piece), piece), :], spread.at[r],
            zs.at[d - 1], zr.at[d - 1],
            device_id={"row": i}, device_id_type=MESH))
    for d in range(1, S):
        partner.append(pltpu.make_async_remote_copy(
            v, mine, ps.at[d - 1], pr.at[d - 1],
            device_id={"sub": lax.rem(s + d, S)}, device_id_type=MESH))
    for copy in across + spreads + partner:
        copy.start()
    local = [
        pltpu.make_async_copy(v, mine, lsem.at[0]),
        pltpu.make_async_copy(
            v.at[pl.ds(pl.multiple_of(r * piece, piece), piece), :], spread.at[r], lsem.at[1]),
    ]
    for copy in local:
        copy.start()
    for d in range(1, X):
        across[d - 1].wait_recv()
        block = own.at[:, columns(lax.rem(x - d + X, X), s)]
        for e in range(1, S):
            copy = pltpu.make_async_remote_copy(
                block, block, fs.at[d - 1, e - 1], fr.at[d - 1, e - 1],
                device_id={"sub": lax.rem(s + e, S)}, device_id_type=MESH)
            copy.start()
            forward.append(copy)
    for copy in across:
        copy.wait_send()
    for copy in spreads + partner + forward:
        copy.wait()
    for copy in local:
        copy.wait()


def gather(v, R, X, S):
    m, kd = v.shape
    dma = pltpu.SemaphoreType.DMA
    return pl.pallas_call(
        functools.partial(gather_kernel, R, X, S),
        out_shape=(
            jax.ShapeDtypeStruct((m, kd * X * S), v.dtype),
            jax.ShapeDtypeStruct((R, m // R, kd), v.dtype),
        ),
        in_specs=[pl.BlockSpec(memory_space=pltpu.VMEM)],
        out_specs=(pl.BlockSpec(memory_space=pl.ANY), pl.BlockSpec(memory_space=pl.ANY)),
        scratch_shapes=[
            dma((2,)), dma((X - 1,)), dma((X - 1,)), dma((R - 1,)), dma((R - 1,)),
            dma((S - 1,)), dma((S - 1,)), dma((X - 1, S - 1)), dma((X - 1, S - 1)),
        ],
        compiler_params=pltpu.CompilerParams(collective_id=0, has_side_effects=True),
        cost_estimate=pl.CostEstimate(flops=0, bytes_accessed=100_000_000, transcendentals=0),
        name="gather",
    )(v)


def regroup_kernel(X, S, spread, mine, lsem, ss, rs):
    x, s = lax.axis_index("col"), lax.axis_index("sub")
    C = X * S
    k = x * S + s
    R, piece, kd = spread.shape
    per = R // C
    barrier = pltpu.get_barrier_semaphore()
    dests = [lax.rem(k + e, C) for e in range(C)]
    for j in dests[1:]:
        pl.semaphore_signal(
            barrier, inc=1, device_id={"col": j // S, "sub": lax.rem(j, S)}, device_id_type=MESH)
    pl.semaphore_wait(barrier, C - 1)
    target = mine.at[:, :, pl.ds(pl.multiple_of(k * kd, kd), kd)]
    copies = []
    for e in range(1, C):
        j = dests[e]
        copies.append(pltpu.make_async_remote_copy(
            spread.at[pl.ds(j * per, per)], target, ss.at[e - 1], rs.at[e - 1],
            device_id={"col": j // S, "sub": lax.rem(j, S)}, device_id_type=MESH))
    copies.append(pltpu.make_async_copy(spread.at[pl.ds(k * per, per)], target, lsem))
    for copy in copies:
        copy.start()
    for copy in copies:
        copy.wait()


def regroup(spread, X, S):
    R, piece, kd = spread.shape
    C = X * S
    dma = pltpu.SemaphoreType.DMA
    return pl.pallas_call(
        functools.partial(regroup_kernel, X, S),
        out_shape=jax.ShapeDtypeStruct((R // C, piece, kd * C), spread.dtype),
        in_specs=[pl.BlockSpec(memory_space=pltpu.VMEM)],
        out_specs=pl.BlockSpec(memory_space=pl.ANY),
        scratch_shapes=[dma, dma((C - 1,)), dma((C - 1,))],
        compiler_params=pltpu.CompilerParams(collective_id=1, has_side_effects=True),
        cost_estimate=pl.CostEstimate(flops=0, bytes_accessed=60_000_000, transcendentals=0),
        name="regroup",
    )(spread)


def project_kernel(R, X, S, relative, p, out, acc, from_sub, from_col, from_row, res, from_pair,
                   a_s, a_r, b_s, b_r, c_s, c_r, d_s, d_r):
    r, x, s = lax.axis_index("row"), lax.axis_index("col"), lax.axis_index("sub")
    K = p.shape[0]
    rb, kd = K // R, K // (X * S)

    def rows(i):
        return pl.ds(pl.multiple_of(i * rb, rb), rb)

    def columns(cx, cs):
        return pl.ds(pl.multiple_of((cx * S + cs) * kd, kd), kd)

    def held(i):
        if not relative:
            return rows(i)
        return rows(lax.rem(i // S + X - x, X) * S + lax.rem(i, S))

    def held_columns(d, cs):
        return columns(d if relative else col(d), cs)

    def col(d):
        return lax.rem(x + d, X)

    peers = [{"col": col(d)} for d in range(1, X)]
    peers += [{"row": lax.rem(r + d, R)} for d in range(1, R)]
    peers += [{"sub": lax.rem(s + d, S)} for d in range(1, S)]
    barrier = pltpu.get_barrier_semaphore()
    for peer in peers:
        pl.semaphore_signal(barrier, inc=1, device_id=peer, device_id_type=MESH)
    pl.semaphore_wait(barrier, len(peers))

    order = list(range(1, X)) + [0]
    steps = list(range(1, R)) + [0]
    pair = {}
    for d in order:
        for e in range(1, S):
            other = lax.rem(s + e, S)
            pair[d, e] = pltpu.make_async_remote_copy(
                p.at[:, held_columns(d, other)], from_sub.at[e - 1, d],
                a_s.at[e - 1, d], a_r.at[e - 1, d],
                device_id={"sub": other}, device_id_type=MESH)
            pair[d, e].start()
    cross = {}
    for d in order:
        for e in range(1, S):
            pair[d, e].wait_recv()
        for q in steps:
            here = rows(lax.rem(r + q, R))
            there = held(lax.rem(r + q, R))
            total = p[there, held_columns(d, s)]
            for e in range(1, S):
                total = total + from_sub[e - 1, d, there, :]
            acc[d, here, :] = total
            if d > 0:
                cross[d, q] = pltpu.make_async_remote_copy(
                    acc.at[d, here], from_col.at[d - 1, here],
                    b_s.at[d - 1, q], b_r.at[d - 1, q],
                    device_id={"col": col(d)}, device_id_type=MESH)
                cross[d, q].start()
    along = []
    for q in steps:
        i = lax.rem(r + q, R)
        here = rows(i)
        total = acc[0, here, :]
        for d in range(1, X):
            cross[d, q].wait_recv()
            total = total + from_col[d - 1, here, :]
        if q > 0:
            acc[0, here, :] = total
            copy = pltpu.make_async_remote_copy(
                acc.at[0, here], from_row.at[q - 1], c_s.at[q - 1], c_r.at[q - 1],
                device_id={"row": i}, device_id_type=MESH)
            copy.start()
            along.append(copy)
    for q in range(1, R):
        along[q - 1].wait_recv()
        total = total + from_row[q - 1]
    res[...] = total
    last = []
    for e in range(1, S):
        copy = pltpu.make_async_remote_copy(
            res, from_pair.at[e - 1], d_s.at[e - 1], d_r.at[e - 1],
            device_id={"sub": lax.rem(s + e, S)}, device_id_type=MESH)
        copy.start()
        last.append(copy)
    out[:, pl.ds(pl.multiple_of(s * kd, kd), kd)] = total
    for e in range(1, S):
        last[e - 1].wait_recv()
        out[:, pl.ds(pl.multiple_of(lax.rem(s - e + S, S) * kd, kd), kd)] = from_pair[e - 1]
    for copy in list(pair.values()) + list(cross.values()) + along + last:
        copy.wait_send()


def project(partial, R, X, S, relative):
    K = partial.shape[0]
    rb, kd = K // R, K // (X * S)
    dma = pltpu.SemaphoreType.DMA
    f32 = jnp.float32
    return pl.pallas_call(
        functools.partial(project_kernel, R, X, S, relative),
        out_shape=jax.ShapeDtypeStruct((rb, S * kd), f32),
        in_specs=[pl.BlockSpec(memory_space=pltpu.VMEM)],
        out_specs=pl.BlockSpec(memory_space=pltpu.VMEM),
        scratch_shapes=[
            pltpu.VMEM((X, K, kd), f32),
            pltpu.VMEM((S - 1, X, K, kd), f32),
            pltpu.VMEM((X - 1, K, kd), f32),
            pltpu.VMEM((R - 1, rb, kd), f32),
            pltpu.VMEM((rb, kd), f32),
            pltpu.VMEM((S - 1, rb, kd), f32),
            dma((S - 1, X)), dma((S - 1, X)), dma((X - 1, R)), dma((X - 1, R)),
            dma((R - 1,)), dma((R - 1,)), dma((S - 1,)), dma((S - 1,)),
        ],
        compiler_params=pltpu.CompilerParams(collective_id=2, has_side_effects=True),
        cost_estimate=pl.CostEstimate(flops=0, bytes_accessed=60_000_000, transcendentals=0),
        name="project",
    )(partial)


def split(value):
    high = value.astype(jnp.bfloat16)
    return high, (value - high.astype(jnp.float32)).astype(jnp.bfloat16)


def dot3(a_high, a_low, b_high, b_low, contract):
    def one(a, b):
        return lax.dot_general(a, b, ((contract, (0,)), ((), ())),
                               preferred_element_type=jnp.float32)
    return one(a_high, b_high) + (one(a_high, b_low) + one(a_low, b_high))


def image_kernel(R, S, Q, v, a, out, vall, img, ybuf, sbuf, ubuf, tbuf, abuf, ahi, alo, vhi, vlo,
                 ihi, ilo, rhi, rlo, lsem, asem, os, orr, xs, xr, fs, fr, hs, hr, ts, tr):
    z, x, s = lax.axis_index("row"), lax.axis_index("col"), lax.axis_index("sub")
    c = x * S + s
    m, kd = v.shape
    half = S * kd
    steps = m // abuf.shape[2]
    w = m // steps
    pw = w // Q
    first = jnp.where(x == 0, c, 0)
    last = jnp.where(x == 0, R - 1, c)
    chained = (z >= first) & (z <= last)
    diag = z == c
    pair = (z == x * S + 1) & (s == 0)
    relay = (z == x * S) & (s == 1 - x)
    adds = (x == 1) & chained
    weight = jnp.where(diag, 0.5, 1.0).astype(jnp.float32)
    other = 1 - s

    def rows(i, n):
        return pl.ds(pl.multiple_of(i * n, n), n)

    def block(hh, ss):
        return pl.ds(pl.multiple_of((hh * S + ss) * kd, kd), kd)

    barrier = pltpu.get_barrier_semaphore()
    pl.semaphore_signal(barrier, inc=1, device_id={"sub": other}, device_id_type=MESH)
    pl.semaphore_signal(barrier, inc=1, device_id={"col": 1 - x}, device_id_type=MESH)

    @pl.when(z > 0)
    def _():
        for t in range(S):
            pl.semaphore_signal(barrier, inc=1, device_id={"row": z - 1, "sub": t}, device_id_type=MESH)

    @pl.when(z < R - 1)
    def _():
        for t in range(S):
            pl.semaphore_signal(barrier, inc=1, device_id={"row": z + 1, "sub": t}, device_id_type=MESH)

    def load(i):
        return pltpu.make_async_copy(a.at[:, rows(i, w)], abuf.at[lax.rem(i, 2)], asem.at[lax.rem(i, 2)])

    def mate():
        return pltpu.make_async_remote_copy(
            v, vall.at[:, block(0, s)], os, orr, device_id={"sub": other}, device_id_type=MESH)

    def across(i):
        return pltpu.make_async_remote_copy(
            v.at[rows(i, w), :], vall.at[rows(i, w), block(1, s)], xs.at[i], xr.at[i],
            device_id={"col": 1 - x}, device_id_type=MESH)

    def share(i):
        here = vall.at[rows(i, w), block(1, s)]
        return pltpu.make_async_remote_copy(
            here, here, fs.at[i], fr.at[i], device_id={"sub": other}, device_id_type=MESH)

    def hand(i):
        return pltpu.make_async_remote_copy(
            vall.at[rows(i, w), pl.ds(half, half)], ubuf.at[rows(i, w), :], hs.at[i], hr.at[i],
            device_id={"row": z + 1, "sub": 0}, device_id_type=MESH)

    def origin(k):
        return pltpu.make_async_remote_copy(
            vall.at[rows(k, pw), pl.ds(0, half)], sbuf.at[rows(k, pw), :], ts.at[k], tr.at[k],
            device_id={"row": z + 1}, device_id_type=MESH)

    def onward(k):
        return pltpu.make_async_remote_copy(
            sbuf.at[rows(k, pw), :], sbuf.at[rows(k, pw), :], ts.at[k], tr.at[k],
            device_id={"row": z + 1}, device_id_type=MESH)

    own = pltpu.make_async_copy(v, vall.at[:, block(0, s)], lsem)
    own.start()
    load(0).start()
    img[...] = jnp.zeros_like(img)
    ybuf[...] = jnp.zeros_like(ybuf)
    pl.semaphore_wait(barrier, 2 + S * ((z > 0).astype(jnp.int32) + (z < R - 1).astype(jnp.int32)))
    mate().start()

    def begin(i, carry):
        across(i).start()
        return carry

    lax.fori_loop(0, steps, begin, 0)
    own.wait()
    mate().wait_recv()
    source = (x == 0) & diag

    @pl.when(source)
    def _():
        def send(k, carry):
            origin(k).start()
            return carry
        lax.fori_loop(0, steps * Q, send, 0)

    def prepare(i, hh):
        here, columns = rows(i, w), pl.ds(hh * half, half)
        high, low = split(vall[here, columns])
        vhi[here, columns] = high
        vlo[here, columns] = low

    def prepare_own(i, carry):
        prepare(i, 0)
        return carry

    lax.fori_loop(0, steps, prepare_own, 0)

    def multiply(columns):
        def tile(t, carry):
            here = rows(t, w)
            img[here, columns] += dot3(ahi[here, :], alo[here, :], rhi[...], rlo[...], (1,))
            return carry
        lax.fori_loop(0, steps, tile, 0)

    def feed(value):
        high, low = split(value)
        rhi[...] = high
        rlo[...] = low

    def open_block(i):
        load(i).wait()

        @pl.when(i < steps - 1)
        def _():
            load(i + 1).start()

        def cut(t, carry):
            high, low = split(abuf[lax.rem(i, 2), rows(t, w), :])
            ahi[rows(t, w), :] = high
            alo[rows(t, w), :] = low
            return carry
        lax.fori_loop(0, steps, cut, 0)

    def receive(i):
        across(i).wait_recv()
        share(i).start()

    def collect(i):
        share(i).wait_recv()
        prepare(i, 1)

        @pl.when(relay)
        def _():
            hand(i).start()

    def fold(hh):
        columns = pl.ds(hh * half, half)

        def halve(t, carry):
            high, low = split(img[rows(t, w), columns])
            ihi[rows(t, w), :] = high
            ilo[rows(t, w), :] = low
            return carry
        lax.fori_loop(0, steps, halve, 0)
        for b in range(2 * S):
            part = slice(b * kd, (b + 1) * kd)
            ybuf[part, columns] = dot3(vhi[:, part], vlo[:, part], ihi[...], ilo[...], (0,))

    def local_step(i, carry):
        receive(i)
        open_block(i)

        @pl.when(x == 0)
        def _():
            feed(0.5 * vall[rows(i, w), pl.ds(0, half)])
            multiply(pl.ds(0, half))
        collect(i)
        feed(0.5 * vall[rows(i, w), pl.ds(half, half)])
        multiply(pl.ds(half, half))
        return carry

    def stream_step(i, carry):
        @pl.when(jnp.logical_not(diag) & (2 * i < steps))
        def _():
            receive(2 * i)
            receive(2 * i + 1)

        open_block(i)

        @pl.when(adds)
        def _():
            tbuf[...] = weight * dot3(ahi[...], alo[...], vhi[:, :half], vlo[:, :half], (0,))

        def piece(p, carry):
            k = i * Q + p

            @pl.when(chained & (z > first))
            def _():
                onward(k).wait_recv()

            @pl.when(adds & (z == first))
            def _():
                sbuf[rows(k, pw), :] = tbuf[rows(p, pw), :]

            @pl.when(adds & (z > first))
            def _():
                sbuf[rows(k, pw), :] += tbuf[rows(p, pw), :]

            @pl.when(chained & (z < last))
            def _():
                onward(k).start()
            return carry
        lax.fori_loop(0, Q, piece, 0)

        lag = jnp.where(relay, 0, steps // 2)

        @pl.when(jnp.logical_not(diag) & (i >= lag) & (2 * (i - lag) < steps))
        def _():
            collect(2 * (i - lag))
            collect(2 * (i - lag) + 1)

        @pl.when((x == 0) & chained)
        def _():
            feed(sbuf[rows(i, w), :])
            multiply(pl.ds(0, half))

        @pl.when((x == 1) & diag)
        def _():
            feed(sbuf[rows(i, w), :])
            for b in range(2 * S):
                part = slice(b * kd, (b + 1) * kd)
                ybuf[part, :half] += dot3(vhi[rows(i, w), part], vlo[rows(i, w), part], rhi[...], rlo[...], (0,))

        @pl.when(pair)
        def _():
            hand(i).wait_recv()
            feed(ubuf[rows(i, w), :])
            multiply(pl.ds(half, half))
        return carry

    @pl.when(diag)
    def _():
        lax.fori_loop(0, steps, local_step, 0)
        fold(1)

        @pl.when(x == 0)
        def _():
            fold(0)

        @pl.when(x == 1)
        def _():
            load(0).start()

    @pl.when(jnp.logical_not(source))
    def _():
        lax.fori_loop(0, steps, stream_step, 0)

    @pl.when(pair)
    def _():
        fold(1)

    @pl.when((x == 0) & chained & jnp.logical_not(diag))
    def _():
        fold(0)

    for b in range(2 * S):
        mine = slice(b * kd, (b + 1) * kd)
        for e in range(b, 2 * S):
            theirs = slice(e * kd, (e + 1) * kd)
            total = ybuf[mine, theirs] + ybuf[theirs, mine].T
            out[mine, theirs] = total
            if e > b:
                out[theirs, mine] = total.T

    mate().wait_send()

    def drain(i, carry):
        across(i).wait_send()
        share(i).wait_send()

        @pl.when(relay)
        def _():
            hand(i).wait_send()
        return carry

    lax.fori_loop(0, steps, drain, 0)

    def sent(k, carry):
        @pl.when(source)
        def _():
            origin(k).wait_send()

        @pl.when(chained & (z < last) & jnp.logical_not(source))
        def _():
            onward(k).wait_send()
        return carry

    lax.fori_loop(0, steps * Q, sent, 0)


def image(v, a, R, S):
    m, kd = v.shape
    w = kd
    steps = m // w
    Q = 4
    half = S * kd
    dma = pltpu.SemaphoreType.DMA
    f32, bf16 = jnp.float32, jnp.bfloat16
    return pl.pallas_call(
        functools.partial(image_kernel, R, S, Q),
        out_shape=jax.ShapeDtypeStruct((2 * half, 2 * half), f32),
        in_specs=[pl.BlockSpec(memory_space=pltpu.VMEM), pl.BlockSpec(memory_space=pl.ANY)],
        out_specs=pl.BlockSpec(memory_space=pltpu.VMEM),
        scratch_shapes=[
            pltpu.VMEM((m, 2 * half), f32), pltpu.VMEM((m, 2 * half), f32),
            pltpu.VMEM((2 * half, 2 * half), f32),
            pltpu.VMEM((m, half), f32), pltpu.VMEM((m, half), f32), pltpu.VMEM((w, half), f32),
            pltpu.VMEM((2, m, w), f32), pltpu.VMEM((m, w), bf16), pltpu.VMEM((m, w), bf16),
            pltpu.VMEM((m, 2 * half), bf16), pltpu.VMEM((m, 2 * half), bf16),
            pltpu.VMEM((m, half), bf16), pltpu.VMEM((m, half), bf16),
            pltpu.VMEM((w, half), bf16), pltpu.VMEM((w, half), bf16),
            dma, dma((2,)), dma, dma, dma((steps,)), dma((steps,)), dma((steps,)), dma((steps,)),
            dma((steps,)), dma((steps,)), dma((steps * Q,)), dma((steps * Q,)),
        ],
        compiler_params=pltpu.CompilerParams(
            collective_id=3, has_side_effects=True, vmem_limit_bytes=60_000_000),
        cost_estimate=pl.CostEstimate(flops=0, bytes_accessed=100_000_000, transcendentals=0),
        name="image",
    )(v, a)


def partial_general(matrix, basis_vectors):
    R = lax.axis_size("row")
    S = lax.axis_size("sub")
    C = lax.axis_size("col") * S
    m, kd = basis_vectors.shape
    K = kd * C
    n = matrix.shape[1]
    per = n // m
    piece = m // R
    own, spread = gather(basis_vectors, R, C // S, S)
    width = K // CHUNKS
    images = []
    for c in range(CHUNKS):
        part = lax.dot_general(
            matrix,
            own[:, c * width : (c + 1) * width],
            (((0,), (0,)), ((), ())),
            precision=lax.Precision.HIGH,
            preferred_element_type=jnp.float32,
        )
        if c == 0:
            part, spread = lax.optimization_barrier((part, spread))
        part = part.reshape(per, R, piece, width).transpose(1, 0, 2, 3).reshape(R * per * piece, width)
        images.append(lax.psum_scatter(part, "row", scatter_dimension=0, tiled=True))
    mine = regroup(spread, C // S, S).reshape(per * piece, K)
    return jnp.concatenate(
        [
            lax.dot_general(
                mine,
                image,
                (((0,), (0,)), ((), ())),
                precision=lax.Precision.HIGH,
                preferred_element_type=jnp.float32,
            )
            for image in images
        ],
        axis=1,
    )


def shards(matrix, basis_vectors, split_size):
    R = lax.axis_size("row")
    X = lax.axis_size("col")
    S = lax.axis_size("sub")
    m, n = matrix.shape
    halves = m == n and R == X * S and X == 2 and S == 2
    if halves:
        partial_proj = image(basis_vectors, matrix, R, S)
    else:
        partial_proj = partial_general(matrix, basis_vectors)
    child_block = project(partial_proj, R, X, S, halves)
    row_ids = (
        jnp.arange(child_block.shape[0], dtype=jnp.int32)
        + lax.axis_index("row") * child_block.shape[0]
    )
    col_ids = (
        jnp.arange(child_block.shape[1], dtype=jnp.int32)
        + lax.axis_index("col") * child_block.shape[1]
    )
    leading = split_size[0]
    row_first = row_ids < leading
    col_first = col_ids < leading
    mask_one = row_first[:, None] & col_first[None, :]
    mask_two = jnp.logical_not(row_first)[:, None] & jnp.logical_not(col_first)[None, :]
    selected = jnp.where(lax.axis_index("sub") == 0, mask_one, mask_two)
    return jnp.where(selected, child_block, jnp.zeros((), jnp.float32))[None]


def solution(mesh):
    placed = (
        P(("groups", "row"), ("col", "sub")),
        P(("groups", "row"), ("col", "sub")),
        P("groups"),
    )
    return jax.shard_map(
        shards,
        mesh=mesh,
        in_specs=placed,
        out_specs=P("sub", ("groups", "row"), "col"),
        check_vma=False,
    )
```

```python
import functools

import jax
import jax.numpy as jnp
from jax import lax
from jax.experimental import pallas as pl
from jax.experimental.pallas import tpu as pltpu
from jax.sharding import PartitionSpec as P

MESH = pl.DeviceIdType.MESH
CHUNKS = 1


def gather_kernel(R, X, S, v, own, spread, lsem, xs, xr, zs, zr, ps, pr, fs, fr):
    r, x, s = lax.axis_index("row"), lax.axis_index("col"), lax.axis_index("sub")
    m, kd = v.shape
    piece = m // R

    def columns(cx, cs):
        return pl.ds(pl.multiple_of((cx * S + cs) * kd, kd), kd)

    peers = [{"col": lax.rem(x + d, X)} for d in range(1, X)]
    peers += [{"row": lax.rem(r + d, R)} for d in range(1, R)]
    peers += [{"sub": lax.rem(s + d, S)} for d in range(1, S)]
    barrier = pltpu.get_barrier_semaphore()
    for peer in peers:
        pl.semaphore_signal(barrier, inc=1, device_id=peer, device_id_type=MESH)
    pl.semaphore_wait(barrier, len(peers))

    mine = own.at[:, columns(x, s)]
    across, spreads, partner, forward = [], [], [], []
    for d in range(1, X):
        across.append(pltpu.make_async_remote_copy(
            v, mine, xs.at[d - 1], xr.at[d - 1],
            device_id={"col": lax.rem(x + d, X)}, device_id_type=MESH))
    for d in range(1, R):
        i = lax.rem(r + d, R)
        spreads.append(pltpu.make_async_remote_copy(
            v.at[pl.ds(pl.multiple_of(i * piece, piece), piece), :], spread.at[r],
            zs.at[d - 1], zr.at[d - 1],
            device_id={"row": i}, device_id_type=MESH))
    for d in range(1, S):
        partner.append(pltpu.make_async_remote_copy(
            v, mine, ps.at[d - 1], pr.at[d - 1],
            device_id={"sub": lax.rem(s + d, S)}, device_id_type=MESH))
    for copy in across + spreads + partner:
        copy.start()
    local = [
        pltpu.make_async_copy(v, mine, lsem.at[0]),
        pltpu.make_async_copy(
            v.at[pl.ds(pl.multiple_of(r * piece, piece), piece), :], spread.at[r], lsem.at[1]),
    ]
    for copy in local:
        copy.start()
    for d in range(1, X):
        across[d - 1].wait_recv()
        block = own.at[:, columns(lax.rem(x - d + X, X), s)]
        for e in range(1, S):
            copy = pltpu.make_async_remote_copy(
                block, block, fs.at[d - 1, e - 1], fr.at[d - 1, e - 1],
                device_id={"sub": lax.rem(s + e, S)}, device_id_type=MESH)
            copy.start()
            forward.append(copy)
    for copy in across:
        copy.wait_send()
    for copy in spreads + partner + forward:
        copy.wait()
    for copy in local:
        copy.wait()


def gather(v, R, X, S):
    m, kd = v.shape
    dma = pltpu.SemaphoreType.DMA
    return pl.pallas_call(
        functools.partial(gather_kernel, R, X, S),
        out_shape=(
            jax.ShapeDtypeStruct((m, kd * X * S), v.dtype),
            jax.ShapeDtypeStruct((R, m // R, kd), v.dtype),
        ),
        in_specs=[pl.BlockSpec(memory_space=pltpu.VMEM)],
        out_specs=(pl.BlockSpec(memory_space=pl.ANY), pl.BlockSpec(memory_space=pl.ANY)),
        scratch_shapes=[
            dma((2,)), dma((X - 1,)), dma((X - 1,)), dma((R - 1,)), dma((R - 1,)),
            dma((S - 1,)), dma((S - 1,)), dma((X - 1, S - 1)), dma((X - 1, S - 1)),
        ],
        compiler_params=pltpu.CompilerParams(collective_id=0, has_side_effects=True),
        cost_estimate=pl.CostEstimate(flops=0, bytes_accessed=100_000_000, transcendentals=0),
        name="gather",
    )(v)


def regroup_kernel(X, S, spread, mine, lsem, ss, rs):
    x, s = lax.axis_index("col"), lax.axis_index("sub")
    C = X * S
    k = x * S + s
    R, piece, kd = spread.shape
    per = R // C
    barrier = pltpu.get_barrier_semaphore()
    dests = [lax.rem(k + e, C) for e in range(C)]
    for j in dests[1:]:
        pl.semaphore_signal(
            barrier, inc=1, device_id={"col": j // S, "sub": lax.rem(j, S)}, device_id_type=MESH)
    pl.semaphore_wait(barrier, C - 1)
    target = mine.at[:, :, pl.ds(pl.multiple_of(k * kd, kd), kd)]
    copies = []
    for e in range(1, C):
        j = dests[e]
        copies.append(pltpu.make_async_remote_copy(
            spread.at[pl.ds(j * per, per)], target, ss.at[e - 1], rs.at[e - 1],
            device_id={"col": j // S, "sub": lax.rem(j, S)}, device_id_type=MESH))
    copies.append(pltpu.make_async_copy(spread.at[pl.ds(k * per, per)], target, lsem))
    for copy in copies:
        copy.start()
    for copy in copies:
        copy.wait()


def regroup(spread, X, S):
    R, piece, kd = spread.shape
    C = X * S
    dma = pltpu.SemaphoreType.DMA
    return pl.pallas_call(
        functools.partial(regroup_kernel, X, S),
        out_shape=jax.ShapeDtypeStruct((R // C, piece, kd * C), spread.dtype),
        in_specs=[pl.BlockSpec(memory_space=pltpu.VMEM)],
        out_specs=pl.BlockSpec(memory_space=pl.ANY),
        scratch_shapes=[dma, dma((C - 1,)), dma((C - 1,))],
        compiler_params=pltpu.CompilerParams(collective_id=1, has_side_effects=True),
        cost_estimate=pl.CostEstimate(flops=0, bytes_accessed=60_000_000, transcendentals=0),
        name="regroup",
    )(spread)


def project_kernel(R, X, S, relative, p, out, acc, from_sub, from_col, from_row, res, from_pair,
                   a_s, a_r, b_s, b_r, c_s, c_r, d_s, d_r):
    r, x, s = lax.axis_index("row"), lax.axis_index("col"), lax.axis_index("sub")
    K = p.shape[0]
    rb, kd = K // R, K // (X * S)

    def rows(i):
        return pl.ds(pl.multiple_of(i * rb, rb), rb)

    def columns(cx, cs):
        return pl.ds(pl.multiple_of((cx * S + cs) * kd, kd), kd)

    def held(i):
        if not relative:
            return rows(i)
        return rows(lax.rem(i // S + X - x, X) * S + lax.rem(i, S))

    def held_columns(d, cs):
        return columns(d if relative else col(d), cs)

    def col(d):
        return lax.rem(x + d, X)

    peers = [{"col": col(d)} for d in range(1, X)]
    peers += [{"row": lax.rem(r + d, R)} for d in range(1, R)]
    peers += [{"sub": lax.rem(s + d, S)} for d in range(1, S)]
    barrier = pltpu.get_barrier_semaphore()
    for peer in peers:
        pl.semaphore_signal(barrier, inc=1, device_id=peer, device_id_type=MESH)
    pl.semaphore_wait(barrier, len(peers))

    order = list(range(1, X)) + [0]
    steps = list(range(1, R)) + [0]
    pair = {}
    for d in order:
        for e in range(1, S):
            other = lax.rem(s + e, S)
            pair[d, e] = pltpu.make_async_remote_copy(
                p.at[:, held_columns(d, other)], from_sub.at[e - 1, d],
                a_s.at[e - 1, d], a_r.at[e - 1, d],
                device_id={"sub": other}, device_id_type=MESH)
            pair[d, e].start()
    cross = {}
    for d in order:
        for e in range(1, S):
            pair[d, e].wait_recv()
        for q in steps:
            here = rows(lax.rem(r + q, R))
            there = held(lax.rem(r + q, R))
            total = p[there, held_columns(d, s)]
            for e in range(1, S):
                total = total + from_sub[e - 1, d, there, :]
            acc[d, here, :] = total
            if d > 0:
                cross[d, q] = pltpu.make_async_remote_copy(
                    acc.at[d, here], from_col.at[d - 1, here],
                    b_s.at[d - 1, q], b_r.at[d - 1, q],
                    device_id={"col": col(d)}, device_id_type=MESH)
                cross[d, q].start()
    along = []
    for q in steps:
        i = lax.rem(r + q, R)
        here = rows(i)
        total = acc[0, here, :]
        for d in range(1, X):
            cross[d, q].wait_recv()
            total = total + from_col[d - 1, here, :]
        if q > 0:
            acc[0, here, :] = total
            copy = pltpu.make_async_remote_copy(
                acc.at[0, here], from_row.at[q - 1], c_s.at[q - 1], c_r.at[q - 1],
                device_id={"row": i}, device_id_type=MESH)
            copy.start()
            along.append(copy)
    for q in range(1, R):
        along[q - 1].wait_recv()
        total = total + from_row[q - 1]
    res[...] = total
    last = []
    for e in range(1, S):
        copy = pltpu.make_async_remote_copy(
            res, from_pair.at[e - 1], d_s.at[e - 1], d_r.at[e - 1],
            device_id={"sub": lax.rem(s + e, S)}, device_id_type=MESH)
        copy.start()
        last.append(copy)
    out[:, pl.ds(pl.multiple_of(s * kd, kd), kd)] = total
    for e in range(1, S):
        last[e - 1].wait_recv()
        out[:, pl.ds(pl.multiple_of(lax.rem(s - e + S, S) * kd, kd), kd)] = from_pair[e - 1]
    for copy in list(pair.values()) + list(cross.values()) + along + last:
        copy.wait_send()


def project(partial, R, X, S, relative):
    K = partial.shape[0]
    rb, kd = K // R, K // (X * S)
    dma = pltpu.SemaphoreType.DMA
    f32 = jnp.float32
    return pl.pallas_call(
        functools.partial(project_kernel, R, X, S, relative),
        out_shape=jax.ShapeDtypeStruct((rb, S * kd), f32),
        in_specs=[pl.BlockSpec(memory_space=pltpu.VMEM)],
        out_specs=pl.BlockSpec(memory_space=pltpu.VMEM),
        scratch_shapes=[
            pltpu.VMEM((X, K, kd), f32),
            pltpu.VMEM((S - 1, X, K, kd), f32),
            pltpu.VMEM((X - 1, K, kd), f32),
            pltpu.VMEM((R - 1, rb, kd), f32),
            pltpu.VMEM((rb, kd), f32),
            pltpu.VMEM((S - 1, rb, kd), f32),
            dma((S - 1, X)), dma((S - 1, X)), dma((X - 1, R)), dma((X - 1, R)),
            dma((R - 1,)), dma((R - 1,)), dma((S - 1,)), dma((S - 1,)),
        ],
        compiler_params=pltpu.CompilerParams(collective_id=2, has_side_effects=True),
        cost_estimate=pl.CostEstimate(flops=0, bytes_accessed=60_000_000, transcendentals=0),
        name="project",
    )(partial)


def split(value):
    high = value.astype(jnp.bfloat16)
    return high, (value - high.astype(jnp.float32)).astype(jnp.bfloat16)


def dot3(a_high, a_low, b_high, b_low, contract):
    def one(a, b):
        return lax.dot_general(a, b, ((contract, (0,)), ((), ())),
                               preferred_element_type=jnp.float32)
    return one(a_high, b_high) + (one(a_high, b_low) + one(a_low, b_high))


def image_kernel(R, S, Q, J, v, a, out, vall, img, ybuf, sbuf, ubuf, tbuf, abuf, ahi, alo, vhi, vlo,
                 ihi, ilo, rhi, rlo, side, dbuf, lsem, asem, os, orr, xs, xr, fs, fr, hs, hr, ts, tr,
                 ds, dr):
    z, x, s = lax.axis_index("row"), lax.axis_index("col"), lax.axis_index("sub")
    c = x * S + s
    m, kd = v.shape
    half = S * kd
    steps = m // abuf.shape[2]
    w = m // steps
    pw = w // Q
    first = jnp.where(x == 0, c, 0)
    last = jnp.where(x == 0, R - 1, c)
    chained = (z >= first) & (z <= last)
    diag = z == c
    pair = (z == x * S + 1) & (s == 0)
    relay = (z == x * S) & (s == 1 - x)
    adds = (x == 1) & chained
    cut = steps - J
    below = jnp.logical_not(diag) & jnp.where(x == 0, z > c, z < c)
    whole = diag | (below & (z // S == x))
    tiles = jnp.where(whole, steps, cut)
    count = jnp.where(x == 0, cut, steps)
    weight = jnp.where(diag, 0.5, 1.0).astype(jnp.float32)
    other = 1 - s

    def rows(i, n):
        return pl.ds(pl.multiple_of(i * n, n), n)

    def block(hh, ss):
        return pl.ds(pl.multiple_of((hh * S + ss) * kd, kd), kd)

    barrier = pltpu.get_barrier_semaphore()
    pl.semaphore_signal(barrier, inc=1, device_id={"sub": other}, device_id_type=MESH)
    pl.semaphore_signal(barrier, inc=1, device_id={"col": 1 - x}, device_id_type=MESH)

    @pl.when(z > 0)
    def _():
        for t in range(S):
            pl.semaphore_signal(barrier, inc=1, device_id={"row": z - 1, "sub": t}, device_id_type=MESH)

    @pl.when(z < R - 1)
    def _():
        for t in range(S):
            pl.semaphore_signal(barrier, inc=1, device_id={"row": z + 1, "sub": t}, device_id_type=MESH)

    def load(i, slot=None):
        slot = lax.rem(i, 2) if slot is None else slot
        return pltpu.make_async_copy(a.at[:, rows(i, w)], abuf.at[slot], asem.at[slot])

    def chunk(n):
        return lax.rem(n + cut, steps)

    def mate():
        return pltpu.make_async_remote_copy(
            v, vall.at[:, block(0, s)], os, orr, device_id={"sub": other}, device_id_type=MESH)

    def across(i):
        return pltpu.make_async_remote_copy(
            v.at[rows(i, w), :], vall.at[rows(i, w), block(1, s)], xs.at[i], xr.at[i],
            device_id={"col": 1 - x}, device_id_type=MESH)

    def share(i):
        here = vall.at[rows(i, w), block(1, s)]
        return pltpu.make_async_remote_copy(
            here, here, fs.at[i], fr.at[i], device_id={"sub": other}, device_id_type=MESH)

    def hand(i):
        return pltpu.make_async_remote_copy(
            vall.at[rows(i, w), pl.ds(half, half)], ubuf.at[rows(i, w), :], hs.at[i], hr.at[i],
            device_id={"row": z + 1, "sub": 0}, device_id_type=MESH)

    def origin(k):
        return pltpu.make_async_remote_copy(
            vall.at[rows(k, pw), pl.ds(0, half)], sbuf.at[rows(k, pw), :], ts.at[k], tr.at[k],
            device_id={"row": z + 1}, device_id_type=MESH)

    def onward(k):
        return pltpu.make_async_remote_copy(
            sbuf.at[rows(k, pw), :], sbuf.at[rows(k, pw), :], ts.at[k], tr.at[k],
            device_id={"row": z + 1}, device_id_type=MESH)

    def fall(k):
        g, p = k // Q, lax.rem(k, Q)
        return pltpu.make_async_remote_copy(
            side.at[g, rows(p, pw), :], dbuf.at[rows(k, pw), :], ds.at[k], dr.at[k],
            device_id={"row": z - 1}, device_id_type=MESH)

    def drop(k, hh):
        base = lax.rem(k, J * Q) + cut * Q
        return pltpu.make_async_remote_copy(
            vall.at[rows(base, pw), pl.ds(hh * half, half)], dbuf.at[rows(k, pw), :], ds.at[k], dr.at[k],
            device_id={"row": z - 1}, device_id_type=MESH)

    def pass_down(k):
        return pltpu.make_async_remote_copy(
            dbuf.at[rows(k, pw), :], dbuf.at[rows(k, pw), :], ds.at[k], dr.at[k],
            device_id={"row": z - 1}, device_id_type=MESH)

    def each(lo, hi, act):
        def go(k, carry):
            act(k)
            return carry
        lax.fori_loop(lo, hi, go, 0)

    own = pltpu.make_async_copy(v, vall.at[:, block(0, s)], lsem)
    own.start()

    @pl.when(diag)
    def _():
        load(chunk(0)).start()

    @pl.when(jnp.logical_not(diag))
    def _():
        load(0).start()
    img[...] = jnp.zeros_like(img)
    ybuf[...] = jnp.zeros_like(ybuf)
    pl.semaphore_wait(barrier, 2 + S * ((z > 0).astype(jnp.int32) + (z < R - 1).astype(jnp.int32)))
    mate().start()

    each(0, steps, lambda n: across(chunk(n)).start())
    own.wait()
    mate().wait_recv()
    source = (x == 0) & diag

    @pl.when(source)
    def _():
        each(0, cut * Q, lambda k: origin(k).start())

    @pl.when((x == 1) & diag)
    def _():
        each(0, J * Q, lambda k: drop(k, 0).start())

    def prepare(i, hh):
        here, columns = rows(i, w), pl.ds(hh * half, half)
        high, low = split(vall[here, columns])
        vhi[here, columns] = high
        vlo[here, columns] = low

    def prepare_own(i, carry):
        prepare(i, 0)
        return carry

    lax.fori_loop(0, steps, prepare_own, 0)

    def multiply(columns):
        def tile(t, carry):
            here = rows(t, w)
            img[here, columns] += dot3(ahi[here, :], alo[here, :], rhi[...], rlo[...], (1,))
            return carry
        lax.fori_loop(0, tiles, tile, 0)

    def feed(value):
        high, low = split(value)
        rhi[...] = high
        rlo[...] = low

    def slice_block(slot):
        def piece(t):
            high, low = split(abuf[slot, rows(t, w), :])
            ahi[rows(t, w), :] = high
            alo[rows(t, w), :] = low
        each(0, steps, piece)

    def open_block(i, until):
        load(i).wait()

        @pl.when(i < until - 1)
        def _():
            load(i + 1).start()
        slice_block(lax.rem(i, 2))

    def sides(hh, slot):
        columns = slice(hh * half, (hh + 1) * half)

        def act(j):
            load(cut + j, slot).start()
            load(cut + j, slot).wait()
            slice_block(slot)
            g = hh * J + j
            side[g] = dot3(ahi[...], alo[...], vhi[:, columns], vlo[:, columns], (0,))

            @pl.when(z == R - 1)
            def _():
                each(g * Q, (g + 1) * Q, lambda k: fall(k).start())
        each(0, J, act)

    def descend(g):
        def act(k):
            pass_down(k).wait_recv()

            @pl.when(x == 0)
            def _():
                side[g, rows(lax.rem(k, Q), pw), :] += dbuf[rows(k, pw), :]
                fall(k).start()

            @pl.when(x == 1)
            def _():
                pass_down(k).start()
        each(g * Q, (g + 1) * Q, act)

    def gather_fold(g_rows, hh, i):
        feed(g_rows)
        columns = rows(hh, half)

        def act(b):
            part = rows(b, kd)
            ybuf[part, columns] += dot3(
                vhi[rows(i, w), part], vlo[rows(i, w), part], rhi[...], rlo[...], (0,))
        each(0, 2 * S, act)

    def receive(i):
        across(i).wait_recv()
        share(i).start()

    def collect(i):
        share(i).wait_recv()
        prepare(i, 1)

        @pl.when(relay & (i < jnp.where(x == 0, cut, steps)))
        def _():
            hand(i).start()

        @pl.when((x == 1) & diag & (i >= cut))
        def _():
            base = (i - cut + J) * Q
            each(base, base + Q, lambda k: drop(k, 1).start())

    def fold(hh):
        columns = pl.ds(hh * half, half)

        def halve(t, carry):
            high, low = split(img[rows(t, w), columns])
            ihi[rows(t, w), :] = high
            ilo[rows(t, w), :] = low
            return carry
        lax.fori_loop(0, steps, halve, 0)
        def act(b):
            part = rows(b, kd)
            ybuf[part, columns] = dot3(vhi[:, part], vlo[:, part], ihi[...], ilo[...], (0,))
        each(0, 2 * S, act)

    def local_step(n, carry):
        i = chunk(n)

        @pl.when(n == 0)
        def _():
            receive(i)

        @pl.when(n < steps - 1)
        def _():
            receive(chunk(n + 1))
        load(i).wait()

        @pl.when(n < steps - 1)
        def _():
            load(chunk(n + 1)).start()
        slice_block(lax.rem(i, 2))

        @pl.when(x == 0)
        def _():
            feed(0.5 * vall[rows(i, w), pl.ds(0, half)])
            multiply(pl.ds(0, half))
        collect(i)
        feed(0.5 * vall[rows(i, w), pl.ds(half, half)])
        multiply(pl.ds(half, half))
        return carry

    def stream_step(i, carry):
        @pl.when(jnp.logical_not(diag) & (2 * i < steps))
        def _():
            receive(chunk(2 * i))
            receive(chunk(2 * i + 1))

        turn = jnp.where(z == R - 1, steps // 2 - 1, steps // 2)

        @pl.when((x == 0) & below & (i == turn))
        def _():
            each(0, steps, lambda n: collect(chunk(n)))
            sides(1, lax.rem(i + 1, 2))

        open_block(i, count)

        @pl.when(adds & whole)
        def _():
            tbuf[...] = weight * dot3(ahi[...], alo[...], vhi[:, :half], vlo[:, :half], (0,))

        @pl.when(adds & jnp.logical_not(whole) & (i < cut))
        def _():
            tbuf[...] = dot3(ahi[:cut * w, :], alo[:cut * w, :], vhi[:cut * w, :half], vlo[:cut * w, :half], (0,))

        def piece(p):
            k = i * Q + p

            @pl.when(chained & (z > first))
            def _():
                onward(k).wait_recv()

            @pl.when(adds & (z == first))
            def _():
                sbuf[rows(k, pw), :] = tbuf[rows(p, pw), :]

            @pl.when(adds & (z > first))
            def _():
                sbuf[rows(k, pw), :] += tbuf[rows(p, pw), :]

            @pl.when(chained & (z < last))
            def _():
                onward(k).start()

        @pl.when(i < cut)
        def _():
            each(0, Q, piece)

        @pl.when((x == 1) & diag & (i >= cut))
        def _():
            sbuf[rows(i, w), :] = tbuf[...]

        for g in range(2 * J):
            due_up = (x == 0) & (z < R - 1) & (i == (g + R - z if g < J else cut - 1))
            if g > J:
                due_up = jnp.bool_(False)
            elif g == J:
                due_up = due_up & (z == R - 2)
            due = due_up | ((x == 1) & (z > 0) & (i == g + c - z))

            @pl.when(below & due)
            def _():
                descend(g)

        lag = jnp.where(relay, 0, steps // 2)

        @pl.when(jnp.logical_not(diag) & ((x == 1) | relay) & (i >= lag) & (2 * (i - lag) < steps))
        def _():
            collect(chunk(2 * (i - lag)))
            collect(chunk(2 * (i - lag) + 1))

        @pl.when((x == 0) & below)
        def _():
            feed(sbuf[rows(i, w), :])
            multiply(pl.ds(0, half))

        @pl.when((x == 1) & diag)
        def _():
            gather_fold(sbuf[rows(i, w), :], 0, i)

        @pl.when((x == 1) & below & (i >= cut))
        def _():
            j = i - cut
            for hh in range(2):
                g = hh * J + j

                @pl.when(z == 0)
                def _():
                    each(g * Q, (g + 1) * Q, lambda k: pass_down(k).wait_recv())
                feed(dbuf[rows(g, w), :])
                multiply(pl.ds(hh * half, half))

        @pl.when(pair)
        def _():
            hand(i).wait_recv()
            feed(ubuf[rows(i, w), :])
            multiply(pl.ds(half, half))
        return carry

    @pl.when((x == 0) & below)
    def _():
        sides(0, 1)

    @pl.when(diag)
    def _():
        lax.fori_loop(0, steps, local_step, 0)
        fold(1)

        @pl.when(x == 0)
        def _():
            fold(0)
            def absorb(g):
                each(g * Q, (g + 1) * Q, lambda k: pass_down(k).wait_recv())
                gather_fold(dbuf[rows(g, w), :], g // J, cut + lax.rem(g, J))
            each(0, 2 * J, absorb)

        @pl.when(x == 1)
        def _():
            load(0).start()

    @pl.when(jnp.logical_not(source))
    def _():
        lax.fori_loop(0, count, stream_step, 0)

    @pl.when((x == 0) & below & (z < R - 1))
    def _():
        @pl.when(z < R - 2)
        def _():
            descend(J)
        for g in range(J + 1, 2 * J):
            descend(g)

    @pl.when(pair | ((x == 1) & below))
    def _():
        fold(1)

    @pl.when(below)
    def _():
        fold(0)

    for b in range(2 * S):
        mine = slice(b * kd, (b + 1) * kd)
        for e in range(b, 2 * S):
            theirs = slice(e * kd, (e + 1) * kd)
            total = ybuf[mine, theirs] + ybuf[theirs, mine].T
            out[mine, theirs] = total
            if e > b:
                out[theirs, mine] = total.T

    mate().wait_send()

    def drain(i):
        across(i).wait_send()
        share(i).wait_send()

        @pl.when(relay & (i < jnp.where(x == 0, cut, steps)))
        def _():
            hand(i).wait_send()
    each(0, steps, drain)

    @pl.when(source)
    def _():
        each(0, cut * Q, lambda k: origin(k).wait_send())

    @pl.when(chained & (z < last) & jnp.logical_not(source))
    def _():
        each(0, cut * Q, lambda k: onward(k).wait_send())

    @pl.when((x == 0) & below)
    def _():
        each(0, 2 * J * Q, lambda k: fall(k).wait_send())

    @pl.when((x == 1) & diag)
    def _():
        each(0, J * Q, lambda k: drop(k, 0).wait_send())
        each(J * Q, 2 * J * Q, lambda k: drop(k, 1).wait_send())

    @pl.when((x == 1) & below & (z > 0))
    def _():
        each(0, 2 * J * Q, lambda k: pass_down(k).wait_send())


def image(v, a, R, S):
    m, kd = v.shape
    w = kd
    steps = m // w
    Q = 4
    J = steps // 4
    half = S * kd
    dma = pltpu.SemaphoreType.DMA
    f32, bf16 = jnp.float32, jnp.bfloat16
    return pl.pallas_call(
        functools.partial(image_kernel, R, S, Q, J),
        out_shape=jax.ShapeDtypeStruct((2 * half, 2 * half), f32),
        in_specs=[pl.BlockSpec(memory_space=pltpu.VMEM), pl.BlockSpec(memory_space=pl.ANY)],
        out_specs=pl.BlockSpec(memory_space=pltpu.VMEM),
        scratch_shapes=[
            pltpu.VMEM((m, 2 * half), f32), pltpu.VMEM((m, 2 * half), f32),
            pltpu.VMEM((2 * half, 2 * half), f32),
            pltpu.VMEM((m, half), f32), pltpu.VMEM((m, half), f32), pltpu.VMEM((w, half), f32),
            pltpu.VMEM((2, m, w), f32), pltpu.VMEM((m, w), bf16), pltpu.VMEM((m, w), bf16),
            pltpu.VMEM((m, 2 * half), bf16), pltpu.VMEM((m, 2 * half), bf16),
            pltpu.VMEM((m, half), bf16), pltpu.VMEM((m, half), bf16),
            pltpu.VMEM((w, half), bf16), pltpu.VMEM((w, half), bf16),
            pltpu.VMEM((2 * J, w, half), f32), pltpu.VMEM((2 * J * w, half), f32),
            dma, dma((2,)), dma, dma, dma((steps,)), dma((steps,)), dma((steps,)), dma((steps,)),
            dma((steps,)), dma((steps,)), dma((steps * Q,)), dma((steps * Q,)),
            dma((2 * J * Q,)), dma((2 * J * Q,)),
        ],
        compiler_params=pltpu.CompilerParams(
            collective_id=3, has_side_effects=True, vmem_limit_bytes=64_000_000),
        cost_estimate=pl.CostEstimate(flops=0, bytes_accessed=100_000_000, transcendentals=0),
        name="image",
    )(v, a)


def partial_general(matrix, basis_vectors):
    R = lax.axis_size("row")
    S = lax.axis_size("sub")
    C = lax.axis_size("col") * S
    m, kd = basis_vectors.shape
    K = kd * C
    n = matrix.shape[1]
    per = n // m
    piece = m // R
    own, spread = gather(basis_vectors, R, C // S, S)
    width = K // CHUNKS
    images = []
    for c in range(CHUNKS):
        part = lax.dot_general(
            matrix,
            own[:, c * width : (c + 1) * width],
            (((0,), (0,)), ((), ())),
            precision=lax.Precision.HIGH,
            preferred_element_type=jnp.float32,
        )
        if c == 0:
            part, spread = lax.optimization_barrier((part, spread))
        part = part.reshape(per, R, piece, width).transpose(1, 0, 2, 3).reshape(R * per * piece, width)
        images.append(lax.psum_scatter(part, "row", scatter_dimension=0, tiled=True))
    mine = regroup(spread, C // S, S).reshape(per * piece, K)
    return jnp.concatenate(
        [
            lax.dot_general(
                mine,
                image,
                (((0,), (0,)), ((), ())),
                precision=lax.Precision.HIGH,
                preferred_element_type=jnp.float32,
            )
            for image in images
        ],
        axis=1,
    )


def shards(matrix, basis_vectors, split_size):
    R = lax.axis_size("row")
    X = lax.axis_size("col")
    S = lax.axis_size("sub")
    m, n = matrix.shape
    halves = m == n and R == X * S and X == 2 and S == 2
    if halves:
        partial_proj = image(basis_vectors, matrix, R, S)
    else:
        partial_proj = partial_general(matrix, basis_vectors)
    child_block = project(partial_proj, R, X, S, halves)
    row_ids = (
        jnp.arange(child_block.shape[0], dtype=jnp.int32)
        + lax.axis_index("row") * child_block.shape[0]
    )
    col_ids = (
        jnp.arange(child_block.shape[1], dtype=jnp.int32)
        + lax.axis_index("col") * child_block.shape[1]
    )
    leading = split_size[0]
    row_first = row_ids < leading
    col_first = col_ids < leading
    mask_one = row_first[:, None] & col_first[None, :]
    mask_two = jnp.logical_not(row_first)[:, None] & jnp.logical_not(col_first)[None, :]
    selected = jnp.where(lax.axis_index("sub") == 0, mask_one, mask_two)
    return jnp.where(selected, child_block, jnp.zeros((), jnp.float32))[None]


def solution(mesh):
    placed = (
        P(("groups", "row"), ("col", "sub")),
        P(("groups", "row"), ("col", "sub")),
        P("groups"),
    )
    return jax.shard_map(
        shards,
        mesh=mesh,
        in_specs=placed,
        out_specs=P("sub", ("groups", "row"), "col"),
        check_vma=False,
    )
```

```python
import functools

import jax
import jax.numpy as jnp
from jax import lax
from jax.experimental import pallas as pl
from jax.experimental.pallas import tpu as pltpu
from jax.sharding import PartitionSpec as P

MESH = pl.DeviceIdType.MESH
CHUNKS = 1


def gather_kernel(R, X, S, v, own, spread, lsem, xs, xr, zs, zr, ps, pr, fs, fr):
    r, x, s = lax.axis_index("row"), lax.axis_index("col"), lax.axis_index("sub")
    m, kd = v.shape
    piece = m // R

    def columns(cx, cs):
        return pl.ds(pl.multiple_of((cx * S + cs) * kd, kd), kd)

    peers = [{"col": lax.rem(x + d, X)} for d in range(1, X)]
    peers += [{"row": lax.rem(r + d, R)} for d in range(1, R)]
    peers += [{"sub": lax.rem(s + d, S)} for d in range(1, S)]
    barrier = pltpu.get_barrier_semaphore()
    for peer in peers:
        pl.semaphore_signal(barrier, inc=1, device_id=peer, device_id_type=MESH)
    pl.semaphore_wait(barrier, len(peers))

    mine = own.at[:, columns(x, s)]
    across, spreads, partner, forward = [], [], [], []
    for d in range(1, X):
        across.append(pltpu.make_async_remote_copy(
            v, mine, xs.at[d - 1], xr.at[d - 1],
            device_id={"col": lax.rem(x + d, X)}, device_id_type=MESH))
    for d in range(1, R):
        i = lax.rem(r + d, R)
        spreads.append(pltpu.make_async_remote_copy(
            v.at[pl.ds(pl.multiple_of(i * piece, piece), piece), :], spread.at[r],
            zs.at[d - 1], zr.at[d - 1],
            device_id={"row": i}, device_id_type=MESH))
    for d in range(1, S):
        partner.append(pltpu.make_async_remote_copy(
            v, mine, ps.at[d - 1], pr.at[d - 1],
            device_id={"sub": lax.rem(s + d, S)}, device_id_type=MESH))
    for copy in across + spreads + partner:
        copy.start()
    local = [
        pltpu.make_async_copy(v, mine, lsem.at[0]),
        pltpu.make_async_copy(
            v.at[pl.ds(pl.multiple_of(r * piece, piece), piece), :], spread.at[r], lsem.at[1]),
    ]
    for copy in local:
        copy.start()
    for d in range(1, X):
        across[d - 1].wait_recv()
        block = own.at[:, columns(lax.rem(x - d + X, X), s)]
        for e in range(1, S):
            copy = pltpu.make_async_remote_copy(
                block, block, fs.at[d - 1, e - 1], fr.at[d - 1, e - 1],
                device_id={"sub": lax.rem(s + e, S)}, device_id_type=MESH)
            copy.start()
            forward.append(copy)
    for copy in across:
        copy.wait_send()
    for copy in spreads + partner + forward:
        copy.wait()
    for copy in local:
        copy.wait()


def gather(v, R, X, S):
    m, kd = v.shape
    dma = pltpu.SemaphoreType.DMA
    return pl.pallas_call(
        functools.partial(gather_kernel, R, X, S),
        out_shape=(
            jax.ShapeDtypeStruct((m, kd * X * S), v.dtype),
            jax.ShapeDtypeStruct((R, m // R, kd), v.dtype),
        ),
        in_specs=[pl.BlockSpec(memory_space=pltpu.VMEM)],
        out_specs=(pl.BlockSpec(memory_space=pl.ANY), pl.BlockSpec(memory_space=pl.ANY)),
        scratch_shapes=[
            dma((2,)), dma((X - 1,)), dma((X - 1,)), dma((R - 1,)), dma((R - 1,)),
            dma((S - 1,)), dma((S - 1,)), dma((X - 1, S - 1)), dma((X - 1, S - 1)),
        ],
        compiler_params=pltpu.CompilerParams(collective_id=0, has_side_effects=True),
        cost_estimate=pl.CostEstimate(flops=0, bytes_accessed=100_000_000, transcendentals=0),
        name="gather",
    )(v)


def regroup_kernel(X, S, spread, mine, lsem, ss, rs):
    x, s = lax.axis_index("col"), lax.axis_index("sub")
    C = X * S
    k = x * S + s
    R, piece, kd = spread.shape
    per = R // C
    barrier = pltpu.get_barrier_semaphore()
    dests = [lax.rem(k + e, C) for e in range(C)]
    for j in dests[1:]:
        pl.semaphore_signal(
            barrier, inc=1, device_id={"col": j // S, "sub": lax.rem(j, S)}, device_id_type=MESH)
    pl.semaphore_wait(barrier, C - 1)
    target = mine.at[:, :, pl.ds(pl.multiple_of(k * kd, kd), kd)]
    copies = []
    for e in range(1, C):
        j = dests[e]
        copies.append(pltpu.make_async_remote_copy(
            spread.at[pl.ds(j * per, per)], target, ss.at[e - 1], rs.at[e - 1],
            device_id={"col": j // S, "sub": lax.rem(j, S)}, device_id_type=MESH))
    copies.append(pltpu.make_async_copy(spread.at[pl.ds(k * per, per)], target, lsem))
    for copy in copies:
        copy.start()
    for copy in copies:
        copy.wait()


def regroup(spread, X, S):
    R, piece, kd = spread.shape
    C = X * S
    dma = pltpu.SemaphoreType.DMA
    return pl.pallas_call(
        functools.partial(regroup_kernel, X, S),
        out_shape=jax.ShapeDtypeStruct((R // C, piece, kd * C), spread.dtype),
        in_specs=[pl.BlockSpec(memory_space=pltpu.VMEM)],
        out_specs=pl.BlockSpec(memory_space=pl.ANY),
        scratch_shapes=[dma, dma((C - 1,)), dma((C - 1,))],
        compiler_params=pltpu.CompilerParams(collective_id=1, has_side_effects=True),
        cost_estimate=pl.CostEstimate(flops=0, bytes_accessed=60_000_000, transcendentals=0),
        name="regroup",
    )(spread)


def project_kernel(R, X, S, p, out, acc, from_sub, from_col, from_row, res, from_pair,
                   a_s, a_r, b_s, b_r, c_s, c_r, d_s, d_r):
    r, x, s = lax.axis_index("row"), lax.axis_index("col"), lax.axis_index("sub")
    K = p.shape[0]
    rb, kd = K // R, K // (X * S)

    def rows(i):
        return pl.ds(pl.multiple_of(i * rb, rb), rb)

    def columns(cx, cs):
        return pl.ds(pl.multiple_of((cx * S + cs) * kd, kd), kd)

    def col(d):
        return lax.rem(x + d, X)

    peers = [{"col": col(d)} for d in range(1, X)]
    peers += [{"row": lax.rem(r + d, R)} for d in range(1, R)]
    peers += [{"sub": lax.rem(s + d, S)} for d in range(1, S)]
    barrier = pltpu.get_barrier_semaphore()
    for peer in peers:
        pl.semaphore_signal(barrier, inc=1, device_id=peer, device_id_type=MESH)
    pl.semaphore_wait(barrier, len(peers))

    order = list(range(1, X)) + [0]
    steps = list(range(1, R)) + [0]
    pair = {}
    for d in order:
        for e in range(1, S):
            other = lax.rem(s + e, S)
            pair[d, e] = pltpu.make_async_remote_copy(
                p.at[:, columns(col(d), other)], from_sub.at[e - 1, d],
                a_s.at[e - 1, d], a_r.at[e - 1, d],
                device_id={"sub": other}, device_id_type=MESH)
            pair[d, e].start()
    cross = {}
    for d in order:
        for e in range(1, S):
            pair[d, e].wait_recv()
        for q in steps:
            here = rows(lax.rem(r + q, R))
            total = p[here, columns(col(d), s)]
            for e in range(1, S):
                total = total + from_sub[e - 1, d, here, :]
            acc[d, here, :] = total
            if d > 0:
                cross[d, q] = pltpu.make_async_remote_copy(
                    acc.at[d, here], from_col.at[d - 1, here],
                    b_s.at[d - 1, q], b_r.at[d - 1, q],
                    device_id={"col": col(d)}, device_id_type=MESH)
                cross[d, q].start()
    along = []
    for q in steps:
        i = lax.rem(r + q, R)
        here = rows(i)
        total = acc[0, here, :]
        for d in range(1, X):
            cross[d, q].wait_recv()
            total = total + from_col[d - 1, here, :]
        if q > 0:
            acc[0, here, :] = total
            copy = pltpu.make_async_remote_copy(
                acc.at[0, here], from_row.at[q - 1], c_s.at[q - 1], c_r.at[q - 1],
                device_id={"row": i}, device_id_type=MESH)
            copy.start()
            along.append(copy)
    for q in range(1, R):
        along[q - 1].wait_recv()
        total = total + from_row[q - 1]
    res[...] = total
    last = []
    for e in range(1, S):
        copy = pltpu.make_async_remote_copy(
            res, from_pair.at[e - 1], d_s.at[e - 1], d_r.at[e - 1],
            device_id={"sub": lax.rem(s + e, S)}, device_id_type=MESH)
        copy.start()
        last.append(copy)
    out[:, pl.ds(pl.multiple_of(s * kd, kd), kd)] = total
    for e in range(1, S):
        last[e - 1].wait_recv()
        out[:, pl.ds(pl.multiple_of(lax.rem(s - e + S, S) * kd, kd), kd)] = from_pair[e - 1]
    for copy in list(pair.values()) + list(cross.values()) + along + last:
        copy.wait_send()


def project(partial, R, X, S):
    K = partial.shape[0]
    rb, kd = K // R, K // (X * S)
    dma = pltpu.SemaphoreType.DMA
    f32 = jnp.float32
    return pl.pallas_call(
        functools.partial(project_kernel, R, X, S),
        out_shape=jax.ShapeDtypeStruct((rb, S * kd), f32),
        in_specs=[pl.BlockSpec(memory_space=pltpu.VMEM)],
        out_specs=pl.BlockSpec(memory_space=pltpu.VMEM),
        scratch_shapes=[
            pltpu.VMEM((X, K, kd), f32),
            pltpu.VMEM((S - 1, X, K, kd), f32),
            pltpu.VMEM((X - 1, K, kd), f32),
            pltpu.VMEM((R - 1, rb, kd), f32),
            pltpu.VMEM((rb, kd), f32),
            pltpu.VMEM((S - 1, rb, kd), f32),
            dma((S - 1, X)), dma((S - 1, X)), dma((X - 1, R)), dma((X - 1, R)),
            dma((R - 1,)), dma((R - 1,)), dma((S - 1,)), dma((S - 1,)),
        ],
        compiler_params=pltpu.CompilerParams(collective_id=2, has_side_effects=True),
        cost_estimate=pl.CostEstimate(flops=0, bytes_accessed=60_000_000, transcendentals=0),
        name="project",
    )(partial)


def split(value):
    high = value.astype(jnp.bfloat16)
    return high, (value - high.astype(jnp.float32)).astype(jnp.bfloat16)


def dot3(a_high, a_low, b_high, b_low, contract):
    def one(a, b):
        return lax.dot_general(a, b, ((contract, (0,)), ((), ())),
                               preferred_element_type=jnp.float32)
    return one(a_high, b_high) + (one(a_high, b_low) + one(a_low, b_high))


def owners(R, S):
    blocks, chips, columns = [], {}, {}
    pairs = [(i, i) for i in range(R)]
    pairs += sorted(((i, j) for i in range(R) for j in range(i + 1, R)), key=lambda p: (p[0] - p[1], p))
    for i, j in pairs:
        choices = [(j // S, i), (i // S, j)]
        best = min(choices, key=lambda o: (chips.get(o, 0), columns.get(o[0], 0)))
        slot = chips.get(best, 0)
        chips[best] = slot + 1
        columns[best[0]] = columns.get(best[0], 0) + 1
        blocks.append((i, j, best[0], best[1], slot))
    return blocks[R:] + blocks[:R], max(chips.values())


def reduce_blocks(R, S, blocks, out, ybuf, part, r_sub, r_col, r_row, flip, tile_ref,
                  ps, pr, qs, qr, us, ur, gs, gr, es, er):
    z, x, s = lax.axis_index("row"), lax.axis_index("col"), lax.axis_index("sub")
    other = 1 - s
    kd = part.shape[1]
    hr = kd // S
    mine = pl.ds(pl.multiple_of(s * hr, hr), hr)
    theirs = pl.ds(pl.multiple_of(other * hr, hr), hr)

    def held(g):
        return pl.ds(pl.multiple_of((jnp.where(x == g // S, 0, 1) * S + g % S) * kd, kd), kd)

    def swap(t):
        return pltpu.make_async_remote_copy(
            part.at[t, theirs, :], r_sub.at[t], ps.at[t], pr.at[t],
            device_id={"sub": other}, device_id_type=MESH)

    def cross(t):
        return pltpu.make_async_remote_copy(
            part.at[t, mine, :], r_col.at[t], qs.at[t], qr.at[t],
            device_id={"col": 1 - x}, device_id_type=MESH)

    def along(t, sender):
        return pltpu.make_async_remote_copy(
            part.at[t, mine, :], r_row.at[sender, blocks[t][4]], us.at[t], ur.at[sender, blocks[t][4]],
            device_id={"row": blocks[t][3]}, device_id_type=MESH)

    def region(t, direct):
        i, j = blocks[t][:2]
        if direct:
            return tile_ref.at[j % S, mine, :]
        return tile_ref.at[i % S, :, mine]

    def chip(t, direct):
        i, j = blocks[t][:2]
        return (j // S, i) if direct else (i // S, j)

    def far(t, direct):
        xo, zo = chip(t, direct)
        return pltpu.make_async_remote_copy(
            part.at[t, mine, :] if direct else flip.at[t], region(t, direct), gs.at[t], gr.at[t],
            device_id={"col": xo, "row": zo}, device_id_type=MESH)

    def near(t, direct):
        slot = blocks[t][1] % S if direct else blocks[t][0] % S
        return pltpu.make_async_remote_copy(
            region(t, direct), region(t, direct), es.at[slot], er.at[slot],
            device_id={"sub": other}, device_id_type=MESH)

    for t, (i, j, xo, zo, slot) in enumerate(blocks):
        part[t] = ybuf[held(i), held(j)] + ybuf[held(j), held(i)].T
        swap(t).start()
    for t, (i, j, xo, zo, slot) in enumerate(blocks):
        swap(t).wait_recv()
        part[t, mine, :] += r_sub[t]

        @pl.when(x != xo)
        def _():
            cross(t).start()
    for t, (i, j, xo, zo, slot) in enumerate(blocks):
        @pl.when(x == xo)
        def _():
            cross(t).wait_recv()
            part[t, mine, :] += r_col[t]

            @pl.when(z != zo)
            def _():
                along(t, z).start()
    for t, (i, j, xo, zo, slot) in enumerate(blocks):
        straight = (xo, zo) == (j // S, i)

        @pl.when((x == xo) & (z == zo))
        def _():
            for q in range(R):
                if q != zo:
                    along(t, q).wait_recv()
                    part[t, mine, :] += r_row[q, slot]
            value = part[t, mine, :]
            if i != j:
                flip[t] = value.T
                far(t, not straight).start()
            if straight:
                tile_ref[j % S, mine, :] = value
            else:
                tile_ref[i % S, :, mine] = value.T
            near(t, straight).start()
    for t, (i, j, xo, zo, slot) in enumerate(blocks):
        straight = (xo, zo) == (j // S, i)
        if i != j:
            xf, zf = chip(t, not straight)

            @pl.when((x == xf) & (z == zf))
            def _():
                far(t, not straight).wait_recv()
                near(t, not straight).start()
    for t, (i, j, xo, zo, slot) in enumerate(blocks):
        straight = (xo, zo) == (j // S, i)
        swap(t).wait_send()

        @pl.when(x != xo)
        def _():
            cross(t).wait_send()

        @pl.when((x == xo) & (z != zo))
        def _():
            along(t, z).wait_send()
        for direct in ((straight, not straight) if i != j else (straight,)):
            xn, zn = chip(t, direct)

            @pl.when((x == xn) & (z == zn))
            def _():
                near(t, direct).wait()
        if i != j:
            @pl.when((x == xo) & (z == zo))
            def _():
                far(t, not straight).wait_send()
    for b in range(S):
        out[:, b * kd:(b + 1) * kd] = tile_ref[b]


def image_kernel(R, S, Q, blocks, v, a, out, vall, img, ybuf, sbuf, ubuf, tbuf, abuf, ahi, alo, vhi, vlo,
                 ihi, ilo, rhi, rlo, lsem, asem, os, orr, xs, xr, fs, fr, hs, hr, ts, tr,
                 part, r_sub, r_col, r_row, flip, tile_ref, ps, pr, qs, qr, us, ur, gs, gr, es, er):
    z, x, s = lax.axis_index("row"), lax.axis_index("col"), lax.axis_index("sub")
    c = x * S + s
    m, kd = v.shape
    half = S * kd
    steps = m // abuf.shape[2]
    w = m // steps
    pw = w // Q
    first = jnp.where(x == 0, c, 0)
    last = jnp.where(x == 0, R - 1, c)
    chained = (z >= first) & (z <= last)
    diag = z == c
    pair = (z == x * S + 1) & (s == 0)
    relay = (z == x * S) & (s == 1 - x)
    adds = (x == 1) & chained
    weight = jnp.where(diag, 0.5, 1.0).astype(jnp.float32)
    other = 1 - s

    def rows(i, n):
        return pl.ds(pl.multiple_of(i * n, n), n)

    def block(hh, ss):
        return pl.ds(pl.multiple_of((hh * S + ss) * kd, kd), kd)

    barrier = pltpu.get_barrier_semaphore()
    pl.semaphore_signal(barrier, inc=1, device_id={"sub": other}, device_id_type=MESH)
    for q in range(R):
        if q > 0:
            pl.semaphore_signal(barrier, inc=1, device_id={"row": lax.rem(z + q, R)}, device_id_type=MESH)
        pl.semaphore_signal(barrier, inc=1, device_id={"col": 1 - x, "row": q}, device_id_type=MESH)

    @pl.when(z > 0)
    def _():
        pl.semaphore_signal(barrier, inc=1, device_id={"row": z - 1, "sub": other}, device_id_type=MESH)

    @pl.when(z < R - 1)
    def _():
        pl.semaphore_signal(barrier, inc=1, device_id={"row": z + 1, "sub": other}, device_id_type=MESH)

    def load(i):
        return pltpu.make_async_copy(a.at[:, rows(i, w)], abuf.at[lax.rem(i, 2)], asem.at[lax.rem(i, 2)])

    def mate():
        return pltpu.make_async_remote_copy(
            v, vall.at[:, block(0, s)], os, orr, device_id={"sub": other}, device_id_type=MESH)

    def across(i):
        return pltpu.make_async_remote_copy(
            v.at[rows(i, w), :], vall.at[rows(i, w), block(1, s)], xs.at[i], xr.at[i],
            device_id={"col": 1 - x}, device_id_type=MESH)

    def share(i):
        here = vall.at[rows(i, w), block(1, s)]
        return pltpu.make_async_remote_copy(
            here, here, fs.at[i], fr.at[i], device_id={"sub": other}, device_id_type=MESH)

    def hand(i):
        return pltpu.make_async_remote_copy(
            vall.at[rows(i, w), pl.ds(half, half)], ubuf.at[rows(i, w), :], hs.at[i], hr.at[i],
            device_id={"row": z + 1, "sub": 0}, device_id_type=MESH)

    def origin(k):
        return pltpu.make_async_remote_copy(
            vall.at[rows(k, pw), pl.ds(0, half)], sbuf.at[rows(k, pw), :], ts.at[k], tr.at[k],
            device_id={"row": z + 1}, device_id_type=MESH)

    def onward(k):
        return pltpu.make_async_remote_copy(
            sbuf.at[rows(k, pw), :], sbuf.at[rows(k, pw), :], ts.at[k], tr.at[k],
            device_id={"row": z + 1}, device_id_type=MESH)

    own = pltpu.make_async_copy(v, vall.at[:, block(0, s)], lsem)
    own.start()
    load(0).start()
    img[...] = jnp.zeros_like(img)
    ybuf[...] = jnp.zeros_like(ybuf)
    pl.semaphore_wait(barrier, 2 * R + (z > 0).astype(jnp.int32) + (z < R - 1).astype(jnp.int32))
    mate().start()

    def begin(i, carry):
        across(i).start()
        return carry

    lax.fori_loop(0, steps, begin, 0)
    own.wait()
    mate().wait_recv()
    source = (x == 0) & diag

    @pl.when(source)
    def _():
        def send(k, carry):
            origin(k).start()
            return carry
        lax.fori_loop(0, steps * Q, send, 0)

    def prepare(i, hh):
        here, columns = rows(i, w), pl.ds(hh * half, half)
        high, low = split(vall[here, columns])
        vhi[here, columns] = high
        vlo[here, columns] = low

    def prepare_own(i, carry):
        prepare(i, 0)
        return carry

    lax.fori_loop(0, steps, prepare_own, 0)

    def multiply(columns):
        def tile(t, carry):
            here = rows(t, w)
            img[here, columns] += dot3(ahi[here, :], alo[here, :], rhi[...], rlo[...], (1,))
            return carry
        lax.fori_loop(0, steps, tile, 0)

    def feed(value):
        high, low = split(value)
        rhi[...] = high
        rlo[...] = low

    def open_block(i):
        load(i).wait()

        @pl.when(i < steps - 1)
        def _():
            load(i + 1).start()

        def cut(t, carry):
            high, low = split(abuf[lax.rem(i, 2), rows(t, w), :])
            ahi[rows(t, w), :] = high
            alo[rows(t, w), :] = low
            return carry
        lax.fori_loop(0, steps, cut, 0)

    def receive(i):
        across(i).wait_recv()
        share(i).start()

    def collect(i):
        share(i).wait_recv()
        prepare(i, 1)

        @pl.when(relay)
        def _():
            hand(i).start()

    def fold(hh):
        columns = pl.ds(hh * half, half)

        def halve(t, carry):
            high, low = split(img[rows(t, w), columns])
            ihi[rows(t, w), :] = high
            ilo[rows(t, w), :] = low
            return carry
        lax.fori_loop(0, steps, halve, 0)
        for b in range(2 * S):
            part = slice(b * kd, (b + 1) * kd)
            ybuf[part, columns] = dot3(vhi[:, part], vlo[:, part], ihi[...], ilo[...], (0,))

    def local_step(i, carry):
        receive(i)
        open_block(i)

        @pl.when(x == 0)
        def _():
            feed(0.5 * vall[rows(i, w), pl.ds(0, half)])
            multiply(pl.ds(0, half))
        collect(i)
        feed(0.5 * vall[rows(i, w), pl.ds(half, half)])
        multiply(pl.ds(half, half))
        return carry

    def stream_step(i, carry):
        @pl.when(jnp.logical_not(diag) & (2 * i < steps))
        def _():
            receive(2 * i)
            receive(2 * i + 1)

        open_block(i)

        @pl.when(adds)
        def _():
            tbuf[...] = weight * dot3(ahi[...], alo[...], vhi[:, :half], vlo[:, :half], (0,))

        def piece(p, carry):
            k = i * Q + p

            @pl.when(chained & (z > first))
            def _():
                onward(k).wait_recv()

            @pl.when(adds & (z == first))
            def _():
                sbuf[rows(k, pw), :] = tbuf[rows(p, pw), :]

            @pl.when(adds & (z > first))
            def _():
                sbuf[rows(k, pw), :] += tbuf[rows(p, pw), :]

            @pl.when(chained & (z < last))
            def _():
                onward(k).start()
            return carry
        lax.fori_loop(0, Q, piece, 0)

        lag = jnp.where(relay, 0, steps // 2)

        @pl.when(jnp.logical_not(diag) & (i >= lag) & (2 * (i - lag) < steps))
        def _():
            collect(2 * (i - lag))
            collect(2 * (i - lag) + 1)

        @pl.when((x == 0) & chained)
        def _():
            feed(sbuf[rows(i, w), :])
            multiply(pl.ds(0, half))

        @pl.when((x == 1) & diag)
        def _():
            feed(sbuf[rows(i, w), :])
            for b in range(2 * S):
                part = slice(b * kd, (b + 1) * kd)
                ybuf[part, :half] += dot3(vhi[rows(i, w), part], vlo[rows(i, w), part], rhi[...], rlo[...], (0,))

        @pl.when(pair)
        def _():
            hand(i).wait_recv()
            feed(ubuf[rows(i, w), :])
            multiply(pl.ds(half, half))
        return carry

    @pl.when(diag)
    def _():
        lax.fori_loop(0, steps, local_step, 0)
        fold(1)

        @pl.when(x == 0)
        def _():
            fold(0)

        @pl.when(x == 1)
        def _():
            load(0).start()

    @pl.when(jnp.logical_not(source))
    def _():
        lax.fori_loop(0, steps, stream_step, 0)

    @pl.when(pair)
    def _():
        fold(1)

    @pl.when((x == 0) & chained & jnp.logical_not(diag))
    def _():
        fold(0)

    reduce_blocks(R, S, blocks, out, ybuf, part, r_sub, r_col, r_row, flip, tile_ref,
                  ps, pr, qs, qr, us, ur, gs, gr, es, er)
    mate().wait_send()

    def drain(i, carry):
        across(i).wait_send()
        share(i).wait_send()

        @pl.when(relay)
        def _():
            hand(i).wait_send()
        return carry

    lax.fori_loop(0, steps, drain, 0)

    def sent(k, carry):
        @pl.when(source)
        def _():
            origin(k).wait_send()

        @pl.when(chained & (z < last) & jnp.logical_not(source))
        def _():
            onward(k).wait_send()
        return carry

    lax.fori_loop(0, steps * Q, sent, 0)


def image(v, a, R, S):
    m, kd = v.shape
    w = kd
    steps = m // w
    Q = 4
    half = S * kd
    dma = pltpu.SemaphoreType.DMA
    f32, bf16 = jnp.float32, jnp.bfloat16
    blocks, most = owners(R, S)
    nb, hr = len(blocks), kd // S
    return pl.pallas_call(
        functools.partial(image_kernel, R, S, Q, blocks),
        out_shape=jax.ShapeDtypeStruct((kd, half), f32),
        in_specs=[pl.BlockSpec(memory_space=pltpu.VMEM), pl.BlockSpec(memory_space=pl.ANY)],
        out_specs=pl.BlockSpec(memory_space=pltpu.VMEM),
        scratch_shapes=[
            pltpu.VMEM((m, 2 * half), f32), pltpu.VMEM((m, 2 * half), f32),
            pltpu.VMEM((2 * half, 2 * half), f32),
            pltpu.VMEM((m, half), f32), pltpu.VMEM((m, half), f32), pltpu.VMEM((w, half), f32),
            pltpu.VMEM((2, m, w), f32), pltpu.VMEM((m, w), bf16), pltpu.VMEM((m, w), bf16),
            pltpu.VMEM((m, 2 * half), bf16), pltpu.VMEM((m, 2 * half), bf16),
            pltpu.VMEM((m, half), bf16), pltpu.VMEM((m, half), bf16),
            pltpu.VMEM((w, half), bf16), pltpu.VMEM((w, half), bf16),
            dma, dma((2,)), dma, dma, dma((steps,)), dma((steps,)), dma((steps,)), dma((steps,)),
            dma((steps,)), dma((steps,)), dma((steps * Q,)), dma((steps * Q,)),
            pltpu.VMEM((nb, kd, kd), f32), pltpu.VMEM((nb, hr, kd), f32), pltpu.VMEM((nb, hr, kd), f32),
            pltpu.VMEM((R, most, hr, kd), f32), pltpu.VMEM((nb, kd, hr), f32), pltpu.VMEM((S, kd, kd), f32),
            dma((nb,)), dma((nb,)), dma((nb,)), dma((nb,)), dma((nb,)), dma((R, most)),
            dma((nb,)), dma((nb,)), dma((S,)), dma((S,)),
        ],
        compiler_params=pltpu.CompilerParams(
            collective_id=3, has_side_effects=True, vmem_limit_bytes=64_000_000),
        cost_estimate=pl.CostEstimate(flops=0, bytes_accessed=100_000_000, transcendentals=0),
        name="image",
    )(v, a)


def partial_general(matrix, basis_vectors):
    R = lax.axis_size("row")
    S = lax.axis_size("sub")
    C = lax.axis_size("col") * S
    m, kd = basis_vectors.shape
    K = kd * C
    n = matrix.shape[1]
    per = n // m
    piece = m // R
    own, spread = gather(basis_vectors, R, C // S, S)
    width = K // CHUNKS
    images = []
    for c in range(CHUNKS):
        part = lax.dot_general(
            matrix,
            own[:, c * width : (c + 1) * width],
            (((0,), (0,)), ((), ())),
            precision=lax.Precision.HIGH,
            preferred_element_type=jnp.float32,
        )
        if c == 0:
            part, spread = lax.optimization_barrier((part, spread))
        part = part.reshape(per, R, piece, width).transpose(1, 0, 2, 3).reshape(R * per * piece, width)
        images.append(lax.psum_scatter(part, "row", scatter_dimension=0, tiled=True))
    mine = regroup(spread, C // S, S).reshape(per * piece, K)
    return jnp.concatenate(
        [
            lax.dot_general(
                mine,
                image,
                (((0,), (0,)), ((), ())),
                precision=lax.Precision.HIGH,
                preferred_element_type=jnp.float32,
            )
            for image in images
        ],
        axis=1,
    )


def shards(matrix, basis_vectors, split_size):
    R = lax.axis_size("row")
    X = lax.axis_size("col")
    S = lax.axis_size("sub")
    m, n = matrix.shape
    halves = m == n and R == X * S and X == 2 and S == 2
    if halves:
        child_block = image(basis_vectors, matrix, R, S)
    else:
        child_block = project(partial_general(matrix, basis_vectors), R, X, S)
    row_ids = (
        jnp.arange(child_block.shape[0], dtype=jnp.int32)
        + lax.axis_index("row") * child_block.shape[0]
    )
    col_ids = (
        jnp.arange(child_block.shape[1], dtype=jnp.int32)
        + lax.axis_index("col") * child_block.shape[1]
    )
    leading = split_size[0]
    row_first = row_ids < leading
    col_first = col_ids < leading
    mask_one = row_first[:, None] & col_first[None, :]
    mask_two = jnp.logical_not(row_first)[:, None] & jnp.logical_not(col_first)[None, :]
    selected = jnp.where(lax.axis_index("sub") == 0, mask_one, mask_two)
    return jnp.where(selected, child_block, jnp.zeros((), jnp.float32))[None]


def solution(mesh):
    placed = (
        P(("groups", "row"), ("col", "sub")),
        P(("groups", "row"), ("col", "sub")),
        P("groups"),
    )
    return jax.shard_map(
        shards,
        mesh=mesh,
        in_specs=placed,
        out_specs=P("sub", ("groups", "row"), "col"),
        check_vma=False,
    )
```

```python
import functools

import jax
import jax.numpy as jnp
from jax import lax
from jax.experimental import pallas as pl
from jax.experimental.pallas import tpu as pltpu
from jax.sharding import PartitionSpec as P

MESH = pl.DeviceIdType.MESH
CHUNKS = 1


def gather_kernel(R, X, S, v, own, spread, lsem, xs, xr, zs, zr, ps, pr, fs, fr):
    r, x, s = lax.axis_index("row"), lax.axis_index("col"), lax.axis_index("sub")
    m, kd = v.shape
    piece = m // R

    def columns(cx, cs):
        return pl.ds(pl.multiple_of((cx * S + cs) * kd, kd), kd)

    peers = [{"col": lax.rem(x + d, X)} for d in range(1, X)]
    peers += [{"row": lax.rem(r + d, R)} for d in range(1, R)]
    peers += [{"sub": lax.rem(s + d, S)} for d in range(1, S)]
    barrier = pltpu.get_barrier_semaphore()
    for peer in peers:
        pl.semaphore_signal(barrier, inc=1, device_id=peer, device_id_type=MESH)
    pl.semaphore_wait(barrier, len(peers))

    mine = own.at[:, columns(x, s)]
    across, spreads, partner, forward = [], [], [], []
    for d in range(1, X):
        across.append(pltpu.make_async_remote_copy(
            v, mine, xs.at[d - 1], xr.at[d - 1],
            device_id={"col": lax.rem(x + d, X)}, device_id_type=MESH))
    for d in range(1, R):
        i = lax.rem(r + d, R)
        spreads.append(pltpu.make_async_remote_copy(
            v.at[pl.ds(pl.multiple_of(i * piece, piece), piece), :], spread.at[r],
            zs.at[d - 1], zr.at[d - 1],
            device_id={"row": i}, device_id_type=MESH))
    for d in range(1, S):
        partner.append(pltpu.make_async_remote_copy(
            v, mine, ps.at[d - 1], pr.at[d - 1],
            device_id={"sub": lax.rem(s + d, S)}, device_id_type=MESH))
    for copy in across + spreads + partner:
        copy.start()
    local = [
        pltpu.make_async_copy(v, mine, lsem.at[0]),
        pltpu.make_async_copy(
            v.at[pl.ds(pl.multiple_of(r * piece, piece), piece), :], spread.at[r], lsem.at[1]),
    ]
    for copy in local:
        copy.start()
    for d in range(1, X):
        across[d - 1].wait_recv()
        block = own.at[:, columns(lax.rem(x - d + X, X), s)]
        for e in range(1, S):
            copy = pltpu.make_async_remote_copy(
                block, block, fs.at[d - 1, e - 1], fr.at[d - 1, e - 1],
                device_id={"sub": lax.rem(s + e, S)}, device_id_type=MESH)
            copy.start()
            forward.append(copy)
    for copy in across:
        copy.wait_send()
    for copy in spreads + partner + forward:
        copy.wait()
    for copy in local:
        copy.wait()


def gather(v, R, X, S):
    m, kd = v.shape
    dma = pltpu.SemaphoreType.DMA
    return pl.pallas_call(
        functools.partial(gather_kernel, R, X, S),
        out_shape=(
            jax.ShapeDtypeStruct((m, kd * X * S), v.dtype),
            jax.ShapeDtypeStruct((R, m // R, kd), v.dtype),
        ),
        in_specs=[pl.BlockSpec(memory_space=pltpu.VMEM)],
        out_specs=(pl.BlockSpec(memory_space=pl.ANY), pl.BlockSpec(memory_space=pl.ANY)),
        scratch_shapes=[
            dma((2,)), dma((X - 1,)), dma((X - 1,)), dma((R - 1,)), dma((R - 1,)),
            dma((S - 1,)), dma((S - 1,)), dma((X - 1, S - 1)), dma((X - 1, S - 1)),
        ],
        compiler_params=pltpu.CompilerParams(collective_id=0, has_side_effects=True),
        cost_estimate=pl.CostEstimate(flops=0, bytes_accessed=100_000_000, transcendentals=0),
        name="gather",
    )(v)


def regroup_kernel(X, S, spread, mine, lsem, ss, rs):
    x, s = lax.axis_index("col"), lax.axis_index("sub")
    C = X * S
    k = x * S + s
    R, piece, kd = spread.shape
    per = R // C
    barrier = pltpu.get_barrier_semaphore()
    dests = [lax.rem(k + e, C) for e in range(C)]
    for j in dests[1:]:
        pl.semaphore_signal(
            barrier, inc=1, device_id={"col": j // S, "sub": lax.rem(j, S)}, device_id_type=MESH)
    pl.semaphore_wait(barrier, C - 1)
    target = mine.at[:, :, pl.ds(pl.multiple_of(k * kd, kd), kd)]
    copies = []
    for e in range(1, C):
        j = dests[e]
        copies.append(pltpu.make_async_remote_copy(
            spread.at[pl.ds(j * per, per)], target, ss.at[e - 1], rs.at[e - 1],
            device_id={"col": j // S, "sub": lax.rem(j, S)}, device_id_type=MESH))
    copies.append(pltpu.make_async_copy(spread.at[pl.ds(k * per, per)], target, lsem))
    for copy in copies:
        copy.start()
    for copy in copies:
        copy.wait()


def regroup(spread, X, S):
    R, piece, kd = spread.shape
    C = X * S
    dma = pltpu.SemaphoreType.DMA
    return pl.pallas_call(
        functools.partial(regroup_kernel, X, S),
        out_shape=jax.ShapeDtypeStruct((R // C, piece, kd * C), spread.dtype),
        in_specs=[pl.BlockSpec(memory_space=pltpu.VMEM)],
        out_specs=pl.BlockSpec(memory_space=pl.ANY),
        scratch_shapes=[dma, dma((C - 1,)), dma((C - 1,))],
        compiler_params=pltpu.CompilerParams(collective_id=1, has_side_effects=True),
        cost_estimate=pl.CostEstimate(flops=0, bytes_accessed=60_000_000, transcendentals=0),
        name="regroup",
    )(spread)


def project_kernel(R, X, S, p, out, acc, from_sub, from_col, from_row, res, from_pair,
                   a_s, a_r, b_s, b_r, c_s, c_r, d_s, d_r):
    r, x, s = lax.axis_index("row"), lax.axis_index("col"), lax.axis_index("sub")
    K = p.shape[0]
    rb, kd = K // R, K // (X * S)

    def rows(i):
        return pl.ds(pl.multiple_of(i * rb, rb), rb)

    def columns(cx, cs):
        return pl.ds(pl.multiple_of((cx * S + cs) * kd, kd), kd)

    def col(d):
        return lax.rem(x + d, X)

    peers = [{"col": col(d)} for d in range(1, X)]
    peers += [{"row": lax.rem(r + d, R)} for d in range(1, R)]
    peers += [{"sub": lax.rem(s + d, S)} for d in range(1, S)]
    barrier = pltpu.get_barrier_semaphore()
    for peer in peers:
        pl.semaphore_signal(barrier, inc=1, device_id=peer, device_id_type=MESH)
    pl.semaphore_wait(barrier, len(peers))

    order = list(range(1, X)) + [0]
    steps = list(range(1, R)) + [0]
    pair = {}
    for d in order:
        for e in range(1, S):
            other = lax.rem(s + e, S)
            pair[d, e] = pltpu.make_async_remote_copy(
                p.at[:, columns(col(d), other)], from_sub.at[e - 1, d],
                a_s.at[e - 1, d], a_r.at[e - 1, d],
                device_id={"sub": other}, device_id_type=MESH)
            pair[d, e].start()
    cross = {}
    for d in order:
        for e in range(1, S):
            pair[d, e].wait_recv()
        for q in steps:
            here = rows(lax.rem(r + q, R))
            total = p[here, columns(col(d), s)]
            for e in range(1, S):
                total = total + from_sub[e - 1, d, here, :]
            acc[d, here, :] = total
            if d > 0:
                cross[d, q] = pltpu.make_async_remote_copy(
                    acc.at[d, here], from_col.at[d - 1, here],
                    b_s.at[d - 1, q], b_r.at[d - 1, q],
                    device_id={"col": col(d)}, device_id_type=MESH)
                cross[d, q].start()
    along = []
    for q in steps:
        i = lax.rem(r + q, R)
        here = rows(i)
        total = acc[0, here, :]
        for d in range(1, X):
            cross[d, q].wait_recv()
            total = total + from_col[d - 1, here, :]
        if q > 0:
            acc[0, here, :] = total
            copy = pltpu.make_async_remote_copy(
                acc.at[0, here], from_row.at[q - 1], c_s.at[q - 1], c_r.at[q - 1],
                device_id={"row": i}, device_id_type=MESH)
            copy.start()
            along.append(copy)
    for q in range(1, R):
        along[q - 1].wait_recv()
        total = total + from_row[q - 1]
    res[...] = total
    last = []
    for e in range(1, S):
        copy = pltpu.make_async_remote_copy(
            res, from_pair.at[e - 1], d_s.at[e - 1], d_r.at[e - 1],
            device_id={"sub": lax.rem(s + e, S)}, device_id_type=MESH)
        copy.start()
        last.append(copy)
    out[:, pl.ds(pl.multiple_of(s * kd, kd), kd)] = total
    for e in range(1, S):
        last[e - 1].wait_recv()
        out[:, pl.ds(pl.multiple_of(lax.rem(s - e + S, S) * kd, kd), kd)] = from_pair[e - 1]
    for copy in list(pair.values()) + list(cross.values()) + along + last:
        copy.wait_send()


def project(partial, R, X, S):
    K = partial.shape[0]
    rb, kd = K // R, K // (X * S)
    dma = pltpu.SemaphoreType.DMA
    f32 = jnp.float32
    return pl.pallas_call(
        functools.partial(project_kernel, R, X, S),
        out_shape=jax.ShapeDtypeStruct((rb, S * kd), f32),
        in_specs=[pl.BlockSpec(memory_space=pltpu.VMEM)],
        out_specs=pl.BlockSpec(memory_space=pltpu.VMEM),
        scratch_shapes=[
            pltpu.VMEM((X, K, kd), f32),
            pltpu.VMEM((S - 1, X, K, kd), f32),
            pltpu.VMEM((X - 1, K, kd), f32),
            pltpu.VMEM((R - 1, rb, kd), f32),
            pltpu.VMEM((rb, kd), f32),
            pltpu.VMEM((S - 1, rb, kd), f32),
            dma((S - 1, X)), dma((S - 1, X)), dma((X - 1, R)), dma((X - 1, R)),
            dma((R - 1,)), dma((R - 1,)), dma((S - 1,)), dma((S - 1,)),
        ],
        compiler_params=pltpu.CompilerParams(collective_id=2, has_side_effects=True),
        cost_estimate=pl.CostEstimate(flops=0, bytes_accessed=60_000_000, transcendentals=0),
        name="project",
    )(partial)


def split(value):
    high = value.astype(jnp.bfloat16)
    return high, (value - high.astype(jnp.float32)).astype(jnp.bfloat16)


def dot3(a_high, a_low, b_high, b_low, contract):
    def one(a, b):
        return lax.dot_general(a, b, ((contract, (0,)), ((), ())),
                               preferred_element_type=jnp.float32)
    return one(a_high, b_high) + (one(a_high, b_low) + one(a_low, b_high))


def owners(R, S):
    blocks, chips, columns = [], {}, {}
    pairs = [(i, i) for i in range(R)]
    pairs += sorted(((i, j) for i in range(R) for j in range(i + 1, R)), key=lambda p: (p[0] - p[1], p))
    for i, j in pairs:
        choices = [(j // S, i), (i // S, j)]
        best = min(choices, key=lambda o: (chips.get(o, 0), columns.get(o[0], 0)))
        slot = chips.get(best, 0)
        chips[best] = slot + 1
        columns[best[0]] = columns.get(best[0], 0) + 1
        blocks.append((i, j, best[0], best[1], slot))
    return blocks[R:] + blocks[:R], max(chips.values())


def reduce_blocks(R, S, blocks, out, ybuf, part, r_sub, r_col, r_row, flip, tile_ref,
                  ps, pr, qs, qr, us, ur, gs, gr, es, er):
    z, x, s = lax.axis_index("row"), lax.axis_index("col"), lax.axis_index("sub")
    other = 1 - s
    kd = part.shape[1]
    hr = kd // S
    mine = pl.ds(pl.multiple_of(s * hr, hr), hr)
    theirs = pl.ds(pl.multiple_of(other * hr, hr), hr)

    def filled(t, side):
        i, j = blocks[t][:2]
        inner = z // S == side
        return inner if side == 1 or min(i // S, j // S) > 0 else z >= 0

    def held(g):
        return pl.ds(pl.multiple_of((jnp.where(x == g // S, 0, 1) * S + g % S) * kd, kd), kd)

    def swap(t):
        return pltpu.make_async_remote_copy(
            part.at[t, theirs, :], r_sub.at[t], ps.at[t], pr.at[t],
            device_id={"sub": other}, device_id_type=MESH)

    def cross(t):
        return pltpu.make_async_remote_copy(
            part.at[t, mine, :], r_col.at[t], qs.at[t], qr.at[t],
            device_id={"col": 1 - x}, device_id_type=MESH)

    def along(t, sender):
        return pltpu.make_async_remote_copy(
            part.at[t, mine, :], r_row.at[sender, blocks[t][4]], us.at[t], ur.at[sender, blocks[t][4]],
            device_id={"row": blocks[t][3]}, device_id_type=MESH)

    def region(t, direct):
        i, j = blocks[t][:2]
        if direct:
            return tile_ref.at[j % S, mine, :]
        return tile_ref.at[i % S, :, mine]

    def chip(t, direct):
        i, j = blocks[t][:2]
        return (j // S, i) if direct else (i // S, j)

    def far(t, direct):
        xo, zo = chip(t, direct)
        return pltpu.make_async_remote_copy(
            part.at[t, mine, :] if direct else flip.at[t], region(t, direct), gs.at[t], gr.at[t],
            device_id={"col": xo, "row": zo}, device_id_type=MESH)

    def near(t, direct):
        slot = blocks[t][1] % S if direct else blocks[t][0] % S
        return pltpu.make_async_remote_copy(
            region(t, direct), region(t, direct), es.at[slot], er.at[slot],
            device_id={"sub": other}, device_id_type=MESH)

    for t, (i, j, xo, zo, slot) in enumerate(blocks):
        part[t] = ybuf[held(i), held(j)] + ybuf[held(j), held(i)].T
        swap(t).start()
    for t, (i, j, xo, zo, slot) in enumerate(blocks):
        swap(t).wait_recv()
        part[t, mine, :] += r_sub[t]

        @pl.when((x != xo) & filled(t, 1 - xo))
        def _():
            cross(t).start()
    for t, (i, j, xo, zo, slot) in enumerate(blocks):
        @pl.when((x == xo) & filled(t, 1 - xo))
        def _():
            cross(t).wait_recv()
            part[t, mine, :] += r_col[t]

        @pl.when((x == xo) & (z != zo))
        def _():
            along(t, z).start()
    for t, (i, j, xo, zo, slot) in enumerate(blocks):
        straight = (xo, zo) == (j // S, i)

        @pl.when((x == xo) & (z == zo))
        def _():
            for q in range(R):
                if q != zo:
                    along(t, q).wait_recv()
                    part[t, mine, :] += r_row[q, slot]
            value = part[t, mine, :]
            if i != j:
                flip[t] = value.T
                far(t, not straight).start()
            if straight:
                tile_ref[j % S, mine, :] = value
            else:
                tile_ref[i % S, :, mine] = value.T
            near(t, straight).start()
    for t, (i, j, xo, zo, slot) in enumerate(blocks):
        straight = (xo, zo) == (j // S, i)
        if i != j:
            xf, zf = chip(t, not straight)

            @pl.when((x == xf) & (z == zf))
            def _():
                far(t, not straight).wait_recv()
                near(t, not straight).start()
    for t, (i, j, xo, zo, slot) in enumerate(blocks):
        straight = (xo, zo) == (j // S, i)
        swap(t).wait_send()

        @pl.when((x != xo) & filled(t, 1 - xo))
        def _():
            cross(t).wait_send()

        @pl.when((x == xo) & (z != zo))
        def _():
            along(t, z).wait_send()
        for direct in ((straight, not straight) if i != j else (straight,)):
            xn, zn = chip(t, direct)

            @pl.when((x == xn) & (z == zn))
            def _():
                near(t, direct).wait()
        if i != j:
            @pl.when((x == xo) & (z == zo))
            def _():
                far(t, not straight).wait_send()
    for b in range(S):
        out[:, b * kd:(b + 1) * kd] = tile_ref[b]


def image_kernel(R, S, Q, blocks, v, a, out, vall, img, ybuf, sbuf, ubuf, tbuf, abuf, ahi, alo, vhi, vlo,
                 ihi, ilo, rhi, rlo, lsem, asem, os, orr, xs, xr, fs, fr, hs, hr, ts, tr,
                 part, r_sub, r_col, r_row, flip, tile_ref, ps, pr, qs, qr, us, ur, gs, gr, es, er):
    z, x, s = lax.axis_index("row"), lax.axis_index("col"), lax.axis_index("sub")
    c = x * S + s
    m, kd = v.shape
    half = S * kd
    steps = m // abuf.shape[2]
    w = m // steps
    pw = w // Q
    first = jnp.where(x == 0, c, 0)
    last = jnp.where(x == 0, R - 1, c)
    chained = (z >= first) & (z <= last)
    diag = z == c
    pair = (x == 1) & (z == x * S + 1) & (s == 0)
    catcher = (x == 0) & diag & (z == 1)
    relay = (x == 1) & (z == x * S) & (s == 1 - x)
    helper = (x == 0) & (z == 0) & (s == 1)
    adds = (x == 1) & chained
    weight = jnp.where(diag, 0.5, 1.0).astype(jnp.float32)
    other = 1 - s

    def rows(i, n):
        return pl.ds(pl.multiple_of(i * n, n), n)

    def block(hh, ss):
        return pl.ds(pl.multiple_of((hh * S + ss) * kd, kd), kd)

    barrier = pltpu.get_barrier_semaphore()
    pl.semaphore_signal(barrier, inc=1, device_id={"sub": other}, device_id_type=MESH)
    for q in range(R):
        if q > 0:
            pl.semaphore_signal(barrier, inc=1, device_id={"row": lax.rem(z + q, R)}, device_id_type=MESH)
        pl.semaphore_signal(barrier, inc=1, device_id={"col": 1 - x, "row": q}, device_id_type=MESH)

    @pl.when(z > 0)
    def _():
        pl.semaphore_signal(barrier, inc=1, device_id={"row": z - 1, "sub": other}, device_id_type=MESH)

    @pl.when(z < R - 1)
    def _():
        pl.semaphore_signal(barrier, inc=1, device_id={"row": z + 1, "sub": other}, device_id_type=MESH)

    def load(i):
        return pltpu.make_async_copy(a.at[:, rows(i, w)], abuf.at[lax.rem(i, 2)], asem.at[lax.rem(i, 2)])

    def mate():
        return pltpu.make_async_remote_copy(
            v, vall.at[:, block(0, s)], os, orr, device_id={"sub": other}, device_id_type=MESH)

    def across(i):
        return pltpu.make_async_remote_copy(
            v.at[rows(i, w), :], vall.at[rows(i, w), block(1, s)], xs.at[i], xr.at[i],
            device_id={"col": 1 - x}, device_id_type=MESH)

    def share(i):
        here = vall.at[rows(i, w), block(1, s)]
        return pltpu.make_async_remote_copy(
            here, here, fs.at[i], fr.at[i], device_id={"sub": other}, device_id_type=MESH)

    def hand(i):
        return pltpu.make_async_remote_copy(
            vall.at[rows(i, w), pl.ds(half, half)], ubuf.at[rows(i, w), :], hs.at[i], hr.at[i],
            device_id={"row": z + 1}, device_id_type=MESH)

    def lift(i):
        return pltpu.make_async_remote_copy(
            sbuf.at[rows(i, w), :], ubuf.at[rows(i, w), :], hs.at[i], hr.at[i],
            device_id={"row": z + 1}, device_id_type=MESH)

    def origin(k):
        return pltpu.make_async_remote_copy(
            vall.at[rows(k, pw), pl.ds(0, half)], sbuf.at[rows(k, pw), :], ts.at[k], tr.at[k],
            device_id={"row": z + 1}, device_id_type=MESH)

    def onward(k):
        return pltpu.make_async_remote_copy(
            sbuf.at[rows(k, pw), :], sbuf.at[rows(k, pw), :], ts.at[k], tr.at[k],
            device_id={"row": z + 1}, device_id_type=MESH)

    own = pltpu.make_async_copy(v, vall.at[:, block(0, s)], lsem)
    own.start()
    load(0).start()
    img[...] = jnp.zeros_like(img)
    ybuf[...] = jnp.zeros_like(ybuf)
    pl.semaphore_wait(barrier, 2 * R + (z > 0).astype(jnp.int32) + (z < R - 1).astype(jnp.int32))
    mate().start()

    def begin(i, carry):
        across(i).start()
        return carry

    lax.fori_loop(0, steps, begin, 0)
    own.wait()
    mate().wait_recv()
    source = (x == 0) & diag

    @pl.when(source)
    def _():
        def send(k, carry):
            origin(k).start()
            return carry
        lax.fori_loop(0, steps * Q, send, 0)

    def prepare(i, hh):
        here, columns = rows(i, w), pl.ds(hh * half, half)
        high, low = split(vall[here, columns])
        vhi[here, columns] = high
        vlo[here, columns] = low

    def prepare_own(i, carry):
        prepare(i, 0)
        return carry

    lax.fori_loop(0, steps, prepare_own, 0)

    def multiply(columns, hook=None):
        def tile(t, carry):
            here = rows(t, w)
            if hook is not None:
                hook(t)
            img[here, columns] += dot3(ahi[here, :], alo[here, :], rhi[...], rlo[...], (1,))
            return carry
        lax.fori_loop(0, steps, tile, 0)

    def feed(value):
        high, low = split(value)
        rhi[...] = high
        rlo[...] = low

    def open_block(i):
        load(i).wait()

        @pl.when(i < steps - 1)
        def _():
            load(i + 1).start()

        def cut(t, carry):
            high, low = split(abuf[lax.rem(i, 2), rows(t, w), :])
            ahi[rows(t, w), :] = high
            alo[rows(t, w), :] = low
            return carry
        lax.fori_loop(0, steps, cut, 0)

    def receive(i):
        across(i).wait_recv()
        share(i).start()

    def collect(i):
        share(i).wait_recv()
        prepare(i, 1)

        @pl.when(relay)
        def _():
            hand(i).start()

    def fold(hh):
        columns = pl.ds(hh * half, half)

        def halve(t, carry):
            high, low = split(img[rows(t, w), columns])
            ihi[rows(t, w), :] = high
            ilo[rows(t, w), :] = low
            return carry
        lax.fori_loop(0, steps, halve, 0)
        def act(b, carry):
            here = rows(b, kd)
            ybuf[here, columns] = dot3(vhi[:, here], vlo[:, here], ihi[...], ilo[...], (0,))
            return carry
        lax.fori_loop(0, 2 * S, act, 0)

    def absorb(value, hh, i):
        feed(value)

        def act(b, carry):
            here, columns = rows(b, kd), pl.ds(hh * half, half)
            ybuf[here, columns] += dot3(vhi[rows(i, w), here], vlo[rows(i, w), here], rhi[...], rlo[...], (0,))
            return carry
        lax.fori_loop(0, 2 * S, act, 0)

    def local_step(i, carry):
        receive(i)
        open_block(i)

        @pl.when(x == 0)
        def _():
            feed(0.5 * vall[rows(i, w), pl.ds(0, half)])
            multiply(pl.ds(0, half))
        collect(i)
        feed(0.5 * vall[rows(i, w), pl.ds(half, half)])
        multiply(pl.ds(half, half))
        return carry

    def stream_step(i, carry):
        @pl.when(jnp.logical_not(diag) & (2 * i < steps))
        def _():
            receive(2 * i)
            receive(2 * i + 1)

        open_block(i)

        @pl.when(adds)
        def _():
            tbuf[...] = weight * dot3(ahi[...], alo[...], vhi[:, :half], vlo[:, :half], (0,))

        def piece(p, carry, i=i):
            k = i * Q + p

            @pl.when(chained & (z > first))
            def _():
                onward(k).wait_recv()

            @pl.when(adds & (z == first))
            def _():
                sbuf[rows(k, pw), :] = tbuf[rows(p, pw), :]

            @pl.when(adds & (z > first))
            def _():
                sbuf[rows(k, pw), :] += tbuf[rows(p, pw), :]

            @pl.when(chained & (z < last))
            def _():
                onward(k).start()
            return carry
        @pl.when((x == 1) | (i == 0))
        def _():
            lax.fori_loop(0, Q, piece, 0)

        lag = steps // 2

        @pl.when(jnp.logical_not(diag) & (i >= lag) & (2 * (i - lag) < steps))
        def _():
            collect(2 * (i - lag))
            collect(2 * (i - lag) + 1)

        @pl.when((x == 0) & chained)
        def _():
            feed(sbuf[rows(i, w), :])

            def hook(t):
                @pl.when((lax.rem(t, steps // Q) == 0) & (i < steps - 1))
                def _():
                    piece(t // (steps // Q), 0, i + 1)
            multiply(pl.ds(0, half), hook)

        @pl.when((x == 1) & diag)
        def _():
            absorb(sbuf[rows(i, w), :], 0, i)

        @pl.when(pair)
        def _():
            hand(i).wait_recv()
            feed(ubuf[rows(i, w), :])
            multiply(pl.ds(half, half))
        return carry

    @pl.when(diag)
    def _():
        lax.fori_loop(0, steps, local_step, 0)
        fold(1)

        @pl.when(x == 0)
        def _():
            fold(0)

        @pl.when(x == 1)
        def _():
            load(0).start()

    @pl.when(catcher)
    def _():
        def catch(i, carry):
            lift(i).wait_recv()
            absorb(ubuf[rows(i, w), :], 1, i)
            return carry
        lax.fori_loop(0, steps, catch, 0)

    @pl.when(helper)
    def _():
        def obtain(i, carry):
            receive(i)
            return carry

        def keep(i, carry):
            collect(i)
            return carry

        def raise_step(i, carry):
            open_block(i)
            sbuf[rows(i, w), :] = dot3(ahi[...], alo[...], vhi[:, half:], vlo[:, half:], (0,))
            lift(i).start()
            return carry
        lax.fori_loop(0, steps, obtain, 0)
        lax.fori_loop(0, steps, keep, 0)
        lax.fori_loop(0, steps, raise_step, 0)

    @pl.when(jnp.logical_not(source | helper))
    def _():
        lax.fori_loop(0, steps, stream_step, 0)

    @pl.when(pair)
    def _():
        fold(1)

    @pl.when((x == 0) & chained & jnp.logical_not(diag))
    def _():
        fold(0)

    reduce_blocks(R, S, blocks, out, ybuf, part, r_sub, r_col, r_row, flip, tile_ref,
                  ps, pr, qs, qr, us, ur, gs, gr, es, er)
    mate().wait_send()

    def drain(i, carry):
        across(i).wait_send()
        share(i).wait_send()

        @pl.when(relay)
        def _():
            hand(i).wait_send()

        @pl.when(helper)
        def _():
            lift(i).wait_send()
        return carry

    lax.fori_loop(0, steps, drain, 0)

    def sent(k, carry):
        @pl.when(source)
        def _():
            origin(k).wait_send()

        @pl.when(chained & (z < last) & jnp.logical_not(source))
        def _():
            onward(k).wait_send()
        return carry

    lax.fori_loop(0, steps * Q, sent, 0)


def image(v, a, R, S):
    m, kd = v.shape
    w = kd
    steps = m // w
    Q = 4
    half = S * kd
    dma = pltpu.SemaphoreType.DMA
    f32, bf16 = jnp.float32, jnp.bfloat16
    blocks, most = owners(R, S)
    nb, hr = len(blocks), kd // S
    return pl.pallas_call(
        functools.partial(image_kernel, R, S, Q, blocks),
        out_shape=jax.ShapeDtypeStruct((kd, half), f32),
        in_specs=[pl.BlockSpec(memory_space=pltpu.VMEM), pl.BlockSpec(memory_space=pl.ANY)],
        out_specs=pl.BlockSpec(memory_space=pltpu.VMEM),
        scratch_shapes=[
            pltpu.VMEM((m, 2 * half), f32), pltpu.VMEM((m, 2 * half), f32),
            pltpu.VMEM((2 * half, 2 * half), f32),
            pltpu.VMEM((m, half), f32), pltpu.VMEM((m, half), f32), pltpu.VMEM((w, half), f32),
            pltpu.VMEM((2, m, w), f32), pltpu.VMEM((m, w), bf16), pltpu.VMEM((m, w), bf16),
            pltpu.VMEM((m, 2 * half), bf16), pltpu.VMEM((m, 2 * half), bf16),
            pltpu.VMEM((m, half), bf16), pltpu.VMEM((m, half), bf16),
            pltpu.VMEM((w, half), bf16), pltpu.VMEM((w, half), bf16),
            dma, dma((2,)), dma, dma, dma((steps,)), dma((steps,)), dma((steps,)), dma((steps,)),
            dma((steps,)), dma((steps,)), dma((steps * Q,)), dma((steps * Q,)),
            pltpu.VMEM((nb, kd, kd), f32), pltpu.VMEM((nb, hr, kd), f32), pltpu.VMEM((nb, hr, kd), f32),
            pltpu.VMEM((R, most, hr, kd), f32), pltpu.VMEM((nb, kd, hr), f32), pltpu.VMEM((S, kd, kd), f32),
            dma((nb,)), dma((nb,)), dma((nb,)), dma((nb,)), dma((nb,)), dma((R, most)),
            dma((nb,)), dma((nb,)), dma((S,)), dma((S,)),
        ],
        compiler_params=pltpu.CompilerParams(
            collective_id=3, has_side_effects=True, vmem_limit_bytes=64_000_000),
        cost_estimate=pl.CostEstimate(flops=0, bytes_accessed=100_000_000, transcendentals=0),
        name="image",
    )(v, a)


def partial_general(matrix, basis_vectors):
    R = lax.axis_size("row")
    S = lax.axis_size("sub")
    C = lax.axis_size("col") * S
    m, kd = basis_vectors.shape
    K = kd * C
    n = matrix.shape[1]
    per = n // m
    piece = m // R
    own, spread = gather(basis_vectors, R, C // S, S)
    width = K // CHUNKS
    images = []
    for c in range(CHUNKS):
        part = lax.dot_general(
            matrix,
            own[:, c * width : (c + 1) * width],
            (((0,), (0,)), ((), ())),
            precision=lax.Precision.HIGH,
            preferred_element_type=jnp.float32,
        )
        if c == 0:
            part, spread = lax.optimization_barrier((part, spread))
        part = part.reshape(per, R, piece, width).transpose(1, 0, 2, 3).reshape(R * per * piece, width)
        images.append(lax.psum_scatter(part, "row", scatter_dimension=0, tiled=True))
    mine = regroup(spread, C // S, S).reshape(per * piece, K)
    return jnp.concatenate(
        [
            lax.dot_general(
                mine,
                image,
                (((0,), (0,)), ((), ())),
                precision=lax.Precision.HIGH,
                preferred_element_type=jnp.float32,
            )
            for image in images
        ],
        axis=1,
    )


def shards(matrix, basis_vectors, split_size):
    R = lax.axis_size("row")
    X = lax.axis_size("col")
    S = lax.axis_size("sub")
    m, n = matrix.shape
    halves = m == n and R == X * S and X == 2 and S == 2
    if halves:
        child_block = image(basis_vectors, matrix, R, S)
    else:
        child_block = project(partial_general(matrix, basis_vectors), R, X, S)
    row_ids = (
        jnp.arange(child_block.shape[0], dtype=jnp.int32)
        + lax.axis_index("row") * child_block.shape[0]
    )
    col_ids = (
        jnp.arange(child_block.shape[1], dtype=jnp.int32)
        + lax.axis_index("col") * child_block.shape[1]
    )
    leading = split_size[0]
    row_first = row_ids < leading
    col_first = col_ids < leading
    mask_one = row_first[:, None] & col_first[None, :]
    mask_two = jnp.logical_not(row_first)[:, None] & jnp.logical_not(col_first)[None, :]
    selected = jnp.where(lax.axis_index("sub") == 0, mask_one, mask_two)
    return jnp.where(selected, child_block, jnp.zeros((), jnp.float32))[None]


def solution(mesh):
    placed = (
        P(("groups", "row"), ("col", "sub")),
        P(("groups", "row"), ("col", "sub")),
        P("groups"),
    )
    return jax.shard_map(
        shards,
        mesh=mesh,
        in_specs=placed,
        out_specs=P("sub", ("groups", "row"), "col"),
        check_vma=False,
    )
```

```python
import functools

import jax
import jax.numpy as jnp
from jax import lax
from jax.experimental import pallas as pl
from jax.experimental.pallas import tpu as pltpu
from jax.sharding import PartitionSpec as P

MESH = pl.DeviceIdType.MESH
CHUNKS = 1


def gather_kernel(R, X, S, v, own, spread, lsem, xs, xr, zs, zr, ps, pr, fs, fr):
    r, x, s = lax.axis_index("row"), lax.axis_index("col"), lax.axis_index("sub")
    m, kd = v.shape
    piece = m // R

    def columns(cx, cs):
        return pl.ds(pl.multiple_of((cx * S + cs) * kd, kd), kd)

    peers = [{"col": lax.rem(x + d, X)} for d in range(1, X)]
    peers += [{"row": lax.rem(r + d, R)} for d in range(1, R)]
    peers += [{"sub": lax.rem(s + d, S)} for d in range(1, S)]
    barrier = pltpu.get_barrier_semaphore()
    for peer in peers:
        pl.semaphore_signal(barrier, inc=1, device_id=peer, device_id_type=MESH)
    pl.semaphore_wait(barrier, len(peers))

    mine = own.at[:, columns(x, s)]
    across, spreads, partner, forward = [], [], [], []
    for d in range(1, X):
        across.append(pltpu.make_async_remote_copy(
            v, mine, xs.at[d - 1], xr.at[d - 1],
            device_id={"col": lax.rem(x + d, X)}, device_id_type=MESH))
    for d in range(1, R):
        i = lax.rem(r + d, R)
        spreads.append(pltpu.make_async_remote_copy(
            v.at[pl.ds(pl.multiple_of(i * piece, piece), piece), :], spread.at[r],
            zs.at[d - 1], zr.at[d - 1],
            device_id={"row": i}, device_id_type=MESH))
    for d in range(1, S):
        partner.append(pltpu.make_async_remote_copy(
            v, mine, ps.at[d - 1], pr.at[d - 1],
            device_id={"sub": lax.rem(s + d, S)}, device_id_type=MESH))
    for copy in across + spreads + partner:
        copy.start()
    local = [
        pltpu.make_async_copy(v, mine, lsem.at[0]),
        pltpu.make_async_copy(
            v.at[pl.ds(pl.multiple_of(r * piece, piece), piece), :], spread.at[r], lsem.at[1]),
    ]
    for copy in local:
        copy.start()
    for d in range(1, X):
        across[d - 1].wait_recv()
        block = own.at[:, columns(lax.rem(x - d + X, X), s)]
        for e in range(1, S):
            copy = pltpu.make_async_remote_copy(
                block, block, fs.at[d - 1, e - 1], fr.at[d - 1, e - 1],
                device_id={"sub": lax.rem(s + e, S)}, device_id_type=MESH)
            copy.start()
            forward.append(copy)
    for copy in across:
        copy.wait_send()
    for copy in spreads + partner + forward:
        copy.wait()
    for copy in local:
        copy.wait()


def gather(v, R, X, S):
    m, kd = v.shape
    dma = pltpu.SemaphoreType.DMA
    return pl.pallas_call(
        functools.partial(gather_kernel, R, X, S),
        out_shape=(
            jax.ShapeDtypeStruct((m, kd * X * S), v.dtype),
            jax.ShapeDtypeStruct((R, m // R, kd), v.dtype),
        ),
        in_specs=[pl.BlockSpec(memory_space=pltpu.VMEM)],
        out_specs=(pl.BlockSpec(memory_space=pl.ANY), pl.BlockSpec(memory_space=pl.ANY)),
        scratch_shapes=[
            dma((2,)), dma((X - 1,)), dma((X - 1,)), dma((R - 1,)), dma((R - 1,)),
            dma((S - 1,)), dma((S - 1,)), dma((X - 1, S - 1)), dma((X - 1, S - 1)),
        ],
        compiler_params=pltpu.CompilerParams(collective_id=0, has_side_effects=True),
        cost_estimate=pl.CostEstimate(flops=0, bytes_accessed=100_000_000, transcendentals=0),
        name="gather",
    )(v)


def regroup_kernel(X, S, spread, mine, lsem, ss, rs):
    x, s = lax.axis_index("col"), lax.axis_index("sub")
    C = X * S
    k = x * S + s
    R, piece, kd = spread.shape
    per = R // C
    barrier = pltpu.get_barrier_semaphore()
    dests = [lax.rem(k + e, C) for e in range(C)]
    for j in dests[1:]:
        pl.semaphore_signal(
            barrier, inc=1, device_id={"col": j // S, "sub": lax.rem(j, S)}, device_id_type=MESH)
    pl.semaphore_wait(barrier, C - 1)
    target = mine.at[:, :, pl.ds(pl.multiple_of(k * kd, kd), kd)]
    copies = []
    for e in range(1, C):
        j = dests[e]
        copies.append(pltpu.make_async_remote_copy(
            spread.at[pl.ds(j * per, per)], target, ss.at[e - 1], rs.at[e - 1],
            device_id={"col": j // S, "sub": lax.rem(j, S)}, device_id_type=MESH))
    copies.append(pltpu.make_async_copy(spread.at[pl.ds(k * per, per)], target, lsem))
    for copy in copies:
        copy.start()
    for copy in copies:
        copy.wait()


def regroup(spread, X, S):
    R, piece, kd = spread.shape
    C = X * S
    dma = pltpu.SemaphoreType.DMA
    return pl.pallas_call(
        functools.partial(regroup_kernel, X, S),
        out_shape=jax.ShapeDtypeStruct((R // C, piece, kd * C), spread.dtype),
        in_specs=[pl.BlockSpec(memory_space=pltpu.VMEM)],
        out_specs=pl.BlockSpec(memory_space=pl.ANY),
        scratch_shapes=[dma, dma((C - 1,)), dma((C - 1,))],
        compiler_params=pltpu.CompilerParams(collective_id=1, has_side_effects=True),
        cost_estimate=pl.CostEstimate(flops=0, bytes_accessed=60_000_000, transcendentals=0),
        name="regroup",
    )(spread)


def project_kernel(R, X, S, p, out, acc, from_sub, from_col, from_row, res, from_pair,
                   a_s, a_r, b_s, b_r, c_s, c_r, d_s, d_r):
    r, x, s = lax.axis_index("row"), lax.axis_index("col"), lax.axis_index("sub")
    K = p.shape[0]
    rb, kd = K // R, K // (X * S)

    def rows(i):
        return pl.ds(pl.multiple_of(i * rb, rb), rb)

    def columns(cx, cs):
        return pl.ds(pl.multiple_of((cx * S + cs) * kd, kd), kd)

    def col(d):
        return lax.rem(x + d, X)

    peers = [{"col": col(d)} for d in range(1, X)]
    peers += [{"row": lax.rem(r + d, R)} for d in range(1, R)]
    peers += [{"sub": lax.rem(s + d, S)} for d in range(1, S)]
    barrier = pltpu.get_barrier_semaphore()
    for peer in peers:
        pl.semaphore_signal(barrier, inc=1, device_id=peer, device_id_type=MESH)
    pl.semaphore_wait(barrier, len(peers))

    order = list(range(1, X)) + [0]
    steps = list(range(1, R)) + [0]
    pair = {}
    for d in order:
        for e in range(1, S):
            other = lax.rem(s + e, S)
            pair[d, e] = pltpu.make_async_remote_copy(
                p.at[:, columns(col(d), other)], from_sub.at[e - 1, d],
                a_s.at[e - 1, d], a_r.at[e - 1, d],
                device_id={"sub": other}, device_id_type=MESH)
            pair[d, e].start()
    cross = {}
    for d in order:
        for e in range(1, S):
            pair[d, e].wait_recv()
        for q in steps:
            here = rows(lax.rem(r + q, R))
            total = p[here, columns(col(d), s)]
            for e in range(1, S):
                total = total + from_sub[e - 1, d, here, :]
            acc[d, here, :] = total
            if d > 0:
                cross[d, q] = pltpu.make_async_remote_copy(
                    acc.at[d, here], from_col.at[d - 1, here],
                    b_s.at[d - 1, q], b_r.at[d - 1, q],
                    device_id={"col": col(d)}, device_id_type=MESH)
                cross[d, q].start()
    along = []
    for q in steps:
        i = lax.rem(r + q, R)
        here = rows(i)
        total = acc[0, here, :]
        for d in range(1, X):
            cross[d, q].wait_recv()
            total = total + from_col[d - 1, here, :]
        if q > 0:
            acc[0, here, :] = total
            copy = pltpu.make_async_remote_copy(
                acc.at[0, here], from_row.at[q - 1], c_s.at[q - 1], c_r.at[q - 1],
                device_id={"row": i}, device_id_type=MESH)
            copy.start()
            along.append(copy)
    for q in range(1, R):
        along[q - 1].wait_recv()
        total = total + from_row[q - 1]
    res[...] = total
    last = []
    for e in range(1, S):
        copy = pltpu.make_async_remote_copy(
            res, from_pair.at[e - 1], d_s.at[e - 1], d_r.at[e - 1],
            device_id={"sub": lax.rem(s + e, S)}, device_id_type=MESH)
        copy.start()
        last.append(copy)
    out[:, pl.ds(pl.multiple_of(s * kd, kd), kd)] = total
    for e in range(1, S):
        last[e - 1].wait_recv()
        out[:, pl.ds(pl.multiple_of(lax.rem(s - e + S, S) * kd, kd), kd)] = from_pair[e - 1]
    for copy in list(pair.values()) + list(cross.values()) + along + last:
        copy.wait_send()


def project(partial, R, X, S):
    K = partial.shape[0]
    rb, kd = K // R, K // (X * S)
    dma = pltpu.SemaphoreType.DMA
    f32 = jnp.float32
    return pl.pallas_call(
        functools.partial(project_kernel, R, X, S),
        out_shape=jax.ShapeDtypeStruct((rb, S * kd), f32),
        in_specs=[pl.BlockSpec(memory_space=pltpu.VMEM)],
        out_specs=pl.BlockSpec(memory_space=pltpu.VMEM),
        scratch_shapes=[
            pltpu.VMEM((X, K, kd), f32),
            pltpu.VMEM((S - 1, X, K, kd), f32),
            pltpu.VMEM((X - 1, K, kd), f32),
            pltpu.VMEM((R - 1, rb, kd), f32),
            pltpu.VMEM((rb, kd), f32),
            pltpu.VMEM((S - 1, rb, kd), f32),
            dma((S - 1, X)), dma((S - 1, X)), dma((X - 1, R)), dma((X - 1, R)),
            dma((R - 1,)), dma((R - 1,)), dma((S - 1,)), dma((S - 1,)),
        ],
        compiler_params=pltpu.CompilerParams(collective_id=2, has_side_effects=True),
        cost_estimate=pl.CostEstimate(flops=0, bytes_accessed=60_000_000, transcendentals=0),
        name="project",
    )(partial)


def split(value):
    high = value.astype(jnp.bfloat16)
    return high, (value - high.astype(jnp.float32)).astype(jnp.bfloat16)


def dot3(a_high, a_low, b_high, b_low, contract):
    def one(a, b):
        return lax.dot_general(a, b, ((contract, (0,)), ((), ())),
                               preferred_element_type=jnp.float32)
    return one(a_high, b_high) + (one(a_high, b_low) + one(a_low, b_high))


def owners(R, S):
    blocks, chips, columns = [], {}, {}
    pairs = [(i, i) for i in range(R)]
    pairs += sorted(((i, j) for i in range(R) for j in range(i + 1, R)), key=lambda p: (p[0] - p[1], p))
    for i, j in pairs:
        choices = [(j // S, i), (i // S, j)]
        best = min(choices, key=lambda o: (chips.get(o, 0), columns.get(o[0], 0)))
        slot = chips.get(best, 0)
        chips[best] = slot + 1
        columns[best[0]] = columns.get(best[0], 0) + 1
        blocks.append((i, j, best[0], best[1], slot))
    return blocks[R:] + blocks[:R], max(chips.values())


def reduce_blocks(R, S, blocks, out, ybuf, part, r_sub, r_col, r_row, flip, tile_ref,
                  ps, pr, qs, qr, us, ur, gs, gr, es, er):
    z, x, s = lax.axis_index("row"), lax.axis_index("col"), lax.axis_index("sub")
    other = 1 - s
    kd = part.shape[1]
    hr = kd // S
    mine = pl.ds(pl.multiple_of(s * hr, hr), hr)
    theirs = pl.ds(pl.multiple_of(other * hr, hr), hr)

    def filled(t, side):
        i, j = blocks[t][:2]
        inner = z // S == side
        return inner if side == 1 or min(i // S, j // S) > 0 else z >= 0

    def held(g):
        return pl.ds(pl.multiple_of((jnp.where(x == g // S, 0, 1) * S + g % S) * kd, kd), kd)

    def swap(t):
        return pltpu.make_async_remote_copy(
            part.at[t, theirs, :], r_sub.at[t], ps.at[t], pr.at[t],
            device_id={"sub": other}, device_id_type=MESH)

    def cross(t):
        return pltpu.make_async_remote_copy(
            part.at[t, mine, :], r_col.at[t], qs.at[t], qr.at[t],
            device_id={"col": 1 - x}, device_id_type=MESH)

    def along(t, sender):
        return pltpu.make_async_remote_copy(
            part.at[t, mine, :], r_row.at[sender, blocks[t][4]], us.at[t], ur.at[sender, blocks[t][4]],
            device_id={"row": blocks[t][3]}, device_id_type=MESH)

    def region(t, direct):
        i, j = blocks[t][:2]
        if direct:
            return tile_ref.at[j % S, mine, :]
        return tile_ref.at[i % S, :, mine]

    def chip(t, direct):
        i, j = blocks[t][:2]
        return (j // S, i) if direct else (i // S, j)

    def far(t, direct):
        xo, zo = chip(t, direct)
        return pltpu.make_async_remote_copy(
            part.at[t, mine, :] if direct else flip.at[t], region(t, direct), gs.at[t], gr.at[t],
            device_id={"col": xo, "row": zo}, device_id_type=MESH)

    def near(t, direct):
        slot = blocks[t][1] % S if direct else blocks[t][0] % S
        return pltpu.make_async_remote_copy(
            region(t, direct), region(t, direct), es.at[slot], er.at[slot],
            device_id={"sub": other}, device_id_type=MESH)

    for t, (i, j, xo, zo, slot) in enumerate(blocks):
        part[t] = ybuf[held(i), held(j)] + ybuf[held(j), held(i)].T
        swap(t).start()
    for t, (i, j, xo, zo, slot) in enumerate(blocks):
        swap(t).wait_recv()
        part[t, mine, :] += r_sub[t]

        @pl.when((x != xo) & filled(t, 1 - xo))
        def _():
            cross(t).start()
    for t, (i, j, xo, zo, slot) in enumerate(blocks):
        @pl.when((x == xo) & filled(t, 1 - xo))
        def _():
            cross(t).wait_recv()
            part[t, mine, :] += r_col[t]

        @pl.when((x == xo) & (z != zo))
        def _():
            along(t, z).start()
    for t, (i, j, xo, zo, slot) in enumerate(blocks):
        straight = (xo, zo) == (j // S, i)

        @pl.when((x == xo) & (z == zo))
        def _():
            for q in range(R):
                if q != zo:
                    along(t, q).wait_recv()
                    part[t, mine, :] += r_row[q, slot]
            value = part[t, mine, :]
            if i != j:
                flip[t] = value.T
                far(t, not straight).start()
            if straight:
                tile_ref[j % S, mine, :] = value
            else:
                tile_ref[i % S, :, mine] = value.T
            near(t, straight).start()
    for t, (i, j, xo, zo, slot) in enumerate(blocks):
        straight = (xo, zo) == (j // S, i)
        if i != j:
            xf, zf = chip(t, not straight)

            @pl.when((x == xf) & (z == zf))
            def _():
                far(t, not straight).wait_recv()
                near(t, not straight).start()
    for t, (i, j, xo, zo, slot) in enumerate(blocks):
        straight = (xo, zo) == (j // S, i)
        swap(t).wait_send()

        @pl.when((x != xo) & filled(t, 1 - xo))
        def _():
            cross(t).wait_send()

        @pl.when((x == xo) & (z != zo))
        def _():
            along(t, z).wait_send()
        for direct in ((straight, not straight) if i != j else (straight,)):
            xn, zn = chip(t, direct)

            @pl.when((x == xn) & (z == zn))
            def _():
                near(t, direct).wait()
        if i != j:
            @pl.when((x == xo) & (z == zo))
            def _():
                far(t, not straight).wait_send()
    for b in range(S):
        out[:, b * kd:(b + 1) * kd] = tile_ref[b]


def image_kernel(R, S, Q, blocks, v, a, out, vall, img, ybuf, sbuf, ubuf, tbuf, abuf, ahi, alo, vhi, vlo,
                 ihi, ilo, rhi, rlo, whi, wlo, lsem, asem, os, orr, xs, xr, fs, fr, hs, hr, ts, tr,
                 part, r_sub, r_col, r_row, flip, tile_ref, ps, pr, qs, qr, us, ur, gs, gr, es, er):
    z, x, s = lax.axis_index("row"), lax.axis_index("col"), lax.axis_index("sub")
    c = x * S + s
    m, kd = v.shape
    half = S * kd
    steps = m // abuf.shape[2]
    w = m // steps
    pw = w // Q
    first = jnp.where(x == 0, c, 0)
    last = jnp.where(x == 0, R - 1, c)
    chained = (z >= first) & (z <= last)
    diag = z == c
    pair = (x == 1) & (z == x * S + 1) & (s == 0)
    catcher = (x == 0) & diag & (z == 1)
    relay = (x == 1) & (z == x * S) & (s == 1 - x)
    helper = (x == 0) & (z == 0) & (s == 1)
    adds = (x == 1) & chained
    weight = jnp.where(diag, 0.5, 1.0).astype(jnp.float32)
    other = 1 - s

    def rows(i, n):
        return pl.ds(pl.multiple_of(i * n, n), n)

    def block(hh, ss):
        return pl.ds(pl.multiple_of((hh * S + ss) * kd, kd), kd)

    barrier = pltpu.get_barrier_semaphore()
    pl.semaphore_signal(barrier, inc=1, device_id={"sub": other}, device_id_type=MESH)
    for q in range(R):
        if q > 0:
            pl.semaphore_signal(barrier, inc=1, device_id={"row": lax.rem(z + q, R)}, device_id_type=MESH)
        pl.semaphore_signal(barrier, inc=1, device_id={"col": 1 - x, "row": q}, device_id_type=MESH)

    @pl.when(z > 0)
    def _():
        pl.semaphore_signal(barrier, inc=1, device_id={"row": z - 1, "sub": other}, device_id_type=MESH)

    @pl.when(z < R - 1)
    def _():
        pl.semaphore_signal(barrier, inc=1, device_id={"row": z + 1, "sub": other}, device_id_type=MESH)

    def load(i):
        return pltpu.make_async_copy(a.at[:, rows(i, w)], abuf.at[lax.rem(i, 2)], asem.at[lax.rem(i, 2)])

    def mate():
        return pltpu.make_async_remote_copy(
            v, vall.at[:, block(0, s)], os, orr, device_id={"sub": other}, device_id_type=MESH)

    def across(i):
        return pltpu.make_async_remote_copy(
            v.at[rows(i, w), :], vall.at[rows(i, w), block(1, s)], xs.at[i], xr.at[i],
            device_id={"col": 1 - x}, device_id_type=MESH)

    def share(i):
        here = vall.at[rows(i, w), block(1, s)]
        return pltpu.make_async_remote_copy(
            here, here, fs.at[i], fr.at[i], device_id={"sub": other}, device_id_type=MESH)

    def hand(i):
        return pltpu.make_async_remote_copy(
            vall.at[rows(i, w), pl.ds(half, half)], ubuf.at[rows(i, w), :], hs.at[i], hr.at[i],
            device_id={"row": z + 1}, device_id_type=MESH)

    def lift(i):
        return pltpu.make_async_remote_copy(
            sbuf.at[rows(i, w), :], ubuf.at[rows(i, w), :], hs.at[i], hr.at[i],
            device_id={"row": z + 1}, device_id_type=MESH)

    def origin(k):
        return pltpu.make_async_remote_copy(
            vall.at[rows(k, pw), pl.ds(0, half)], sbuf.at[rows(k, pw), :], ts.at[k], tr.at[k],
            device_id={"row": z + 1}, device_id_type=MESH)

    def onward(k):
        return pltpu.make_async_remote_copy(
            sbuf.at[rows(k, pw), :], sbuf.at[rows(k, pw), :], ts.at[k], tr.at[k],
            device_id={"row": z + 1}, device_id_type=MESH)

    own = pltpu.make_async_copy(v, vall.at[:, block(0, s)], lsem)
    own.start()
    load(0).start()
    img[...] = jnp.zeros_like(img)
    ybuf[...] = jnp.zeros_like(ybuf)
    pl.semaphore_wait(barrier, 2 * R + (z > 0).astype(jnp.int32) + (z < R - 1).astype(jnp.int32))
    mate().start()

    def begin(i, carry):
        across(i).start()
        return carry

    lax.fori_loop(0, steps, begin, 0)
    own.wait()
    mate().wait_recv()
    source = (x == 0) & diag

    @pl.when(source)
    def _():
        def send(k, carry):
            origin(k).start()
            return carry
        lax.fori_loop(0, steps * Q, send, 0)

    def prepare(i, hh):
        here, columns = rows(i, w), pl.ds(hh * half, half)
        high, low = split(vall[here, columns])
        vhi[here, columns] = high
        vlo[here, columns] = low

    def prepare_own(i, carry):
        prepare(i, 0)
        return carry

    lax.fori_loop(0, steps, prepare_own, 0)

    def multiply(columns):
        def tile(t, carry):
            here = rows(t, w)
            img[here, columns] += dot3(ahi[here, :], alo[here, :], rhi[...], rlo[...], (1,))
            return carry
        lax.fori_loop(0, steps, tile, 0)

    def feed(value):
        high, low = split(value)
        rhi[...] = high
        rlo[...] = low

    def open_block(i):
        load(i).wait()

        @pl.when(i < steps - 1)
        def _():
            load(i + 1).start()

        def cut(t, carry):
            high, low = split(abuf[lax.rem(i, 2), rows(t, w), :])
            ahi[rows(t, w), :] = high
            alo[rows(t, w), :] = low
            return carry
        lax.fori_loop(0, steps, cut, 0)

    def receive(i):
        across(i).wait_recv()
        share(i).start()

    def collect(i):
        share(i).wait_recv()
        prepare(i, 1)

        @pl.when(relay)
        def _():
            hand(i).start()

    def fold(hh):
        columns = pl.ds(hh * half, half)

        def halve(t, carry):
            high, low = split(img[rows(t, w), columns])
            ihi[rows(t, w), :] = high
            ilo[rows(t, w), :] = low
            return carry
        lax.fori_loop(0, steps, halve, 0)
        def act(b, carry):
            here = rows(b, kd)
            ybuf[here, columns] = dot3(vhi[:, here], vlo[:, here], ihi[...], ilo[...], (0,))
            return carry
        lax.fori_loop(0, 2 * S, act, 0)

    def absorb(value, hh, i):
        feed(value)

        def act(b, carry):
            here, columns = rows(b, kd), pl.ds(hh * half, half)
            ybuf[here, columns] += dot3(vhi[rows(i, w), here], vlo[rows(i, w), here], rhi[...], rlo[...], (0,))
            return carry
        lax.fori_loop(0, 2 * S, act, 0)

    def local_step(i, carry):
        @pl.when(i == 0)
        def _():
            receive(i)

        @pl.when(i < steps - 1)
        def _():
            receive(i + 1)
        open_block(i)

        @pl.when(x == 0)
        def _():
            feed(0.5 * vall[rows(i, w), pl.ds(0, half)])
            multiply(pl.ds(0, half))
        collect(i)
        feed(0.5 * vall[rows(i, w), pl.ds(half, half)])
        multiply(pl.ds(half, half))
        return carry

    def piece(k, p, adding):
        @pl.when(chained & (z > first))
        def _():
            onward(k).wait_recv()

        if adding:
            @pl.when(adds & (z == first))
            def _():
                sbuf[rows(k, pw), :] = tbuf[rows(p, pw), :]

            @pl.when(adds & (z > first))
            def _():
                sbuf[rows(k, pw), :] += tbuf[rows(p, pw), :]

        @pl.when(chained & (z < last))
        def _():
            onward(k).start()

    def stream_step(i, carry):
        @pl.when(jnp.logical_not(diag) & (2 * i < steps))
        def _():
            receive(2 * i)
            receive(2 * i + 1)

        open_block(i)

        @pl.when(adds)
        def _():
            tbuf[...] = weight * dot3(ahi[...], alo[...], vhi[:, :half], vlo[:, :half], (0,))

        def next_piece(p, c2):
            piece(i * Q + p, p, True)
            return c2
        lax.fori_loop(0, Q, next_piece, 0)

        lag = steps // 2

        @pl.when(jnp.logical_not(diag) & (i >= lag) & (2 * (i - lag) < steps))
        def _():
            collect(2 * (i - lag))
            collect(2 * (i - lag) + 1)

        @pl.when(diag)
        def _():
            absorb(sbuf[rows(i, w), :], 0, i)
        return carry

    def early_step(i, carry):
        receive(2 * i)
        receive(2 * i + 1)

        def next_piece(p, c2):
            piece(i * Q + p, p, False)
            return c2
        lax.fori_loop(0, Q, next_piece, 0)
        return carry

    def wide_step(n, carry):
        open_block(n)

        def widen(b, c2):
            here = rows(b, kd)
            high, low = split(dot3(vhi[:, here], vlo[:, here], ahi[...], alo[...], (0,)))
            whi[here, :] = high
            wlo[here, :] = low

            @pl.when(lax.rem(b, 2) == 0)
            def _():
                piece(steps // 2 * Q + n * (Q // 2) + b // 2, 0, False)
            return c2
        lax.fori_loop(0, 2 * S, widen, 0)

        @pl.when(x == 0)
        def _():
            feed(sbuf[rows(n, w), :])

        @pl.when(x == 1)
        def _():
            hand(n).wait_recv()
            feed(ubuf[rows(n, w), :])
        columns = rows(x, half)

        def add(b, c2):
            here = rows(b, kd)
            ybuf[here, columns] += dot3(whi[here, :], wlo[here, :], rhi[...], rlo[...], (1,))
            return c2
        lax.fori_loop(0, 2 * S, add, 0)
        return carry

    @pl.when(diag)
    def _():
        lax.fori_loop(0, steps, local_step, 0)
        fold(1)

        @pl.when(x == 0)
        def _():
            fold(0)

        @pl.when(x == 1)
        def _():
            load(0).start()

    @pl.when(catcher)
    def _():
        def catch(i, carry):
            lift(i).wait_recv()
            absorb(ubuf[rows(i, w), :], 1, i)
            return carry
        lax.fori_loop(0, steps, catch, 0)

    @pl.when(helper)
    def _():
        def obtain(i, carry):
            receive(i)
            return carry

        def keep(i, carry):
            collect(i)
            return carry

        def raise_step(i, carry):
            open_block(i)
            sbuf[rows(i, w), :] = dot3(ahi[...], alo[...], vhi[:, half:], vlo[:, half:], (0,))
            lift(i).start()
            return carry
        lax.fori_loop(0, steps, obtain, 0)
        lax.fori_loop(0, steps, keep, 0)
        lax.fori_loop(0, steps, raise_step, 0)

    wide = pair | ((x == 0) & chained & jnp.logical_not(diag))

    @pl.when(wide)
    def _():
        def keep_all(i, carry):
            collect(i)
            return carry
        lax.fori_loop(0, steps // 2, early_step, 0)
        lax.fori_loop(0, steps, keep_all, 0)
        lax.fori_loop(0, steps, wide_step, 0)

    @pl.when((x == 1) & jnp.logical_not(pair))
    def _():
        lax.fori_loop(0, steps, stream_step, 0)

    reduce_blocks(R, S, blocks, out, ybuf, part, r_sub, r_col, r_row, flip, tile_ref,
                  ps, pr, qs, qr, us, ur, gs, gr, es, er)
    mate().wait_send()

    def drain(i, carry):
        across(i).wait_send()
        share(i).wait_send()

        @pl.when(relay)
        def _():
            hand(i).wait_send()

        @pl.when(helper)
        def _():
            lift(i).wait_send()
        return carry

    lax.fori_loop(0, steps, drain, 0)

    def sent(k, carry):
        @pl.when(source)
        def _():
            origin(k).wait_send()

        @pl.when(chained & (z < last) & jnp.logical_not(source))
        def _():
            onward(k).wait_send()
        return carry

    lax.fori_loop(0, steps * Q, sent, 0)


def image(v, a, R, S):
    m, kd = v.shape
    w = kd
    steps = m // w
    Q = 4
    half = S * kd
    dma = pltpu.SemaphoreType.DMA
    f32, bf16 = jnp.float32, jnp.bfloat16
    blocks, most = owners(R, S)
    nb, hr = len(blocks), kd // S
    return pl.pallas_call(
        functools.partial(image_kernel, R, S, Q, blocks),
        out_shape=jax.ShapeDtypeStruct((kd, half), f32),
        in_specs=[pl.BlockSpec(memory_space=pltpu.VMEM), pl.BlockSpec(memory_space=pl.ANY)],
        out_specs=pl.BlockSpec(memory_space=pltpu.VMEM),
        scratch_shapes=[
            pltpu.VMEM((m, 2 * half), f32), pltpu.VMEM((m, 2 * half), f32),
            pltpu.VMEM((2 * half, 2 * half), f32),
            pltpu.VMEM((m, half), f32), pltpu.VMEM((m, half), f32), pltpu.VMEM((w, half), f32),
            pltpu.VMEM((2, m, w), f32), pltpu.VMEM((m, w), bf16), pltpu.VMEM((m, w), bf16),
            pltpu.VMEM((m, 2 * half), bf16), pltpu.VMEM((m, 2 * half), bf16),
            pltpu.VMEM((m, half), bf16), pltpu.VMEM((m, half), bf16),
            pltpu.VMEM((w, half), bf16), pltpu.VMEM((w, half), bf16),
            pltpu.VMEM((2 * half, w), bf16), pltpu.VMEM((2 * half, w), bf16),
            dma, dma((2,)), dma, dma, dma((steps,)), dma((steps,)), dma((steps,)), dma((steps,)),
            dma((steps,)), dma((steps,)), dma((steps * Q,)), dma((steps * Q,)),
            pltpu.VMEM((nb, kd, kd), f32), pltpu.VMEM((nb, hr, kd), f32), pltpu.VMEM((nb, hr, kd), f32),
            pltpu.VMEM((R, most, hr, kd), f32), pltpu.VMEM((nb, kd, hr), f32), pltpu.VMEM((S, kd, kd), f32),
            dma((nb,)), dma((nb,)), dma((nb,)), dma((nb,)), dma((nb,)), dma((R, most)),
            dma((nb,)), dma((nb,)), dma((S,)), dma((S,)),
        ],
        compiler_params=pltpu.CompilerParams(
            collective_id=3, has_side_effects=True, vmem_limit_bytes=64_000_000),
        cost_estimate=pl.CostEstimate(flops=0, bytes_accessed=100_000_000, transcendentals=0),
        name="image",
    )(v, a)


def partial_general(matrix, basis_vectors):
    R = lax.axis_size("row")
    S = lax.axis_size("sub")
    C = lax.axis_size("col") * S
    m, kd = basis_vectors.shape
    K = kd * C
    n = matrix.shape[1]
    per = n // m
    piece = m // R
    own, spread = gather(basis_vectors, R, C // S, S)
    width = K // CHUNKS
    images = []
    for c in range(CHUNKS):
        part = lax.dot_general(
            matrix,
            own[:, c * width : (c + 1) * width],
            (((0,), (0,)), ((), ())),
            precision=lax.Precision.HIGH,
            preferred_element_type=jnp.float32,
        )
        if c == 0:
            part, spread = lax.optimization_barrier((part, spread))
        part = part.reshape(per, R, piece, width).transpose(1, 0, 2, 3).reshape(R * per * piece, width)
        images.append(lax.psum_scatter(part, "row", scatter_dimension=0, tiled=True))
    mine = regroup(spread, C // S, S).reshape(per * piece, K)
    return jnp.concatenate(
        [
            lax.dot_general(
                mine,
                image,
                (((0,), (0,)), ((), ())),
                precision=lax.Precision.HIGH,
                preferred_element_type=jnp.float32,
            )
            for image in images
        ],
        axis=1,
    )


def shards(matrix, basis_vectors, split_size):
    R = lax.axis_size("row")
    X = lax.axis_size("col")
    S = lax.axis_size("sub")
    m, n = matrix.shape
    halves = m == n and R == X * S and X == 2 and S == 2
    if halves:
        child_block = image(basis_vectors, matrix, R, S)
    else:
        child_block = project(partial_general(matrix, basis_vectors), R, X, S)
    row_ids = (
        jnp.arange(child_block.shape[0], dtype=jnp.int32)
        + lax.axis_index("row") * child_block.shape[0]
    )
    col_ids = (
        jnp.arange(child_block.shape[1], dtype=jnp.int32)
        + lax.axis_index("col") * child_block.shape[1]
    )
    leading = split_size[0]
    row_first = row_ids < leading
    col_first = col_ids < leading
    mask_one = row_first[:, None] & col_first[None, :]
    mask_two = jnp.logical_not(row_first)[:, None] & jnp.logical_not(col_first)[None, :]
    selected = jnp.where(lax.axis_index("sub") == 0, mask_one, mask_two)
    return jnp.where(selected, child_block, jnp.zeros((), jnp.float32))[None]


def solution(mesh):
    placed = (
        P(("groups", "row"), ("col", "sub")),
        P(("groups", "row"), ("col", "sub")),
        P("groups"),
    )
    return jax.shard_map(
        shards,
        mesh=mesh,
        in_specs=placed,
        out_specs=P("sub", ("groups", "row"), "col"),
        check_vma=False,
    )
```

```python
import functools

import jax
import jax.numpy as jnp
from jax import lax
from jax.experimental import pallas as pl
from jax.experimental.pallas import tpu as pltpu
from jax.sharding import PartitionSpec as P

MESH = pl.DeviceIdType.MESH
CHUNKS = 1


def gather_kernel(R, X, S, v, own, spread, lsem, xs, xr, zs, zr, ps, pr, fs, fr):
    r, x, s = lax.axis_index("row"), lax.axis_index("col"), lax.axis_index("sub")
    m, kd = v.shape
    piece = m // R

    def columns(cx, cs):
        return pl.ds(pl.multiple_of((cx * S + cs) * kd, kd), kd)

    peers = [{"col": lax.rem(x + d, X)} for d in range(1, X)]
    peers += [{"row": lax.rem(r + d, R)} for d in range(1, R)]
    peers += [{"sub": lax.rem(s + d, S)} for d in range(1, S)]
    barrier = pltpu.get_barrier_semaphore()
    for peer in peers:
        pl.semaphore_signal(barrier, inc=1, device_id=peer, device_id_type=MESH)
    pl.semaphore_wait(barrier, len(peers))

    mine = own.at[:, columns(x, s)]
    across, spreads, partner, forward = [], [], [], []
    for d in range(1, X):
        across.append(pltpu.make_async_remote_copy(
            v, mine, xs.at[d - 1], xr.at[d - 1],
            device_id={"col": lax.rem(x + d, X)}, device_id_type=MESH))
    for d in range(1, R):
        i = lax.rem(r + d, R)
        spreads.append(pltpu.make_async_remote_copy(
            v.at[pl.ds(pl.multiple_of(i * piece, piece), piece), :], spread.at[r],
            zs.at[d - 1], zr.at[d - 1],
            device_id={"row": i}, device_id_type=MESH))
    for d in range(1, S):
        partner.append(pltpu.make_async_remote_copy(
            v, mine, ps.at[d - 1], pr.at[d - 1],
            device_id={"sub": lax.rem(s + d, S)}, device_id_type=MESH))
    for copy in across + spreads + partner:
        copy.start()
    local = [
        pltpu.make_async_copy(v, mine, lsem.at[0]),
        pltpu.make_async_copy(
            v.at[pl.ds(pl.multiple_of(r * piece, piece), piece), :], spread.at[r], lsem.at[1]),
    ]
    for copy in local:
        copy.start()
    for d in range(1, X):
        across[d - 1].wait_recv()
        block = own.at[:, columns(lax.rem(x - d + X, X), s)]
        for e in range(1, S):
            copy = pltpu.make_async_remote_copy(
                block, block, fs.at[d - 1, e - 1], fr.at[d - 1, e - 1],
                device_id={"sub": lax.rem(s + e, S)}, device_id_type=MESH)
            copy.start()
            forward.append(copy)
    for copy in across:
        copy.wait_send()
    for copy in spreads + partner + forward:
        copy.wait()
    for copy in local:
        copy.wait()


def gather(v, R, X, S):
    m, kd = v.shape
    dma = pltpu.SemaphoreType.DMA
    return pl.pallas_call(
        functools.partial(gather_kernel, R, X, S),
        out_shape=(
            jax.ShapeDtypeStruct((m, kd * X * S), v.dtype),
            jax.ShapeDtypeStruct((R, m // R, kd), v.dtype),
        ),
        in_specs=[pl.BlockSpec(memory_space=pltpu.VMEM)],
        out_specs=(pl.BlockSpec(memory_space=pl.ANY), pl.BlockSpec(memory_space=pl.ANY)),
        scratch_shapes=[
            dma((2,)), dma((X - 1,)), dma((X - 1,)), dma((R - 1,)), dma((R - 1,)),
            dma((S - 1,)), dma((S - 1,)), dma((X - 1, S - 1)), dma((X - 1, S - 1)),
        ],
        compiler_params=pltpu.CompilerParams(collective_id=0, has_side_effects=True),
        cost_estimate=pl.CostEstimate(flops=0, bytes_accessed=100_000_000, transcendentals=0),
        name="gather",
    )(v)


def regroup_kernel(X, S, spread, mine, lsem, ss, rs):
    x, s = lax.axis_index("col"), lax.axis_index("sub")
    C = X * S
    k = x * S + s
    R, piece, kd = spread.shape
    per = R // C
    barrier = pltpu.get_barrier_semaphore()
    dests = [lax.rem(k + e, C) for e in range(C)]
    for j in dests[1:]:
        pl.semaphore_signal(
            barrier, inc=1, device_id={"col": j // S, "sub": lax.rem(j, S)}, device_id_type=MESH)
    pl.semaphore_wait(barrier, C - 1)
    target = mine.at[:, :, pl.ds(pl.multiple_of(k * kd, kd), kd)]
    copies = []
    for e in range(1, C):
        j = dests[e]
        copies.append(pltpu.make_async_remote_copy(
            spread.at[pl.ds(j * per, per)], target, ss.at[e - 1], rs.at[e - 1],
            device_id={"col": j // S, "sub": lax.rem(j, S)}, device_id_type=MESH))
    copies.append(pltpu.make_async_copy(spread.at[pl.ds(k * per, per)], target, lsem))
    for copy in copies:
        copy.start()
    for copy in copies:
        copy.wait()


def regroup(spread, X, S):
    R, piece, kd = spread.shape
    C = X * S
    dma = pltpu.SemaphoreType.DMA
    return pl.pallas_call(
        functools.partial(regroup_kernel, X, S),
        out_shape=jax.ShapeDtypeStruct((R // C, piece, kd * C), spread.dtype),
        in_specs=[pl.BlockSpec(memory_space=pltpu.VMEM)],
        out_specs=pl.BlockSpec(memory_space=pl.ANY),
        scratch_shapes=[dma, dma((C - 1,)), dma((C - 1,))],
        compiler_params=pltpu.CompilerParams(collective_id=1, has_side_effects=True),
        cost_estimate=pl.CostEstimate(flops=0, bytes_accessed=60_000_000, transcendentals=0),
        name="regroup",
    )(spread)


def project_kernel(R, X, S, p, out, acc, from_sub, from_col, from_row, res, from_pair,
                   a_s, a_r, b_s, b_r, c_s, c_r, d_s, d_r):
    r, x, s = lax.axis_index("row"), lax.axis_index("col"), lax.axis_index("sub")
    K = p.shape[0]
    rb, kd = K // R, K // (X * S)

    def rows(i):
        return pl.ds(pl.multiple_of(i * rb, rb), rb)

    def columns(cx, cs):
        return pl.ds(pl.multiple_of((cx * S + cs) * kd, kd), kd)

    def col(d):
        return lax.rem(x + d, X)

    peers = [{"col": col(d)} for d in range(1, X)]
    peers += [{"row": lax.rem(r + d, R)} for d in range(1, R)]
    peers += [{"sub": lax.rem(s + d, S)} for d in range(1, S)]
    barrier = pltpu.get_barrier_semaphore()
    for peer in peers:
        pl.semaphore_signal(barrier, inc=1, device_id=peer, device_id_type=MESH)
    pl.semaphore_wait(barrier, len(peers))

    order = list(range(1, X)) + [0]
    steps = list(range(1, R)) + [0]
    pair = {}
    for d in order:
        for e in range(1, S):
            other = lax.rem(s + e, S)
            pair[d, e] = pltpu.make_async_remote_copy(
                p.at[:, columns(col(d), other)], from_sub.at[e - 1, d],
                a_s.at[e - 1, d], a_r.at[e - 1, d],
                device_id={"sub": other}, device_id_type=MESH)
            pair[d, e].start()
    cross = {}
    for d in order:
        for e in range(1, S):
            pair[d, e].wait_recv()
        for q in steps:
            here = rows(lax.rem(r + q, R))
            total = p[here, columns(col(d), s)]
            for e in range(1, S):
                total = total + from_sub[e - 1, d, here, :]
            acc[d, here, :] = total
            if d > 0:
                cross[d, q] = pltpu.make_async_remote_copy(
                    acc.at[d, here], from_col.at[d - 1, here],
                    b_s.at[d - 1, q], b_r.at[d - 1, q],
                    device_id={"col": col(d)}, device_id_type=MESH)
                cross[d, q].start()
    along = []
    for q in steps:
        i = lax.rem(r + q, R)
        here = rows(i)
        total = acc[0, here, :]
        for d in range(1, X):
            cross[d, q].wait_recv()
            total = total + from_col[d - 1, here, :]
        if q > 0:
            acc[0, here, :] = total
            copy = pltpu.make_async_remote_copy(
                acc.at[0, here], from_row.at[q - 1], c_s.at[q - 1], c_r.at[q - 1],
                device_id={"row": i}, device_id_type=MESH)
            copy.start()
            along.append(copy)
    for q in range(1, R):
        along[q - 1].wait_recv()
        total = total + from_row[q - 1]
    res[...] = total
    last = []
    for e in range(1, S):
        copy = pltpu.make_async_remote_copy(
            res, from_pair.at[e - 1], d_s.at[e - 1], d_r.at[e - 1],
            device_id={"sub": lax.rem(s + e, S)}, device_id_type=MESH)
        copy.start()
        last.append(copy)
    out[:, pl.ds(pl.multiple_of(s * kd, kd), kd)] = total
    for e in range(1, S):
        last[e - 1].wait_recv()
        out[:, pl.ds(pl.multiple_of(lax.rem(s - e + S, S) * kd, kd), kd)] = from_pair[e - 1]
    for copy in list(pair.values()) + list(cross.values()) + along + last:
        copy.wait_send()


def project(partial, R, X, S):
    K = partial.shape[0]
    rb, kd = K // R, K // (X * S)
    dma = pltpu.SemaphoreType.DMA
    f32 = jnp.float32
    return pl.pallas_call(
        functools.partial(project_kernel, R, X, S),
        out_shape=jax.ShapeDtypeStruct((rb, S * kd), f32),
        in_specs=[pl.BlockSpec(memory_space=pltpu.VMEM)],
        out_specs=pl.BlockSpec(memory_space=pltpu.VMEM),
        scratch_shapes=[
            pltpu.VMEM((X, K, kd), f32),
            pltpu.VMEM((S - 1, X, K, kd), f32),
            pltpu.VMEM((X - 1, K, kd), f32),
            pltpu.VMEM((R - 1, rb, kd), f32),
            pltpu.VMEM((rb, kd), f32),
            pltpu.VMEM((S - 1, rb, kd), f32),
            dma((S - 1, X)), dma((S - 1, X)), dma((X - 1, R)), dma((X - 1, R)),
            dma((R - 1,)), dma((R - 1,)), dma((S - 1,)), dma((S - 1,)),
        ],
        compiler_params=pltpu.CompilerParams(collective_id=2, has_side_effects=True),
        cost_estimate=pl.CostEstimate(flops=0, bytes_accessed=60_000_000, transcendentals=0),
        name="project",
    )(partial)


def split(value):
    high = value.astype(jnp.bfloat16)
    return high, (value - high.astype(jnp.float32)).astype(jnp.bfloat16)


def dot3(a_high, a_low, b_high, b_low, contract):
    def one(a, b):
        return lax.dot_general(a, b, ((contract, (0,)), ((), ())),
                               preferred_element_type=jnp.float32)
    return one(a_high, b_high) + (one(a_high, b_low) + one(a_low, b_high))


def owners(R, S):
    blocks, chips, columns = [], {}, {}
    pairs = [(i, i) for i in range(R)]
    pairs += sorted(((i, j) for i in range(R) for j in range(i + 1, R)), key=lambda p: (p[0] - p[1], p))
    for i, j in pairs:
        choices = [(j // S, i), (i // S, j)]
        best = min(choices, key=lambda o: (chips.get(o, 0), columns.get(o[0], 0)))
        slot = chips.get(best, 0)
        chips[best] = slot + 1
        columns[best[0]] = columns.get(best[0], 0) + 1
        blocks.append((i, j, best[0], best[1], slot))
    return blocks[R:] + blocks[:R], max(chips.values())


def reduce_blocks(R, S, blocks, out, ybuf, part, r_sub, r_col, r_row, flip, tile_ref,
                  ps, pr, qs, qr, us, ur, gs, gr, es, er):
    z, x, s = lax.axis_index("row"), lax.axis_index("col"), lax.axis_index("sub")
    other = 1 - s
    kd = part.shape[1]
    hr = kd // S
    mine = pl.ds(pl.multiple_of(s * hr, hr), hr)
    theirs = pl.ds(pl.multiple_of(other * hr, hr), hr)

    def filled(t, side):
        i, j = blocks[t][:2]
        inner = z // S == side
        return inner if side == 1 or min(i // S, j // S) > 0 else z >= 0

    def held(g):
        return pl.ds(pl.multiple_of((jnp.where(x == g // S, 0, 1) * S + g % S) * kd, kd), kd)

    def swap(t):
        return pltpu.make_async_remote_copy(
            part.at[t, theirs, :], r_sub.at[t], ps.at[t], pr.at[t],
            device_id={"sub": other}, device_id_type=MESH)

    def cross(t):
        return pltpu.make_async_remote_copy(
            part.at[t, mine, :], r_col.at[t], qs.at[t], qr.at[t],
            device_id={"col": 1 - x}, device_id_type=MESH)

    def along(t, sender):
        return pltpu.make_async_remote_copy(
            part.at[t, mine, :], r_row.at[sender, blocks[t][4]], us.at[t], ur.at[sender, blocks[t][4]],
            device_id={"row": blocks[t][3]}, device_id_type=MESH)

    def region(t, direct):
        i, j = blocks[t][:2]
        if direct:
            return tile_ref.at[j % S, mine, :]
        return tile_ref.at[i % S, :, mine]

    def chip(t, direct):
        i, j = blocks[t][:2]
        return (j // S, i) if direct else (i // S, j)

    def far(t, direct):
        xo, zo = chip(t, direct)
        return pltpu.make_async_remote_copy(
            part.at[t, mine, :] if direct else flip.at[t], region(t, direct), gs.at[t], gr.at[t],
            device_id={"col": xo, "row": zo}, device_id_type=MESH)

    def near(t, direct):
        slot = blocks[t][1] % S if direct else blocks[t][0] % S
        return pltpu.make_async_remote_copy(
            region(t, direct), region(t, direct), es.at[slot], er.at[slot],
            device_id={"sub": other}, device_id_type=MESH)

    for t, (i, j, xo, zo, slot) in enumerate(blocks):
        part[t] = ybuf[held(i), held(j)] + ybuf[held(j), held(i)].T
        swap(t).start()
    for t, (i, j, xo, zo, slot) in enumerate(blocks):
        swap(t).wait_recv()
        part[t, mine, :] += r_sub[t]

        @pl.when((x != xo) & filled(t, 1 - xo))
        def _():
            cross(t).start()
    for t, (i, j, xo, zo, slot) in enumerate(blocks):
        @pl.when((x == xo) & filled(t, 1 - xo))
        def _():
            cross(t).wait_recv()
            part[t, mine, :] += r_col[t]

        @pl.when((x == xo) & (z != zo))
        def _():
            along(t, z).start()
    for t, (i, j, xo, zo, slot) in enumerate(blocks):
        straight = (xo, zo) == (j // S, i)

        @pl.when((x == xo) & (z == zo))
        def _():
            for q in range(R):
                if q != zo:
                    along(t, q).wait_recv()
                    part[t, mine, :] += r_row[q, slot]
            value = part[t, mine, :]
            if i != j:
                flip[t] = value.T
                far(t, not straight).start()
            if straight:
                tile_ref[j % S, mine, :] = value
            else:
                tile_ref[i % S, :, mine] = value.T
            near(t, straight).start()
    for t, (i, j, xo, zo, slot) in enumerate(blocks):
        straight = (xo, zo) == (j // S, i)
        if i != j:
            xf, zf = chip(t, not straight)

            @pl.when((x == xf) & (z == zf))
            def _():
                far(t, not straight).wait_recv()
                near(t, not straight).start()
    for t, (i, j, xo, zo, slot) in enumerate(blocks):
        straight = (xo, zo) == (j // S, i)
        swap(t).wait_send()

        @pl.when((x != xo) & filled(t, 1 - xo))
        def _():
            cross(t).wait_send()

        @pl.when((x == xo) & (z != zo))
        def _():
            along(t, z).wait_send()
        for direct in ((straight, not straight) if i != j else (straight,)):
            xn, zn = chip(t, direct)

            @pl.when((x == xn) & (z == zn))
            def _():
                near(t, direct).wait()
        if i != j:
            @pl.when((x == xo) & (z == zo))
            def _():
                far(t, not straight).wait_send()
    for b in range(S):
        out[:, b * kd:(b + 1) * kd] = tile_ref[b]


def image_kernel(R, S, Q, blocks, v, a, out, vall, img, ybuf, sbuf, ubuf, tbuf, abuf, ahi, alo, vhi, vlo,
                 ihi, ilo, rhi, rlo, whi, wlo, lsem, asem, os, orr, xs, xr, fs, fr, hs, hr, ts, tr,
                 part, r_sub, r_col, r_row, flip, tile_ref, ps, pr, qs, qr, us, ur, gs, gr, es, er):
    z, x, s = lax.axis_index("row"), lax.axis_index("col"), lax.axis_index("sub")
    c = x * S + s
    m, kd = v.shape
    half = S * kd
    steps = m // abuf.shape[2]
    w = m // steps
    pw = w // Q
    first = jnp.where(x == 0, c, 0)
    last = jnp.where(x == 0, R - 1, c)
    chained = (z >= first) & (z <= last)
    diag = z == c
    pair = (x == 1) & (z == x * S + 1) & (s == 0)
    catcher = (x == 0) & diag & (z == 1)
    relay = (x == 1) & (z == x * S) & (s == 1 - x)
    helper = (x == 0) & (z == 0) & (s == 1)
    adds = (x == 1) & chained
    weight = jnp.where(diag, 0.5, 1.0).astype(jnp.float32)
    other = 1 - s

    def rows(i, n):
        return pl.ds(pl.multiple_of(i * n, n), n)

    def block(hh, ss):
        return pl.ds(pl.multiple_of((hh * S + ss) * kd, kd), kd)

    barrier = pltpu.get_barrier_semaphore()
    pl.semaphore_signal(barrier, inc=1, device_id={"sub": other}, device_id_type=MESH)
    for q in range(R):
        if q > 0:
            pl.semaphore_signal(barrier, inc=1, device_id={"row": lax.rem(z + q, R)}, device_id_type=MESH)
        pl.semaphore_signal(barrier, inc=1, device_id={"col": 1 - x, "row": q}, device_id_type=MESH)

    @pl.when(z > 0)
    def _():
        pl.semaphore_signal(barrier, inc=1, device_id={"row": z - 1, "sub": other}, device_id_type=MESH)

    @pl.when(z < R - 1)
    def _():
        pl.semaphore_signal(barrier, inc=1, device_id={"row": z + 1, "sub": other}, device_id_type=MESH)

    def load(i):
        return pltpu.make_async_copy(a.at[:, rows(i, w)], abuf.at[lax.rem(i, 2)], asem.at[lax.rem(i, 2)])

    def mate():
        return pltpu.make_async_remote_copy(
            v, vall.at[:, block(0, s)], os, orr, device_id={"sub": other}, device_id_type=MESH)

    def across(i):
        return pltpu.make_async_remote_copy(
            v.at[rows(i, w), :], vall.at[rows(i, w), block(1, s)], xs.at[i], xr.at[i],
            device_id={"col": 1 - x}, device_id_type=MESH)

    def share(i):
        here = vall.at[rows(i, w), block(1, s)]
        return pltpu.make_async_remote_copy(
            here, here, fs.at[i], fr.at[i], device_id={"sub": other}, device_id_type=MESH)

    def hand(i):
        return pltpu.make_async_remote_copy(
            vall.at[rows(i, w), pl.ds(half, half)], ubuf.at[rows(i, w), :], hs.at[i], hr.at[i],
            device_id={"row": z + 1}, device_id_type=MESH)

    def lift(i):
        return pltpu.make_async_remote_copy(
            sbuf.at[rows(i, w), :], ubuf.at[rows(i, w), :], hs.at[i], hr.at[i],
            device_id={"row": z + 1}, device_id_type=MESH)

    def origin(k):
        return pltpu.make_async_remote_copy(
            vall.at[rows(k, pw), pl.ds(0, half)], sbuf.at[rows(k, pw), :], ts.at[k], tr.at[k],
            device_id={"row": z + 1}, device_id_type=MESH)

    def onward(k):
        return pltpu.make_async_remote_copy(
            sbuf.at[rows(k, pw), :], sbuf.at[rows(k, pw), :], ts.at[k], tr.at[k],
            device_id={"row": z + 1}, device_id_type=MESH)

    own = pltpu.make_async_copy(v, vall.at[:, block(0, s)], lsem)
    own.start()
    load(0).start()
    img[...] = jnp.zeros_like(img)
    ybuf[...] = jnp.zeros_like(ybuf)
    pl.semaphore_wait(barrier, 2 * R + (z > 0).astype(jnp.int32) + (z < R - 1).astype(jnp.int32))
    mate().start()

    def begin(i, carry):
        across(i).start()
        return carry

    lax.fori_loop(0, steps, begin, 0)
    own.wait()
    mate().wait_recv()
    source = (x == 0) & diag

    @pl.when(source)
    def _():
        def send(k, carry):
            origin(k).start()
            return carry
        lax.fori_loop(0, steps * Q, send, 0)

    def prepare(i, hh):
        here, columns = rows(i, w), pl.ds(hh * half, half)
        high, low = split(vall[here, columns])
        vhi[here, columns] = high
        vlo[here, columns] = low

    def prepare_own(i, carry):
        prepare(i, 0)
        return carry

    lax.fori_loop(0, steps, prepare_own, 0)

    def multiply(columns):
        def tile(t, carry):
            here = rows(t, w)
            img[here, columns] += dot3(ahi[here, :], alo[here, :], rhi[...], rlo[...], (1,))
            return carry
        lax.fori_loop(0, steps, tile, 0)

    def feed(value):
        high, low = split(value)
        rhi[...] = high
        rlo[...] = low

    def open_block(i):
        load(i).wait()

        @pl.when(i < steps - 1)
        def _():
            load(i + 1).start()

        def cut(t, carry):
            high, low = split(abuf[lax.rem(i, 2), rows(t, w), :])
            ahi[rows(t, w), :] = high
            alo[rows(t, w), :] = low
            return carry
        lax.fori_loop(0, steps, cut, 0)

    def receive(i):
        across(i).wait_recv()
        share(i).start()

    def collect(i):
        share(i).wait_recv()
        prepare(i, 1)

        @pl.when(relay)
        def _():
            hand(i).start()

    def fold(hh):
        columns = pl.ds(hh * half, half)

        def halve(t, carry):
            high, low = split(img[rows(t, w), columns])
            ihi[rows(t, w), :] = high
            ilo[rows(t, w), :] = low
            return carry
        lax.fori_loop(0, steps, halve, 0)
        def act(b, carry):
            here = rows(b, kd)
            ybuf[here, columns] = dot3(vhi[:, here], vlo[:, here], ihi[...], ilo[...], (0,))
            return carry
        lax.fori_loop(0, 2 * S, act, 0)

    def absorb(value, hh, i):
        feed(value)

        def act(b, carry):
            here, columns = rows(b, kd), pl.ds(hh * half, half)
            ybuf[here, columns] += dot3(vhi[rows(i, w), here], vlo[rows(i, w), here], rhi[...], rlo[...], (0,))
            return carry
        lax.fori_loop(0, 2 * S, act, 0)

    def local_step(i, carry):
        @pl.when(i == 0)
        def _():
            receive(i)

        @pl.when(i < steps - 1)
        def _():
            receive(i + 1)
        open_block(i)

        @pl.when(x == 0)
        def _():
            feed(0.5 * vall[rows(i, w), pl.ds(0, half)])
            multiply(pl.ds(0, half))
        collect(i)
        feed(0.5 * vall[rows(i, w), pl.ds(half, half)])
        multiply(pl.ds(half, half))
        return carry

    def piece(k, p=0, buffer=None):
        @pl.when(chained & (z > first))
        def _():
            onward(k).wait_recv()

        if buffer is not None:
            @pl.when(adds & (z == first))
            def _():
                sbuf[rows(k, pw), :] = tbuf[buffer, rows(p, pw), :]

            @pl.when(adds & (z > first))
            def _():
                sbuf[rows(k, pw), :] += tbuf[buffer, rows(p, pw), :]

        @pl.when(chained & (z < last))
        def _():
            onward(k).start()

    def own_tile(i):
        open_block(i)

        @pl.when(adds)
        def _():
            tbuf[lax.rem(i, 2)] = weight * dot3(ahi[...], alo[...], vhi[:, :half], vlo[:, :half], (0,))

    def stream_step(i, carry):
        @pl.when(jnp.logical_not(diag) & (2 * i < steps))
        def _():
            receive(2 * i)
            receive(2 * i + 1)

        @pl.when(i < steps - 1)
        def _():
            own_tile(i + 1)

        def next_piece(p, c2):
            piece(i * Q + p, p, lax.rem(i, 2))
            return c2
        lax.fori_loop(0, Q, next_piece, 0)

        lag = steps // 2

        @pl.when(jnp.logical_not(diag) & (i >= lag) & (2 * (i - lag) < steps))
        def _():
            collect(2 * (i - lag))
            collect(2 * (i - lag) + 1)

        @pl.when(diag)
        def _():
            absorb(sbuf[rows(i, w), :], 0, i)
        return carry

    early = jnp.where((x == 0) & (z == 1), steps, 3 * steps // 8)
    left = (steps - early) * Q
    turns = steps * 2 * S

    def early_step(i, carry):
        @pl.when(2 * i < steps)
        def _():
            receive(2 * i)
            receive(2 * i + 1)

        def next_piece(p, c2):
            piece(i * Q + p)
            return c2
        lax.fori_loop(0, Q, next_piece, 0)
        return carry

    def wide_step(n, carry):
        open_block(n)

        def widen(b, c2):
            here = rows(b, kd)
            high, low = split(dot3(vhi[:, here], vlo[:, here], ahi[...], alo[...], (0,)))
            whi[here, :] = high
            wlo[here, :] = low

            turn = n * 2 * S + b

            @pl.when((turn + 1) * left // turns > turn * left // turns)
            def _():
                piece(early * Q + turn * left // turns)
            return c2
        lax.fori_loop(0, 2 * S, widen, 0)

        @pl.when(x == 0)
        def _():
            feed(sbuf[rows(n, w), :])

        @pl.when(x == 1)
        def _():
            hand(n).wait_recv()
            feed(ubuf[rows(n, w), :])
        columns = rows(x, half)

        def add(b, c2):
            here = rows(b, kd)
            ybuf[here, columns] += dot3(whi[here, :], wlo[here, :], rhi[...], rlo[...], (1,))
            return c2
        lax.fori_loop(0, 2 * S, add, 0)
        return carry

    @pl.when(diag)
    def _():
        lax.fori_loop(0, steps, local_step, 0)
        fold(1)

        @pl.when(x == 0)
        def _():
            fold(0)

        @pl.when(x == 1)
        def _():
            load(0).start()

    @pl.when(catcher)
    def _():
        def catch(i, carry):
            lift(i).wait_recv()
            absorb(ubuf[rows(i, w), :], 1, i)
            return carry
        lax.fori_loop(0, steps, catch, 0)

    @pl.when(helper)
    def _():
        def obtain(i, carry):
            receive(i)
            return carry

        def keep(i, carry):
            collect(i)
            return carry

        def raise_step(i, carry):
            open_block(i)
            sbuf[rows(i, w), :] = dot3(ahi[...], alo[...], vhi[:, half:], vlo[:, half:], (0,))
            lift(i).start()
            return carry
        lax.fori_loop(0, steps, obtain, 0)
        lax.fori_loop(0, steps, keep, 0)
        lax.fori_loop(0, steps, raise_step, 0)

    wide = pair | ((x == 0) & chained & jnp.logical_not(diag))

    @pl.when(wide)
    def _():
        def keep_all(i, carry):
            collect(i)
            return carry
        lax.fori_loop(0, early, early_step, 0)

        def rest(i, carry):
            receive(i)
            return carry
        lax.fori_loop(jnp.minimum(2 * early, steps), steps, rest, 0)
        lax.fori_loop(0, steps, keep_all, 0)
        lax.fori_loop(0, steps, wide_step, 0)

    @pl.when((x == 1) & jnp.logical_not(pair))
    def _():
        own_tile(0)
        lax.fori_loop(0, steps, stream_step, 0)

    reduce_blocks(R, S, blocks, out, ybuf, part, r_sub, r_col, r_row, flip, tile_ref,
                  ps, pr, qs, qr, us, ur, gs, gr, es, er)
    mate().wait_send()

    def drain(i, carry):
        across(i).wait_send()
        share(i).wait_send()

        @pl.when(relay)
        def _():
            hand(i).wait_send()

        @pl.when(helper)
        def _():
            lift(i).wait_send()
        return carry

    lax.fori_loop(0, steps, drain, 0)

    def sent(k, carry):
        @pl.when(source)
        def _():
            origin(k).wait_send()

        @pl.when(chained & (z < last) & jnp.logical_not(source))
        def _():
            onward(k).wait_send()
        return carry

    lax.fori_loop(0, steps * Q, sent, 0)


def image(v, a, R, S):
    m, kd = v.shape
    w = kd
    steps = m // w
    Q = 4
    half = S * kd
    dma = pltpu.SemaphoreType.DMA
    f32, bf16 = jnp.float32, jnp.bfloat16
    blocks, most = owners(R, S)
    nb, hr = len(blocks), kd // S
    return pl.pallas_call(
        functools.partial(image_kernel, R, S, Q, blocks),
        out_shape=jax.ShapeDtypeStruct((kd, half), f32),
        in_specs=[pl.BlockSpec(memory_space=pltpu.VMEM), pl.BlockSpec(memory_space=pl.ANY)],
        out_specs=pl.BlockSpec(memory_space=pltpu.VMEM),
        scratch_shapes=[
            pltpu.VMEM((m, 2 * half), f32), pltpu.VMEM((m, 2 * half), f32),
            pltpu.VMEM((2 * half, 2 * half), f32),
            pltpu.VMEM((m, half), f32), pltpu.VMEM((m, half), f32), pltpu.VMEM((2, w, half), f32),
            pltpu.VMEM((2, m, w), f32), pltpu.VMEM((m, w), bf16), pltpu.VMEM((m, w), bf16),
            pltpu.VMEM((m, 2 * half), bf16), pltpu.VMEM((m, 2 * half), bf16),
            pltpu.VMEM((m, half), bf16), pltpu.VMEM((m, half), bf16),
            pltpu.VMEM((w, half), bf16), pltpu.VMEM((w, half), bf16),
            pltpu.VMEM((2 * half, w), bf16), pltpu.VMEM((2 * half, w), bf16),
            dma, dma((2,)), dma, dma, dma((steps,)), dma((steps,)), dma((steps,)), dma((steps,)),
            dma((steps,)), dma((steps,)), dma((steps * Q,)), dma((steps * Q,)),
            pltpu.VMEM((nb, kd, kd), f32), pltpu.VMEM((nb, hr, kd), f32), pltpu.VMEM((nb, hr, kd), f32),
            pltpu.VMEM((R, most, hr, kd), f32), pltpu.VMEM((nb, kd, hr), f32), pltpu.VMEM((S, kd, kd), f32),
            dma((nb,)), dma((nb,)), dma((nb,)), dma((nb,)), dma((nb,)), dma((R, most)),
            dma((nb,)), dma((nb,)), dma((S,)), dma((S,)),
        ],
        compiler_params=pltpu.CompilerParams(
            collective_id=3, has_side_effects=True, vmem_limit_bytes=66_000_000),
        cost_estimate=pl.CostEstimate(flops=0, bytes_accessed=100_000_000, transcendentals=0),
        name="image",
    )(v, a)


def partial_general(matrix, basis_vectors):
    R = lax.axis_size("row")
    S = lax.axis_size("sub")
    C = lax.axis_size("col") * S
    m, kd = basis_vectors.shape
    K = kd * C
    n = matrix.shape[1]
    per = n // m
    piece = m // R
    own, spread = gather(basis_vectors, R, C // S, S)
    width = K // CHUNKS
    images = []
    for c in range(CHUNKS):
        part = lax.dot_general(
            matrix,
            own[:, c * width : (c + 1) * width],
            (((0,), (0,)), ((), ())),
            precision=lax.Precision.HIGH,
            preferred_element_type=jnp.float32,
        )
        if c == 0:
            part, spread = lax.optimization_barrier((part, spread))
        part = part.reshape(per, R, piece, width).transpose(1, 0, 2, 3).reshape(R * per * piece, width)
        images.append(lax.psum_scatter(part, "row", scatter_dimension=0, tiled=True))
    mine = regroup(spread, C // S, S).reshape(per * piece, K)
    return jnp.concatenate(
        [
            lax.dot_general(
                mine,
                image,
                (((0,), (0,)), ((), ())),
                precision=lax.Precision.HIGH,
                preferred_element_type=jnp.float32,
            )
            for image in images
        ],
        axis=1,
    )


def shards(matrix, basis_vectors, split_size):
    R = lax.axis_size("row")
    X = lax.axis_size("col")
    S = lax.axis_size("sub")
    m, n = matrix.shape
    halves = m == n and R == X * S and X == 2 and S == 2
    if halves:
        child_block = image(basis_vectors, matrix, R, S)
    else:
        child_block = project(partial_general(matrix, basis_vectors), R, X, S)
    row_ids = (
        jnp.arange(child_block.shape[0], dtype=jnp.int32)
        + lax.axis_index("row") * child_block.shape[0]
    )
    col_ids = (
        jnp.arange(child_block.shape[1], dtype=jnp.int32)
        + lax.axis_index("col") * child_block.shape[1]
    )
    leading = split_size[0]
    row_first = row_ids < leading
    col_first = col_ids < leading
    mask_one = row_first[:, None] & col_first[None, :]
    mask_two = jnp.logical_not(row_first)[:, None] & jnp.logical_not(col_first)[None, :]
    selected = jnp.where(lax.axis_index("sub") == 0, mask_one, mask_two)
    return jnp.where(selected, child_block, jnp.zeros((), jnp.float32))[None]


def solution(mesh):
    placed = (
        P(("groups", "row"), ("col", "sub")),
        P(("groups", "row"), ("col", "sub")),
        P("groups"),
    )
    return jax.shard_map(
        shards,
        mesh=mesh,
        in_specs=placed,
        out_specs=P("sub", ("groups", "row"), "col"),
        check_vma=False,
    )
```

```python
import functools

import jax
import jax.numpy as jnp
from jax import lax
from jax.experimental import pallas as pl
from jax.experimental.pallas import tpu as pltpu
from jax.sharding import PartitionSpec as P

MESH = pl.DeviceIdType.MESH
CHUNKS = 1


def gather_kernel(R, X, S, v, own, spread, lsem, xs, xr, zs, zr, ps, pr, fs, fr):
    r, x, s = lax.axis_index("row"), lax.axis_index("col"), lax.axis_index("sub")
    m, kd = v.shape
    piece = m // R

    def columns(cx, cs):
        return pl.ds(pl.multiple_of((cx * S + cs) * kd, kd), kd)

    peers = [{"col": lax.rem(x + d, X)} for d in range(1, X)]
    peers += [{"row": lax.rem(r + d, R)} for d in range(1, R)]
    peers += [{"sub": lax.rem(s + d, S)} for d in range(1, S)]
    barrier = pltpu.get_barrier_semaphore()
    for peer in peers:
        pl.semaphore_signal(barrier, inc=1, device_id=peer, device_id_type=MESH)
    pl.semaphore_wait(barrier, len(peers))

    mine = own.at[:, columns(x, s)]
    across, spreads, partner, forward = [], [], [], []
    for d in range(1, X):
        across.append(pltpu.make_async_remote_copy(
            v, mine, xs.at[d - 1], xr.at[d - 1],
            device_id={"col": lax.rem(x + d, X)}, device_id_type=MESH))
    for d in range(1, R):
        i = lax.rem(r + d, R)
        spreads.append(pltpu.make_async_remote_copy(
            v.at[pl.ds(pl.multiple_of(i * piece, piece), piece), :], spread.at[r],
            zs.at[d - 1], zr.at[d - 1],
            device_id={"row": i}, device_id_type=MESH))
    for d in range(1, S):
        partner.append(pltpu.make_async_remote_copy(
            v, mine, ps.at[d - 1], pr.at[d - 1],
            device_id={"sub": lax.rem(s + d, S)}, device_id_type=MESH))
    for copy in across + spreads + partner:
        copy.start()
    local = [
        pltpu.make_async_copy(v, mine, lsem.at[0]),
        pltpu.make_async_copy(
            v.at[pl.ds(pl.multiple_of(r * piece, piece), piece), :], spread.at[r], lsem.at[1]),
    ]
    for copy in local:
        copy.start()
    for d in range(1, X):
        across[d - 1].wait_recv()
        block = own.at[:, columns(lax.rem(x - d + X, X), s)]
        for e in range(1, S):
            copy = pltpu.make_async_remote_copy(
                block, block, fs.at[d - 1, e - 1], fr.at[d - 1, e - 1],
                device_id={"sub": lax.rem(s + e, S)}, device_id_type=MESH)
            copy.start()
            forward.append(copy)
    for copy in across:
        copy.wait_send()
    for copy in spreads + partner + forward:
        copy.wait()
    for copy in local:
        copy.wait()


def gather(v, R, X, S):
    m, kd = v.shape
    dma = pltpu.SemaphoreType.DMA
    return pl.pallas_call(
        functools.partial(gather_kernel, R, X, S),
        out_shape=(
            jax.ShapeDtypeStruct((m, kd * X * S), v.dtype),
            jax.ShapeDtypeStruct((R, m // R, kd), v.dtype),
        ),
        in_specs=[pl.BlockSpec(memory_space=pltpu.VMEM)],
        out_specs=(pl.BlockSpec(memory_space=pl.ANY), pl.BlockSpec(memory_space=pl.ANY)),
        scratch_shapes=[
            dma((2,)), dma((X - 1,)), dma((X - 1,)), dma((R - 1,)), dma((R - 1,)),
            dma((S - 1,)), dma((S - 1,)), dma((X - 1, S - 1)), dma((X - 1, S - 1)),
        ],
        compiler_params=pltpu.CompilerParams(collective_id=0, has_side_effects=True),
        cost_estimate=pl.CostEstimate(flops=0, bytes_accessed=100_000_000, transcendentals=0),
        name="gather",
    )(v)


def regroup_kernel(X, S, spread, mine, lsem, ss, rs):
    x, s = lax.axis_index("col"), lax.axis_index("sub")
    C = X * S
    k = x * S + s
    R, piece, kd = spread.shape
    per = R // C
    barrier = pltpu.get_barrier_semaphore()
    dests = [lax.rem(k + e, C) for e in range(C)]
    for j in dests[1:]:
        pl.semaphore_signal(
            barrier, inc=1, device_id={"col": j // S, "sub": lax.rem(j, S)}, device_id_type=MESH)
    pl.semaphore_wait(barrier, C - 1)
    target = mine.at[:, :, pl.ds(pl.multiple_of(k * kd, kd), kd)]
    copies = []
    for e in range(1, C):
        j = dests[e]
        copies.append(pltpu.make_async_remote_copy(
            spread.at[pl.ds(j * per, per)], target, ss.at[e - 1], rs.at[e - 1],
            device_id={"col": j // S, "sub": lax.rem(j, S)}, device_id_type=MESH))
    copies.append(pltpu.make_async_copy(spread.at[pl.ds(k * per, per)], target, lsem))
    for copy in copies:
        copy.start()
    for copy in copies:
        copy.wait()


def regroup(spread, X, S):
    R, piece, kd = spread.shape
    C = X * S
    dma = pltpu.SemaphoreType.DMA
    return pl.pallas_call(
        functools.partial(regroup_kernel, X, S),
        out_shape=jax.ShapeDtypeStruct((R // C, piece, kd * C), spread.dtype),
        in_specs=[pl.BlockSpec(memory_space=pltpu.VMEM)],
        out_specs=pl.BlockSpec(memory_space=pl.ANY),
        scratch_shapes=[dma, dma((C - 1,)), dma((C - 1,))],
        compiler_params=pltpu.CompilerParams(collective_id=1, has_side_effects=True),
        cost_estimate=pl.CostEstimate(flops=0, bytes_accessed=60_000_000, transcendentals=0),
        name="regroup",
    )(spread)


def project_kernel(R, X, S, p, out, acc, from_sub, from_col, from_row, res, from_pair,
                   a_s, a_r, b_s, b_r, c_s, c_r, d_s, d_r):
    r, x, s = lax.axis_index("row"), lax.axis_index("col"), lax.axis_index("sub")
    K = p.shape[0]
    rb, kd = K // R, K // (X * S)

    def rows(i):
        return pl.ds(pl.multiple_of(i * rb, rb), rb)

    def columns(cx, cs):
        return pl.ds(pl.multiple_of((cx * S + cs) * kd, kd), kd)

    def col(d):
        return lax.rem(x + d, X)

    peers = [{"col": col(d)} for d in range(1, X)]
    peers += [{"row": lax.rem(r + d, R)} for d in range(1, R)]
    peers += [{"sub": lax.rem(s + d, S)} for d in range(1, S)]
    barrier = pltpu.get_barrier_semaphore()
    for peer in peers:
        pl.semaphore_signal(barrier, inc=1, device_id=peer, device_id_type=MESH)
    pl.semaphore_wait(barrier, len(peers))

    order = list(range(1, X)) + [0]
    steps = list(range(1, R)) + [0]
    pair = {}
    for d in order:
        for e in range(1, S):
            other = lax.rem(s + e, S)
            pair[d, e] = pltpu.make_async_remote_copy(
                p.at[:, columns(col(d), other)], from_sub.at[e - 1, d],
                a_s.at[e - 1, d], a_r.at[e - 1, d],
                device_id={"sub": other}, device_id_type=MESH)
            pair[d, e].start()
    cross = {}
    for d in order:
        for e in range(1, S):
            pair[d, e].wait_recv()
        for q in steps:
            here = rows(lax.rem(r + q, R))
            total = p[here, columns(col(d), s)]
            for e in range(1, S):
                total = total + from_sub[e - 1, d, here, :]
            acc[d, here, :] = total
            if d > 0:
                cross[d, q] = pltpu.make_async_remote_copy(
                    acc.at[d, here], from_col.at[d - 1, here],
                    b_s.at[d - 1, q], b_r.at[d - 1, q],
                    device_id={"col": col(d)}, device_id_type=MESH)
                cross[d, q].start()
    along = []
    for q in steps:
        i = lax.rem(r + q, R)
        here = rows(i)
        total = acc[0, here, :]
        for d in range(1, X):
            cross[d, q].wait_recv()
            total = total + from_col[d - 1, here, :]
        if q > 0:
            acc[0, here, :] = total
            copy = pltpu.make_async_remote_copy(
                acc.at[0, here], from_row.at[q - 1], c_s.at[q - 1], c_r.at[q - 1],
                device_id={"row": i}, device_id_type=MESH)
            copy.start()
            along.append(copy)
    for q in range(1, R):
        along[q - 1].wait_recv()
        total = total + from_row[q - 1]
    res[...] = total
    last = []
    for e in range(1, S):
        copy = pltpu.make_async_remote_copy(
            res, from_pair.at[e - 1], d_s.at[e - 1], d_r.at[e - 1],
            device_id={"sub": lax.rem(s + e, S)}, device_id_type=MESH)
        copy.start()
        last.append(copy)
    out[:, pl.ds(pl.multiple_of(s * kd, kd), kd)] = total
    for e in range(1, S):
        last[e - 1].wait_recv()
        out[:, pl.ds(pl.multiple_of(lax.rem(s - e + S, S) * kd, kd), kd)] = from_pair[e - 1]
    for copy in list(pair.values()) + list(cross.values()) + along + last:
        copy.wait_send()


def project(partial, R, X, S):
    K = partial.shape[0]
    rb, kd = K // R, K // (X * S)
    dma = pltpu.SemaphoreType.DMA
    f32 = jnp.float32
    return pl.pallas_call(
        functools.partial(project_kernel, R, X, S),
        out_shape=jax.ShapeDtypeStruct((rb, S * kd), f32),
        in_specs=[pl.BlockSpec(memory_space=pltpu.VMEM)],
        out_specs=pl.BlockSpec(memory_space=pltpu.VMEM),
        scratch_shapes=[
            pltpu.VMEM((X, K, kd), f32),
            pltpu.VMEM((S - 1, X, K, kd), f32),
            pltpu.VMEM((X - 1, K, kd), f32),
            pltpu.VMEM((R - 1, rb, kd), f32),
            pltpu.VMEM((rb, kd), f32),
            pltpu.VMEM((S - 1, rb, kd), f32),
            dma((S - 1, X)), dma((S - 1, X)), dma((X - 1, R)), dma((X - 1, R)),
            dma((R - 1,)), dma((R - 1,)), dma((S - 1,)), dma((S - 1,)),
        ],
        compiler_params=pltpu.CompilerParams(collective_id=2, has_side_effects=True),
        cost_estimate=pl.CostEstimate(flops=0, bytes_accessed=60_000_000, transcendentals=0),
        name="project",
    )(partial)


def split(value):
    high = value.astype(jnp.bfloat16)
    return high, (value - high.astype(jnp.float32)).astype(jnp.bfloat16)


def dot3(a_high, a_low, b_high, b_low, contract):
    def one(a, b):
        return lax.dot_general(a, b, ((contract, (0,)), ((), ())),
                               preferred_element_type=jnp.float32)
    return one(a_high, b_high) + (one(a_high, b_low) + one(a_low, b_high))


def owners(R, S):
    blocks, chips, columns = [], {}, {}
    pairs = [(i, i) for i in range(R)]
    pairs += sorted(((i, j) for i in range(R) for j in range(i + 1, R)), key=lambda p: (p[0] - p[1], p))
    for i, j in pairs:
        choices = [(j // S, i), (i // S, j)]
        best = min(choices, key=lambda o: (chips.get(o, 0), columns.get(o[0], 0)))
        slot = chips.get(best, 0)
        chips[best] = slot + 1
        columns[best[0]] = columns.get(best[0], 0) + 1
        blocks.append((i, j, best[0], best[1], slot))
    return blocks[R:] + blocks[:R], max(chips.values())


def reduce_blocks(R, S, blocks, out, ybuf, part, r_sub, r_col, r_row, flip, tile_ref,
                  ps, pr, qs, qr, us, ur, gs, gr, es, er):
    z, x, s = lax.axis_index("row"), lax.axis_index("col"), lax.axis_index("sub")
    other = 1 - s
    kd = part.shape[1]
    hr = kd // S
    mine = pl.ds(pl.multiple_of(s * hr, hr), hr)
    theirs = pl.ds(pl.multiple_of(other * hr, hr), hr)

    def filled(t, side):
        i, j = blocks[t][:2]
        inner = z // S == side
        return inner if side == 1 or min(i // S, j // S) > 0 else z >= 0

    def held(g):
        return pl.ds(pl.multiple_of((jnp.where(x == g // S, 0, 1) * S + g % S) * kd, kd), kd)

    def swap(t):
        return pltpu.make_async_remote_copy(
            part.at[t, theirs, :], r_sub.at[t], ps.at[t], pr.at[t],
            device_id={"sub": other}, device_id_type=MESH)

    def cross(t):
        return pltpu.make_async_remote_copy(
            part.at[t, mine, :], r_col.at[t], qs.at[t], qr.at[t],
            device_id={"col": 1 - x}, device_id_type=MESH)

    def along(t, sender):
        return pltpu.make_async_remote_copy(
            part.at[t, mine, :], r_row.at[sender, blocks[t][4]], us.at[t], ur.at[sender, blocks[t][4]],
            device_id={"row": blocks[t][3]}, device_id_type=MESH)

    def region(t, direct):
        i, j = blocks[t][:2]
        if direct:
            return tile_ref.at[j % S, mine, :]
        return tile_ref.at[i % S, :, mine]

    def chip(t, direct):
        i, j = blocks[t][:2]
        return (j // S, i) if direct else (i // S, j)

    def far(t, direct):
        xo, zo = chip(t, direct)
        return pltpu.make_async_remote_copy(
            part.at[t, mine, :] if direct else flip.at[t], region(t, direct), gs.at[t], gr.at[t],
            device_id={"col": xo, "row": zo}, device_id_type=MESH)

    def near(t, direct):
        slot = blocks[t][1] % S if direct else blocks[t][0] % S
        return pltpu.make_async_remote_copy(
            region(t, direct), region(t, direct), es.at[slot], er.at[slot],
            device_id={"sub": other}, device_id_type=MESH)

    for t, (i, j, xo, zo, slot) in enumerate(blocks):
        part[t] = ybuf[held(i), held(j)] + ybuf[held(j), held(i)].T
        swap(t).start()
    for t, (i, j, xo, zo, slot) in enumerate(blocks):
        swap(t).wait_recv()
        part[t, mine, :] += r_sub[t]

        @pl.when((x != xo) & filled(t, 1 - xo))
        def _():
            cross(t).start()
    for t, (i, j, xo, zo, slot) in enumerate(blocks):
        @pl.when((x == xo) & filled(t, 1 - xo))
        def _():
            cross(t).wait_recv()
            part[t, mine, :] += r_col[t]

        @pl.when((x == xo) & (z != zo))
        def _():
            along(t, z).start()
    for t, (i, j, xo, zo, slot) in enumerate(blocks):
        straight = (xo, zo) == (j // S, i)

        @pl.when((x == xo) & (z == zo))
        def _():
            for q in range(R):
                if q != zo:
                    along(t, q).wait_recv()
                    part[t, mine, :] += r_row[q, slot]
            value = part[t, mine, :]
            if i != j:
                flip[t] = value.T
                far(t, not straight).start()
            if straight:
                tile_ref[j % S, mine, :] = value
            else:
                tile_ref[i % S, :, mine] = value.T
            near(t, straight).start()
    for t, (i, j, xo, zo, slot) in enumerate(blocks):
        straight = (xo, zo) == (j // S, i)
        if i != j:
            xf, zf = chip(t, not straight)

            @pl.when((x == xf) & (z == zf))
            def _():
                far(t, not straight).wait_recv()
                near(t, not straight).start()
    for t, (i, j, xo, zo, slot) in enumerate(blocks):
        straight = (xo, zo) == (j // S, i)
        swap(t).wait_send()

        @pl.when((x != xo) & filled(t, 1 - xo))
        def _():
            cross(t).wait_send()

        @pl.when((x == xo) & (z != zo))
        def _():
            along(t, z).wait_send()
        for direct in ((straight, not straight) if i != j else (straight,)):
            xn, zn = chip(t, direct)

            @pl.when((x == xn) & (z == zn))
            def _():
                near(t, direct).wait()
        if i != j:
            @pl.when((x == xo) & (z == zo))
            def _():
                far(t, not straight).wait_send()
    for b in range(S):
        out[:, b * kd:(b + 1) * kd] = tile_ref[b]


def image_kernel(R, S, Q, blocks, v, a, out, vall, img, ybuf, sbuf, ubuf, tbuf, abuf, ahi, alo, vhi, vlo,
                 ihi, ilo, rhi, rlo, whi, wlo, lsem, asem, os, orr, xs, xr, fs, fr, hs, hr, ts, tr,
                 part, r_sub, r_col, r_row, flip, tile_ref, ps, pr, qs, qr, us, ur, gs, gr, es, er):
    z, x, s = lax.axis_index("row"), lax.axis_index("col"), lax.axis_index("sub")
    c = x * S + s
    m, kd = v.shape
    half = S * kd
    steps = m // abuf.shape[2]
    w = m // steps
    pw = w // Q
    first = jnp.where(x == 0, c, 0)
    last = jnp.where(x == 0, R - 1, c)
    chained = (z >= first) & (z <= last)
    diag = z == c
    pair = (x == 1) & (z == x * S + 1) & (s == 0)
    catcher = (x == 0) & diag & (z == 1)
    relay = (x == 1) & (z == x * S) & (s == 1 - x)
    helper = (x == 0) & (z == 0) & (s == 1)
    adds = (x == 1) & chained
    weight = jnp.where(diag, 0.5, 1.0).astype(jnp.float32)
    other = 1 - s

    def rows(i, n):
        return pl.ds(pl.multiple_of(i * n, n), n)

    def block(hh, ss):
        return pl.ds(pl.multiple_of((hh * S + ss) * kd, kd), kd)

    barrier = pltpu.get_barrier_semaphore()
    pl.semaphore_signal(barrier, inc=1, device_id={"sub": other}, device_id_type=MESH)
    for q in range(R):
        if q > 0:
            pl.semaphore_signal(barrier, inc=1, device_id={"row": lax.rem(z + q, R)}, device_id_type=MESH)
        pl.semaphore_signal(barrier, inc=1, device_id={"col": 1 - x, "row": q}, device_id_type=MESH)

    @pl.when(z > 0)
    def _():
        pl.semaphore_signal(barrier, inc=1, device_id={"row": z - 1, "sub": other}, device_id_type=MESH)

    @pl.when(z < R - 1)
    def _():
        pl.semaphore_signal(barrier, inc=1, device_id={"row": z + 1, "sub": other}, device_id_type=MESH)

    def load(i):
        return pltpu.make_async_copy(a.at[:, rows(i, w)], abuf.at[lax.rem(i, 2)], asem.at[lax.rem(i, 2)])

    def mate():
        return pltpu.make_async_remote_copy(
            v, vall.at[:, block(0, s)], os, orr, device_id={"sub": other}, device_id_type=MESH)

    def across(i):
        return pltpu.make_async_remote_copy(
            v.at[rows(i, w), :], vall.at[rows(i, w), block(1, s)], xs.at[i], xr.at[i],
            device_id={"col": 1 - x}, device_id_type=MESH)

    def share(i):
        here = vall.at[rows(i, w), block(1, s)]
        return pltpu.make_async_remote_copy(
            here, here, fs.at[i], fr.at[i], device_id={"sub": other}, device_id_type=MESH)

    def hand(i):
        return pltpu.make_async_remote_copy(
            vall.at[rows(i, w), pl.ds(half, half)], ubuf.at[rows(i, w), :], hs.at[i], hr.at[i],
            device_id={"row": z + 1}, device_id_type=MESH)

    def lift(i):
        return pltpu.make_async_remote_copy(
            sbuf.at[rows(i, w), :], ubuf.at[rows(i, w), :], hs.at[i], hr.at[i],
            device_id={"row": z + 1}, device_id_type=MESH)

    def origin(k):
        return pltpu.make_async_remote_copy(
            vall.at[rows(k, pw), pl.ds(0, half)], sbuf.at[rows(k, pw), :], ts.at[k], tr.at[k],
            device_id={"row": z + 1}, device_id_type=MESH)

    def onward(k):
        return pltpu.make_async_remote_copy(
            sbuf.at[rows(k, pw), :], sbuf.at[rows(k, pw), :], ts.at[k], tr.at[k],
            device_id={"row": z + 1}, device_id_type=MESH)

    own = pltpu.make_async_copy(v, vall.at[:, block(0, s)], lsem)
    own.start()
    load(0).start()
    pl.semaphore_wait(barrier, 2 * R + (z > 0).astype(jnp.int32) + (z < R - 1).astype(jnp.int32))
    mate().start()

    def begin(i, carry):
        across(i).start()
        return carry

    lax.fori_loop(0, steps, begin, 0)
    img[...] = jnp.zeros_like(img)
    ybuf[...] = jnp.zeros_like(ybuf)
    own.wait()
    mate().wait_recv()
    source = (x == 0) & diag

    @pl.when(source)
    def _():
        def send(k, carry):
            origin(k).start()
            return carry
        lax.fori_loop(0, steps * Q, send, 0)

    def prepare(i, hh):
        here, columns = rows(i, w), pl.ds(hh * half, half)
        high, low = split(vall[here, columns])
        vhi[here, columns] = high
        vlo[here, columns] = low

    def prepare_own(i, carry):
        prepare(i, 0)
        return carry

    lax.fori_loop(0, steps, prepare_own, 0)

    def multiply(columns):
        def tile(t, carry):
            here = rows(t, w)
            img[here, columns] += dot3(ahi[here, :], alo[here, :], rhi[...], rlo[...], (1,))
            return carry
        lax.fori_loop(0, steps, tile, 0)

    def feed(value):
        high, low = split(value)
        rhi[...] = high
        rlo[...] = low

    def open_block(i):
        load(i).wait()

        @pl.when(i < steps - 1)
        def _():
            load(i + 1).start()

        def cut(t, carry):
            high, low = split(abuf[lax.rem(i, 2), rows(t, w), :])
            ahi[rows(t, w), :] = high
            alo[rows(t, w), :] = low
            return carry
        lax.fori_loop(0, steps, cut, 0)

    def receive(i):
        across(i).wait_recv()
        share(i).start()

    def collect(i):
        share(i).wait_recv()
        prepare(i, 1)

        @pl.when(relay)
        def _():
            hand(i).start()

    def fold(hh):
        columns = pl.ds(hh * half, half)

        def halve(t, carry):
            high, low = split(img[rows(t, w), columns])
            ihi[rows(t, w), :] = high
            ilo[rows(t, w), :] = low
            return carry
        lax.fori_loop(0, steps, halve, 0)
        def act(b, carry):
            here = rows(b, kd)
            ybuf[here, columns] = dot3(vhi[:, here], vlo[:, here], ihi[...], ilo[...], (0,))
            return carry
        lax.fori_loop(0, 2 * S, act, 0)

    def absorb(value, hh, i):
        feed(value)

        def act(b, carry):
            here, columns = rows(b, kd), pl.ds(hh * half, half)
            ybuf[here, columns] += dot3(vhi[rows(i, w), here], vlo[rows(i, w), here], rhi[...], rlo[...], (0,))
            return carry
        lax.fori_loop(0, 2 * S, act, 0)

    def local_step(i, carry):
        @pl.when(i == 0)
        def _():
            receive(i)

        @pl.when(i < steps - 1)
        def _():
            receive(i + 1)
        open_block(i)

        @pl.when(x == 0)
        def _():
            feed(0.5 * vall[rows(i, w), pl.ds(0, half)])
            multiply(pl.ds(0, half))
        collect(i)
        feed(0.5 * vall[rows(i, w), pl.ds(half, half)])
        multiply(pl.ds(half, half))
        return carry

    def piece(k, p=0, buffer=None):
        @pl.when(chained & (z > first))
        def _():
            onward(k).wait_recv()

        if buffer is not None:
            @pl.when(adds & (z == first))
            def _():
                sbuf[rows(k, pw), :] = tbuf[buffer, rows(p, pw), :]

            @pl.when(adds & (z > first))
            def _():
                sbuf[rows(k, pw), :] += tbuf[buffer, rows(p, pw), :]

        @pl.when(chained & (z < last))
        def _():
            onward(k).start()

    def own_tile(i):
        open_block(i)

        @pl.when(adds)
        def _():
            tbuf[lax.rem(i, 2)] = weight * dot3(ahi[...], alo[...], vhi[:, :half], vlo[:, :half], (0,))

    def stream_step(i, carry):
        @pl.when(jnp.logical_not(diag) & (2 * i < steps))
        def _():
            receive(2 * i)
            receive(2 * i + 1)

        @pl.when(i < steps - 1)
        def _():
            own_tile(i + 1)

        def next_piece(p, c2):
            piece(i * Q + p, p, lax.rem(i, 2))
            return c2
        lax.fori_loop(0, Q, next_piece, 0)

        lag = steps // 2

        @pl.when(jnp.logical_not(diag) & (i >= lag) & (2 * (i - lag) < steps))
        def _():
            collect(2 * (i - lag))
            collect(2 * (i - lag) + 1)

        @pl.when(diag)
        def _():
            absorb(sbuf[rows(i, w), :], 0, i)
        return carry

    early = jnp.where((x == 0) & (z == 1), steps, 3 * steps // 8)
    left = (steps - early) * Q
    turns = steps * 2 * S

    def early_step(i, carry):
        @pl.when(2 * i < steps)
        def _():
            receive(2 * i)
            receive(2 * i + 1)

        def next_piece(p, c2):
            piece(i * Q + p)
            return c2
        lax.fori_loop(0, Q, next_piece, 0)
        return carry

    def wide_step(n, carry):
        open_block(n)

        def widen(b, c2):
            here = rows(b, kd)
            high, low = split(dot3(vhi[:, here], vlo[:, here], ahi[...], alo[...], (0,)))
            whi[here, :] = high
            wlo[here, :] = low

            turn = n * 2 * S + b

            @pl.when((turn + 1) * left // turns > turn * left // turns)
            def _():
                piece(early * Q + turn * left // turns)
            return c2
        lax.fori_loop(0, 2 * S, widen, 0)

        @pl.when(x == 0)
        def _():
            feed(sbuf[rows(n, w), :])

        @pl.when(x == 1)
        def _():
            hand(n).wait_recv()
            feed(ubuf[rows(n, w), :])
        columns = rows(x, half)

        def add(b, c2):
            here = rows(b, kd)
            ybuf[here, columns] += dot3(whi[here, :], wlo[here, :], rhi[...], rlo[...], (1,))
            return c2
        lax.fori_loop(0, 2 * S, add, 0)
        return carry

    @pl.when(diag)
    def _():
        lax.fori_loop(0, steps, local_step, 0)
        fold(1)

        @pl.when(x == 0)
        def _():
            fold(0)

        @pl.when(x == 1)
        def _():
            load(0).start()

    @pl.when(catcher)
    def _():
        def catch(i, carry):
            lift(i).wait_recv()
            absorb(ubuf[rows(i, w), :], 1, i)
            return carry
        lax.fori_loop(0, steps, catch, 0)

    @pl.when(helper)
    def _():
        def obtain(i, carry):
            receive(i)
            return carry

        def keep(i, carry):
            collect(i)
            return carry

        def raise_step(i, carry):
            open_block(i)
            sbuf[rows(i, w), :] = dot3(ahi[...], alo[...], vhi[:, half:], vlo[:, half:], (0,))
            lift(i).start()
            return carry
        lax.fori_loop(0, steps, obtain, 0)
        lax.fori_loop(0, steps, keep, 0)
        lax.fori_loop(0, steps, raise_step, 0)

    wide = pair | ((x == 0) & chained & jnp.logical_not(diag))

    @pl.when(wide)
    def _():
        def keep_all(i, carry):
            collect(i)
            return carry
        lax.fori_loop(0, early, early_step, 0)

        def rest(i, carry):
            receive(i)
            return carry
        lax.fori_loop(jnp.minimum(2 * early, steps), steps, rest, 0)
        lax.fori_loop(0, steps, keep_all, 0)
        lax.fori_loop(0, steps, wide_step, 0)

    @pl.when((x == 1) & jnp.logical_not(pair))
    def _():
        own_tile(0)
        lax.fori_loop(0, steps, stream_step, 0)

    reduce_blocks(R, S, blocks, out, ybuf, part, r_sub, r_col, r_row, flip, tile_ref,
                  ps, pr, qs, qr, us, ur, gs, gr, es, er)
    mate().wait_send()

    def drain(i, carry):
        across(i).wait_send()
        share(i).wait_send()

        @pl.when(relay)
        def _():
            hand(i).wait_send()

        @pl.when(helper)
        def _():
            lift(i).wait_send()
        return carry

    lax.fori_loop(0, steps, drain, 0)

    def sent(k, carry):
        @pl.when(source)
        def _():
            origin(k).wait_send()

        @pl.when(chained & (z < last) & jnp.logical_not(source))
        def _():
            onward(k).wait_send()
        return carry

    lax.fori_loop(0, steps * Q, sent, 0)


def image(v, a, R, S):
    m, kd = v.shape
    w = kd
    steps = m // w
    Q = 4
    half = S * kd
    dma = pltpu.SemaphoreType.DMA
    f32, bf16 = jnp.float32, jnp.bfloat16
    blocks, most = owners(R, S)
    nb, hr = len(blocks), kd // S
    return pl.pallas_call(
        functools.partial(image_kernel, R, S, Q, blocks),
        out_shape=jax.ShapeDtypeStruct((kd, half), f32),
        in_specs=[pl.BlockSpec(memory_space=pltpu.VMEM), pl.BlockSpec(memory_space=pl.ANY)],
        out_specs=pl.BlockSpec(memory_space=pltpu.VMEM),
        scratch_shapes=[
            pltpu.VMEM((m, 2 * half), f32), pltpu.VMEM((m, 2 * half), f32),
            pltpu.VMEM((2 * half, 2 * half), f32),
            pltpu.VMEM((m, half), f32), pltpu.VMEM((m, half), f32), pltpu.VMEM((2, w, half), f32),
            pltpu.VMEM((2, m, w), f32), pltpu.VMEM((m, w), bf16), pltpu.VMEM((m, w), bf16),
            pltpu.VMEM((m, 2 * half), bf16), pltpu.VMEM((m, 2 * half), bf16),
            pltpu.VMEM((m, half), bf16), pltpu.VMEM((m, half), bf16),
            pltpu.VMEM((w, half), bf16), pltpu.VMEM((w, half), bf16),
            pltpu.VMEM((2 * half, w), bf16), pltpu.VMEM((2 * half, w), bf16),
            dma, dma((2,)), dma, dma, dma((steps,)), dma((steps,)), dma((steps,)), dma((steps,)),
            dma((steps,)), dma((steps,)), dma((steps * Q,)), dma((steps * Q,)),
            pltpu.VMEM((nb, kd, kd), f32), pltpu.VMEM((nb, hr, kd), f32), pltpu.VMEM((nb, hr, kd), f32),
            pltpu.VMEM((R, most, hr, kd), f32), pltpu.VMEM((nb, kd, hr), f32), pltpu.VMEM((S, kd, kd), f32),
            dma((nb,)), dma((nb,)), dma((nb,)), dma((nb,)), dma((nb,)), dma((R, most)),
            dma((nb,)), dma((nb,)), dma((S,)), dma((S,)),
        ],
        compiler_params=pltpu.CompilerParams(
            collective_id=3, has_side_effects=True, vmem_limit_bytes=66_000_000),
        cost_estimate=pl.CostEstimate(flops=0, bytes_accessed=100_000_000, transcendentals=0),
        name="image",
    )(v, a)


def partial_general(matrix, basis_vectors):
    R = lax.axis_size("row")
    S = lax.axis_size("sub")
    C = lax.axis_size("col") * S
    m, kd = basis_vectors.shape
    K = kd * C
    n = matrix.shape[1]
    per = n // m
    piece = m // R
    own, spread = gather(basis_vectors, R, C // S, S)
    width = K // CHUNKS
    images = []
    for c in range(CHUNKS):
        part = lax.dot_general(
            matrix,
            own[:, c * width : (c + 1) * width],
            (((0,), (0,)), ((), ())),
            precision=lax.Precision.HIGH,
            preferred_element_type=jnp.float32,
        )
        if c == 0:
            part, spread = lax.optimization_barrier((part, spread))
        part = part.reshape(per, R, piece, width).transpose(1, 0, 2, 3).reshape(R * per * piece, width)
        images.append(lax.psum_scatter(part, "row", scatter_dimension=0, tiled=True))
    mine = regroup(spread, C // S, S).reshape(per * piece, K)
    return jnp.concatenate(
        [
            lax.dot_general(
                mine,
                image,
                (((0,), (0,)), ((), ())),
                precision=lax.Precision.HIGH,
                preferred_element_type=jnp.float32,
            )
            for image in images
        ],
        axis=1,
    )


def shards(matrix, basis_vectors, split_size):
    R = lax.axis_size("row")
    X = lax.axis_size("col")
    S = lax.axis_size("sub")
    m, n = matrix.shape
    halves = m == n and R == X * S and X == 2 and S == 2
    if halves:
        child_block = image(basis_vectors, matrix, R, S)
    else:
        child_block = project(partial_general(matrix, basis_vectors), R, X, S)
    row_ids = (
        jnp.arange(child_block.shape[0], dtype=jnp.int32)
        + lax.axis_index("row") * child_block.shape[0]
    )
    col_ids = (
        jnp.arange(child_block.shape[1], dtype=jnp.int32)
        + lax.axis_index("col") * child_block.shape[1]
    )
    leading = split_size[0]
    row_first = row_ids < leading
    col_first = col_ids < leading
    mask_one = row_first[:, None] & col_first[None, :]
    mask_two = jnp.logical_not(row_first)[:, None] & jnp.logical_not(col_first)[None, :]
    selected = jnp.where(lax.axis_index("sub") == 0, mask_one, mask_two)
    return jnp.where(selected, child_block, jnp.zeros((), jnp.float32))[None]


def solution(mesh):
    placed = (
        P(("groups", "row"), ("col", "sub")),
        P(("groups", "row"), ("col", "sub")),
        P("groups"),
    )
    return jax.shard_map(
        shards,
        mesh=mesh,
        in_specs=placed,
        out_specs=P("sub", ("groups", "row"), "col"),
        check_vma=False,
    )
```
